16 devices in a mesh: ep: 16 (over z, y, x, core).
Axes of the slice: x: 2, y: 2, z: 2, core: 2. Of those that a mesh axis runs over, the one named last changes fastest.
Arguments:
- x: bfloat16 [4096, 2048], P('ep')
- gate_w: bfloat16 [2048, 64], replicated
- up_w: bfloat16 [64, 2048, 1408], P('ep')
- down_w: bfloat16 [64, 1408, 2048], P('ep')
- expert_picks: int32 [64, 128], P('ep')
- loss_w: bfloat16 [4096, 2048], P('ep')
Outputs:
- output 1: bfloat16 [4096, 2048], P('ep')
- output 2: float32 [], replicated
- output 3: bfloat16 [4096, 2048], P('ep')
- output 4: bfloat16 [64, 2048, 1408], P('ep')
- output 5: bfloat16 [64, 1408, 2048], P('ep')
- output 6: float32 [2048, 64], replicated
All inputs are finite; a program needn't handle non-finite values.
Results may differ from the reference program's by a relative error of at most 0.02.
Values are sent between devices in bfloat16 or wider.
A program may use at most 1 GiB of HBM per device.

```python
import functools
import math
import jax
import jax.numpy as jnp
from jax import lax

HIDDEN = 2048
FFN_DIM = 1408
EXPERTS = 64
TOK_DEV = 256
GROUP_DEVS = 16

TOKENS = TOK_DEV * GROUP_DEVS
CAPACITY = 2 * TOKENS // EXPERTS
LOCAL_EXPERTS = EXPERTS // GROUP_DEVS
SHARD_PICKS = CAPACITY // GROUP_DEVS
POOL_SIZE = max(SHARD_PICKS, LOCAL_EXPERTS * SHARD_PICKS // 2)


@jax.custom_vjp
def grad_to_bf16(in_value):
    return in_value


def grad_to_bf16_fwd(in_value):
    return in_value, None


def grad_to_bf16_bwd(residual, cotangent):
    return (cotangent.astype(jnp.bfloat16).astype(jnp.float32),)


grad_to_bf16.defvjp(grad_to_bf16_fwd, grad_to_bf16_bwd)


def draw_picks(base_key):
    perm_keys = jax.random.split(jax.random.fold_in(base_key, 1), GROUP_DEVS)
    shard_perms = jax.vmap(functools.partial(jax.random.permutation, x=TOK_DEV))(perm_keys)
    offsets = jax.random.randint(jax.random.fold_in(base_key, 2), (GROUP_DEVS, GROUP_DEVS), 0, TOK_DEV)
    pool_pos = (jnp.arange(LOCAL_EXPERTS)[:, None] * SHARD_PICKS + jnp.arange(SHARD_PICKS)[None, :]) % POOL_SIZE
    perm_pos = (offsets[:, None, :, None] + pool_pos[None, :, None, :]) % TOK_DEV
    src_ids = jnp.arange(GROUP_DEVS)[None, None, :, None]
    token_ids = src_ids * TOK_DEV + shard_perms[src_ids, perm_pos]
    return token_ids.reshape(EXPERTS, CAPACITY).astype(jnp.int32)


def setup_inputs(seed: int = 0) -> dict:
    key_list = jax.random.split(jax.random.key(seed), 6)
    x = jax.random.normal(key_list[0], (TOKENS, HIDDEN), jnp.float32)
    gate_w = jax.random.normal(key_list[1], (HIDDEN, EXPERTS), jnp.float32) * HIDDEN ** -0.5
    up_w = jax.random.normal(key_list[2], (EXPERTS, HIDDEN, FFN_DIM), jnp.float32) * HIDDEN ** -0.5
    down_w = jax.random.normal(key_list[3], (EXPERTS, FFN_DIM, HIDDEN), jnp.float32) * (EXPERTS / (2.0 * math.sqrt(FFN_DIM)))
    loss_w = jax.random.normal(key_list[5], (TOKENS, HIDDEN), jnp.float32)
    return {'x': x.astype(jnp.bfloat16), 'gate_w': gate_w.astype(jnp.bfloat16), 'up_w': up_w.astype(jnp.bfloat16), 'down_w': down_w.astype(jnp.bfloat16), 'expert_picks': draw_picks(key_list[4]), 'loss_w': loss_w.astype(jnp.bfloat16)}


def mixed_tokens(x_f32, gate_w32, up_w, down_w, expert_picks):
    logits = grad_to_bf16(jnp.dot(x_f32, gate_w32))
    gate_probs = jax.nn.softmax(logits, axis=-1)
    gate_vals = gate_probs[expert_picks, jnp.arange(EXPERTS)[:, None]]

    def one_expert(operands):
        pick_ids, up_one, down_one, gate_one = operands
        tok_rows = grad_to_bf16(x_f32[pick_ids])
        pre_act = grad_to_bf16(jnp.dot(tok_rows, up_one.astype(jnp.float32)))
        hidden_act = jax.nn.gelu(pre_act).astype(jnp.bfloat16)
        expert_out = jnp.dot(hidden_act.astype(jnp.float32), down_one.astype(jnp.float32)).astype(jnp.bfloat16)
        return gate_one[:, None] * expert_out.astype(jnp.float32)

    contrib = lax.map(jax.checkpoint(one_expert), (expert_picks, up_w, down_w, gate_vals))
    return x_f32.at[expert_picks.reshape(-1)].add(contrib.reshape(-1, HIDDEN))


def reference(x, gate_w, up_w, down_w, expert_picks, loss_w):
    loss_scale = 1.0 / math.sqrt(TOKENS * HIDDEN)
    mixed_f32, pullback = jax.vjp(functools.partial(mixed_tokens, expert_picks=expert_picks), x.astype(jnp.float32), gate_w.astype(jnp.float32), up_w, down_w)
    y = mixed_f32.astype(jnp.bfloat16)
    weight_f32 = loss_w.astype(jnp.float32)
    loss = jnp.sum(y.astype(jnp.float32) * weight_f32) * loss_scale
    grad_x, grad_gate, grad_up, grad_down = pullback(weight_f32 * loss_scale)
    return y, loss, grad_x.astype(jnp.bfloat16), grad_up, grad_down, grad_gate
```

```python
import functools
import math
import jax
import jax.numpy as jnp
from jax import lax
from jax.experimental import pallas as pl
from jax.experimental.pallas import tpu as pltpu
from jax.sharding import PartitionSpec as P

BF = jnp.bfloat16
F32 = jnp.float32
MESH = pl.DeviceIdType.MESH
N = 16
TOK = 256
LE = 4
CAP = 128
HID = 2048
FF = 1408
CH = 512
NCH = HID // CH
ORDER = (14, 15, 6, 10, 12, 7, 11, 13, 2, 4, 8, 3, 5, 9, 1)


def dot(a, b, ca=1, cb=0):
    return lax.dot_general(a, b, (((ca,), (cb,)), ((), ())), preferred_element_type=F32)


def iota(shape, dim):
    return lax.broadcasted_iota(jnp.int32, shape, dim)


def ones_where(cond):
    return jnp.where(cond, 1.0, 0.0).astype(BF)


def split3(v):
    hi = v.astype(BF)
    rest = v - hi.astype(F32)
    mid = rest.astype(BF)
    low = (rest - mid.astype(F32)).astype(BF)
    return hi, mid, low


def flip(me, k):
    out = 0
    for b in range(4):
        bit = (me // (1 << b)) % 2
        if (k >> b) & 1:
            bit = 1 - bit
        out = out + bit * (1 << b)
    return out


def comm_kernel(scale, sel_ref, x_hbm, gw_hbm, up_hbm, dn_hbm, r_hbm,
                y_out, gx_out, gg_out, loss_out, xl_out, u_out, dh_out, da_out,
                x_v, r_v, gw_v, w1, w2, xsend, rsend, xrecv, rrecv, hsend, hrecv, gsend, grecv,
                xl_v, dh_v, u_v, gp_v, da_v, ggsend, ggrecv, ggall, selsend, selall, gates, gates_all,
                losssend, lossall, one_v, c_v, e_v, probs_v, dlog_v,
                ld_sem, w_sem, out_sem, send_sem, recv_sem):
    me = lax.axis_index('ep')
    peers = [flip(me, k) for k in ORDER]

    def load(src, dst, i):
        return pltpu.make_async_copy(src, dst, ld_sem.at[i])

    def weight1(e, slot):
        return pltpu.make_async_copy(up_hbm.at[e], w1.at[slot], w_sem.at[0, slot])

    def weight2(e, slot):
        return pltpu.make_async_copy(dn_hbm.at[e], w2.at[slot], w_sem.at[1, slot])

    def push(src, dst, peer, i):
        return pltpu.make_async_remote_copy(src_ref=src, dst_ref=dst, send_sem=send_sem.at[i], recv_sem=recv_sem.at[i],
                                            device_id=(peer,), device_id_type=MESH)

    def wait_recv(buf, i):
        part = buf.at[pl.ds(0, N - 1)]
        pltpu.make_async_copy(part, part, recv_sem.at[i]).wait()

    def wait_send(buf, i):
        part = buf.at[pl.ds(0, N - 1)]
        pltpu.make_async_copy(part, part, send_sem.at[i]).wait()

    cp_x = load(x_hbm, x_v, 0)
    cp_g = load(gw_hbm, gw_v, 1)
    cp_r = load(r_hbm, r_v, 2)
    cp_x.start()
    cp_g.start()
    cp_r.start()

    sel = sel_ref[...]
    selsend[...] = jnp.zeros_like(selsend)
    selsend[0:LE, :] = sel
    selall[pl.ds(me, 1)] = selsend[...].reshape(1, 8, CAP)

    barrier = pltpu.get_barrier_semaphore()
    for p in peers:
        pl.semaphore_signal(barrier, inc=1, device_id=(p,), device_id_type=MESH)
    pl.semaphore_wait(barrier, N - 1)

    for p in peers:
        push(selsend, selall.at[me], p, 0).start()
    for e in range(3):
        weight1(e, e).start()
        weight2(e, e).start()

    cp_g.wait()
    cp_x.wait()
    logits = dot(x_v[...], gw_v[...], 1, 1)
    ex = jnp.exp(logits - jnp.max(logits, axis=1, keepdims=True))
    probs = ex / jnp.sum(ex, axis=1, keepdims=True)
    probs_v[...] = probs

    below = ones_where(iota((TOK, TOK), 1) < iota((TOK, TOK), 0))
    slot_lane = (iota((TOK, TOK), 1) % 16).astype(F32)

    tok_row = iota((TOK, CAP), 0)
    same = iota((CAP, TOK), 0) // 8 == iota((CAP, TOK), 1) // 16
    fold = ones_where(same)
    base = (iota((1, CAP), 1) // 8) * TOK
    hits = [ones_where(tok_row == sel[l:l + 1, :] - base) for l in range(LE)]
    count = dot(hits[0], fold)
    for l in range(1, LE):
        count = count + dot(hits[l], fold)
    pres = count > 0.5
    rank = dot(below, ones_where(pres))
    pick_of = jnp.where(pres, jnp.where(rank == slot_lane, 1.0, 0.0), 0.0).astype(BF)
    for l in range(LE):
        e_v[l] = jnp.where(same, dot(hits[l], pick_of, 0, 0), 0.0).astype(BF)

    for_wait = selall.at[pl.ds(0, N - 1)]
    pltpu.make_async_copy(for_wait, for_wait, recv_sem.at[0]).wait()
    everyone = selall[...].reshape(8 * N, CAP)
    mine = jnp.where(iota((8 * N, CAP), 1) // 8 == me, everyone - me * TOK, 0).astype(F32).astype(BF)
    place = ones_where(iota((CAP, 512), 0) % 8 == iota((CAP, 512), 1) % 8)
    spread = dot(mine, place)
    lane = iota((8 * N, 512), 1)
    want = ((lane % 256) // 16) * 8 + 2 * (lane // 256) + (lane % 16) // 8
    ids = jnp.sum(jnp.where(iota((8 * N, 512), 0) == want, spread, 0.0), axis=0, keepdims=True)
    one = jnp.where(iota((TOK, 512), 0).astype(F32) == ids, 1.0, 0.0)
    one_v[...] = one.astype(BF)
    fold2 = ones_where((iota((512, TOK), 0) % 256) // 16 == iota((512, TOK), 1) // 16)
    pres2 = dot(one_v[...], fold2) > 0.5
    rank2 = dot(below, ones_where(pres2))
    give = jnp.where(pres2, jnp.where(rank2 == slot_lane, 1.0, 0.0), 0.0).astype(BF)
    give_t = give.T

    def gather(src, dst):
        def step(c, carry):
            cols = pl.ds(pl.multiple_of(c * CH, CH), CH)
            dst[:, :, cols] = dot(give_t, src[:, cols]).astype(BF).reshape(N, 16, CH)
            return carry
        lax.fori_loop(0, NCH, step, 0)

    gather(x_v, xsend)
    for p in peers:
        push(xsend.at[p], xrecv.at[me], p, 1).start()
    xrecv[pl.ds(me, 1)] = xsend[pl.ds(me, 1)]

    rep = ones_where(iota((64, 512), 0) == 4 * ((iota((64, 512), 1) % 256) // 16) + 2 * (iota((64, 512), 1) // 256)
                     + (iota((64, 512), 1) % 16) // 8)
    wide = 0.0
    for term in split3(probs_v[...]):
        wide = wide + dot(term, rep)
    comb = wide * one
    for i, term in enumerate(split3(comb)):
        c_v[i] = term
    gates[...] = jnp.sum(comb, axis=0, keepdims=True)
    for p in peers:
        push(gates, gates_all.at[me], p, 2).start()
    gates_all[pl.ds(me, 1)] = gates[...].reshape(1, 1, 512)

    cp_r.wait()
    gather(r_v, rsend)
    for p in peers:
        push(rsend.at[p], rrecv.at[me], p, 3).start()
    rrecv[pl.ds(me, 1)] = rsend[pl.ds(me, 1)]

    wait_recv(xrecv, 1)

    def fwd(q, carry):
        for j in range(2):
            e = 2 * q + j
            slot = e % 3
            xl = dot(e_v[e], xrecv[...].reshape(TOK, HID)).astype(BF)
            xl_v[e] = xl
            weight1(e, slot).wait()
            a = dot(xl_v[e], w1[slot])
            if j == 0:
                @pl.when(q == 0)
                def _():
                    weight1(3, 0).start()
            k0 = math.sqrt(2.0 / math.pi)
            t = jnp.tanh(k0 * (a + 0.044715 * (a * a * a)))
            u_v[e] = (0.5 * a * (1.0 + t)).astype(BF)
            gp_v[e] = 0.5 * (1.0 + t) + 0.5 * a * (1.0 - t * t) * (k0 * (1.0 + 3.0 * 0.044715 * (a * a)))
        weight2(2 * q, (2 * q) % 3).wait()
        weight2(2 * q + 1, (2 * q + 1) % 3).wait()

        def step(c, carry):
            cols = pl.ds(pl.multiple_of(c * CH, CH), CH)
            outs = [dot(u_v[2 * q + j], w2[(2 * q + j) % 3, :, cols]).reshape(N, 8, CH) for j in range(2)]
            hsend[q, :, :, cols] = jnp.concatenate(outs, axis=1).astype(BF)
            return carry
        lax.fori_loop(0, NCH, step, 0)

        @pl.when(q == 0)
        def _():
            weight2(3, 0).start()
        for p in peers:
            push(hsend.at[q, p], hrecv.at[q, me], p, 4 + q).start()
        hrecv[q, pl.ds(me, 1)] = hsend[q, pl.ds(me, 1)]
        return carry
    lax.fori_loop(0, 2, fwd, 0)
    pltpu.make_async_copy(xl_v, xl_out, out_sem.at[0]).start()
    pltpu.make_async_copy(u_v, u_out, out_sem.at[1]).start()

    wait_recv(gates_all, 2)
    wait_recv(rrecv, 3)

    def bwd(q, carry):
        for j in range(2):
            e = 2 * (1 - q) + j
            slot = (1 - q) * (2 - 2 * j) + q * (2 - j)
            if j == 0:
                @pl.when(q == 1)
                def _():
                    weight1(0, 2).wait()
                    weight2(0, 2).wait()
            rows = jnp.broadcast_to(gates_all[...], (N, 8, 512)).reshape(CAP, 512)
            here = iota((CAP, 512), 1) == (1 - q) * 256 + me * 16 + j * 8 + iota((CAP, 512), 0) % 8
            gcol = jnp.sum(jnp.where(here, rows, 0.0), axis=1, keepdims=True)

            def rstep(c, carry):
                cols = pl.ds(pl.multiple_of(c * CH, CH), CH)
                rl = dot(e_v[e], rrecv[:, :, cols].reshape(TOK, CH))
                dh_v[e, :, cols] = (gcol * (rl * scale)).astype(BF)
                return carry
            lax.fori_loop(0, NCH, rstep, 0)
            du = dot(dh_v[e], w2[slot], 1, 1).astype(BF).astype(F32)
            if j == 0:
                @pl.when(q == 0)
                def _():
                    weight2(0, 2).start()
            da_v[e] = (gp_v[e] * du).astype(BF)

        def step(c, carry):
            cols = pl.ds(pl.multiple_of(c * CH, CH), CH)
            outs = []
            for j in range(2):
                slot = (1 - q) * (2 - 2 * j) + q * (2 - j)
                outs.append(dot(da_v[2 * (1 - q) + j], w1[slot, cols, :], 1, 1).reshape(N, 8, CH))
            gsend[1 - q, :, :, cols] = jnp.concatenate(outs, axis=1).astype(BF)
            return carry
        lax.fori_loop(0, NCH, step, 0)

        @pl.when(q == 0)
        def _():
            weight1(0, 2).start()
        for p in peers:
            push(gsend.at[1 - q, p], grecv.at[1 - q, me], p, 6 + q).start()
        grecv[1 - q, pl.ds(me, 1)] = gsend[1 - q, pl.ds(me, 1)]
        return carry
    lax.fori_loop(0, 2, bwd, 0)
    pltpu.make_async_copy(dh_v, dh_out, out_sem.at[2]).start()
    pltpu.make_async_copy(da_v, da_out, out_sem.at[3]).start()

    wait_recv(hrecv.at[0], 4)
    wait_recv(hrecv.at[1], 5)
    inner = dot(r_v[...], hrecv[...].reshape(512, HID), 1, 1)
    masked = inner * one_v[...].astype(F32)
    gather_e = ones_where(iota((512, 64), 1) == 4 * ((iota((512, 64), 0) % 256) // 16) + 2 * (iota((512, 64), 0) // 256)
                          + (iota((512, 64), 0) % 16) // 8)
    ds = 0.0
    for term in split3(masked):
        ds = ds + dot(term, gather_e)
    ds = ds * scale
    probs = probs_v[...]
    dlog = (probs * (ds - jnp.sum(probs * ds, axis=1, keepdims=True))).astype(BF)
    dlog_v[...] = dlog
    dlog_t = dlog.astype(F32).T.astype(BF)
    for c in range(NCH):
        part = dot(dlog_t, x_v[:, c * CH:(c + 1) * CH])
        for i in range(CH // 128):
            ggsend[c * (CH // 128) + i] = part[:, i * 128:(i + 1) * 128]
    for p in peers:
        push(ggsend.at[p], ggrecv.at[me], p, 8).start()
    ggrecv[pl.ds(me, 1)] = ggsend[pl.ds(me, 1)]

    wait_send(xsend, 1)

    def ystep(c, acc):
        cols = pl.ds(pl.multiple_of(c * CH, CH), CH)
        h = hrecv[:, :, :, cols].reshape(512, CH)
        tot = x_v[:, cols].astype(F32) + (dot(c_v[0], h) + dot(c_v[1], h) + dot(c_v[2], h))
        y = tot.astype(BF)
        xsend[:, :, cols] = y.reshape(N, 16, CH)
        return acc + jnp.sum(y.astype(F32) * r_v[:, cols].astype(F32), axis=0, keepdims=True)
    losssend[...] = lax.fori_loop(0, NCH, ystep, jnp.zeros((1, CH), F32))
    cp_y = pltpu.make_async_copy(xsend, y_out, out_sem.at[4])
    cp_y.start()
    for p in peers:
        push(losssend, lossall.at[me], p, 9).start()
    lossall[pl.ds(me, 1)] = losssend[...].reshape(1, 1, CH)

    wait_recv(ggrecv, 8)
    total = ggrecv[0]
    for i in range(1, N):
        total = total + ggrecv[i]
    wait_send(ggsend, 8)
    ggsend[0] = total
    for p in peers:
        push(ggsend.at[0], ggall.at[me], p, 10).start()
    ggall[pl.ds(me, 1)] = total.reshape(1, 64, 128)

    wait_send(rsend, 3)
    wait_recv(grecv.at[1], 6)
    wait_recv(grecv.at[0], 7)

    def gstep(c, carry):
        cols = pl.ds(pl.multiple_of(c * CH, CH), CH)
        tot = r_v[:, cols].astype(F32) * scale + dot(one_v[...], grecv[:, :, :, cols].reshape(512, CH))
        tot = tot + dot(dlog_v[...], gw_v[:, cols])
        rsend[:, :, cols] = tot.astype(BF).reshape(N, 16, CH)
        return carry
    lax.fori_loop(0, NCH, gstep, 0)
    cp_gx = pltpu.make_async_copy(rsend, gx_out, out_sem.at[5])
    cp_gx.start()

    wait_recv(lossall, 9)
    loss_out[0, 0] = jnp.sum(lossall[...]) * scale
    wait_recv(ggall, 10)
    cp_gg = [pltpu.make_async_copy(ggall.at[i], gg_out.at[:, pl.ds(i * 128, 128)], out_sem.at[6]) for i in range(N)]
    for cp in cp_gg:
        cp.start()

    wait_send(selall, 0)
    wait_send(gates_all, 2)
    wait_send(hsend.at[0], 4)
    wait_send(hsend.at[1], 5)
    wait_send(gsend.at[1], 6)
    wait_send(gsend.at[0], 7)
    wait_send(lossall, 9)
    wait_send(ggall, 10)
    pltpu.make_async_copy(xl_v, xl_out, out_sem.at[0]).wait()
    pltpu.make_async_copy(u_v, u_out, out_sem.at[1]).wait()
    pltpu.make_async_copy(dh_v, dh_out, out_sem.at[2]).wait()
    pltpu.make_async_copy(da_v, da_out, out_sem.at[3]).wait()
    cp_y.wait()
    cp_gx.wait()
    for cp in cp_gg:
        cp.wait()


def comm_call(sel, x, gw, up, dn, r, scale):
    any_ = pl.BlockSpec(memory_space=pl.ANY)
    vmem = pl.BlockSpec(memory_space=pltpu.VMEM)
    V = pltpu.VMEM
    shape = jax.ShapeDtypeStruct
    return pl.pallas_call(
        functools.partial(comm_kernel, scale),
        out_shape=[shape((N, 16, HID), BF), shape((N, 16, HID), BF), shape((64, HID), F32), shape((1, 1), F32),
                   shape((LE, CAP, HID), BF), shape((LE, CAP, FF), BF), shape((LE, CAP, HID), BF), shape((LE, CAP, FF), BF)],
        in_specs=[vmem, any_, any_, any_, any_, any_],
        out_specs=[any_, any_, any_, pl.BlockSpec(memory_space=pltpu.SMEM), any_, any_, any_, any_],
        scratch_shapes=[
            V((TOK, HID), BF), V((TOK, HID), BF), V((64, HID), BF),
            V((3, HID, FF), BF), V((3, FF, HID), BF),
            V((N, 16, HID), BF), V((N, 16, HID), BF), V((N, 16, HID), BF), V((N, 16, HID), BF),
            V((2, N, 16, HID), BF), V((2, N, 16, HID), BF), V((2, N, 16, HID), BF), V((2, N, 16, HID), BF),
            V((LE, CAP, HID), BF), V((LE, CAP, HID), BF), V((LE, CAP, FF), BF), V((LE, CAP, FF), F32), V((LE, CAP, FF), BF),
            V((N, 64, 128), F32), V((N, 64, 128), F32), V((N, 64, 128), F32),
            V((8, CAP), jnp.int32), V((N, 8, CAP), jnp.int32), V((1, 512), F32), V((N, 1, 512), F32),
            V((1, CH), F32), V((N, 1, CH), F32),
            V((TOK, 512), BF), V((3, TOK, 512), BF), V((LE, CAP, TOK), BF), V((TOK, 64), F32), V((TOK, 64), BF),
            pltpu.SemaphoreType.DMA((3,)), pltpu.SemaphoreType.DMA((2, 3)), pltpu.SemaphoreType.DMA((7,)),
            pltpu.SemaphoreType.DMA((11,)), pltpu.SemaphoreType.DMA((11,)),
        ],
        compiler_params=pltpu.CompilerParams(collective_id=0, has_side_effects=True, vmem_limit_bytes=67043328),
        name='exchange',
    )(sel, x, gw, up, dn, r)


def wgrad_kernel(xl, da, u, dh, y_in, gx_in, gg_in, loss_in, g1, g2, y, gx, gg, loss):
    g1[0] = dot(xl[0], da[0], 0, 0).astype(BF)
    g2[0] = dot(u[0], dh[0], 0, 0).astype(BF)
    y[...] = y_in[...]
    gx[...] = gx_in[...]
    gg[...] = gg_in[...]

    @pl.when((pl.program_id(0) == 0) & (pl.program_id(1) == 0))
    def _():
        loss[0, 0] = loss_in[0, 0]


def wgrad_call(xl, u, dh, da, y, gx, gg, loss):
    shape = jax.ShapeDtypeStruct
    rows = pl.BlockSpec((1, 16, HID), lambda e, c: (e * NCH + c, 0, 0))
    cols = pl.BlockSpec((64, 128), lambda e, c: (0, e * NCH + c))
    whole = pl.BlockSpec(memory_space=pltpu.SMEM)
    return pl.pallas_call(
        wgrad_kernel,
        grid=(LE, NCH),
        in_specs=[pl.BlockSpec((1, CAP, CH), lambda e, c: (e, 0, c)), pl.BlockSpec((1, CAP, FF), lambda e, c: (e, 0, 0)),
                  pl.BlockSpec((1, CAP, FF), lambda e, c: (e, 0, 0)), pl.BlockSpec((1, CAP, CH), lambda e, c: (e, 0, c)),
                  rows, rows, cols, whole],
        out_specs=[pl.BlockSpec((1, CH, FF), lambda e, c: (e, c, 0)), pl.BlockSpec((1, FF, CH), lambda e, c: (e, 0, c)),
                   rows, rows, cols, whole],
        out_shape=[shape((LE, HID, FF), BF), shape((LE, FF, HID), BF), shape((N, 16, HID), BF), shape((N, 16, HID), BF),
                   shape((64, HID), F32), shape((1, 1), F32)],
        compiler_params=pltpu.CompilerParams(vmem_limit_bytes=67043328),
        name='weight_grads',
    )(xl, da, u, dh, y, gx, gg, loss)


def solution(mesh):
    def device_step(x, gate_w, up_w, down_w, expert_picks, loss_w):
        scale = 1.0 / math.sqrt(TOK * N * HID)
        y, gx, gg, loss, xl, u, dh, da = comm_call(expert_picks, x, gate_w.T, up_w, down_w, loss_w, scale)
        grad_up, grad_down, y, gx, gg, loss = wgrad_call(xl, u, dh, da, y, gx, gg, loss)
        return y.reshape(TOK, HID), loss[0, 0], gx.reshape(TOK, HID), grad_up, grad_down, gg.T

    return jax.shard_map(device_step, mesh=mesh,
                         in_specs=(P('ep'), P(), P('ep'), P('ep'), P('ep'), P('ep')),
                         out_specs=(P('ep'), P(), P('ep'), P('ep'), P('ep'), P()),
                         check_vma=False)
```

```python
import functools
import math
import jax
import jax.numpy as jnp
from jax import lax
from jax.experimental import pallas as pl
from jax.experimental.pallas import tpu as pltpu
from jax.sharding import PartitionSpec as P

BF = jnp.bfloat16
F32 = jnp.float32
MESH = pl.DeviceIdType.MESH
N = 16
TOK = 256
LE = 4
CAP = 128
HID = 2048
FF = 1408
CH = 512
NCH = HID // CH
NOW = 2
ORDER = (14, 15, 6, 10, 12, 7, 11, 13, 2, 4, 8, 3, 5, 9, 1)


def dot(a, b, ca=1, cb=0):
    return lax.dot_general(a, b, (((ca,), (cb,)), ((), ())), preferred_element_type=F32)


def iota(shape, dim):
    return lax.broadcasted_iota(jnp.int32, shape, dim)


def ones_where(cond):
    return jnp.where(cond, 1.0, 0.0).astype(BF)


def split3(v):
    hi = v.astype(BF)
    rest = v - hi.astype(F32)
    mid = rest.astype(BF)
    low = (rest - mid.astype(F32)).astype(BF)
    return hi, mid, low


def flip(me, k):
    out = 0
    for b in range(4):
        bit = (me // (1 << b)) % 2
        if (k >> b) & 1:
            bit = 1 - bit
        out = out + bit * (1 << b)
    return out


def comm_kernel(scale, sel_ref, x_hbm, gw_hbm, up_hbm, dn_hbm, r_hbm,
                y_out, gnow_out, glater_out, one_out, dlog_out, gg_out, loss_out, xl_out, u_out, dh_out, da_out,
                x_v, r_v, gw_v, w1, w2, xsend, rsend, xrecv, rrecv, hsend, hrecv, gsend,
                xl_v, dh_v, u_v, gp_v, da_v, ggpart, ggpair, gghalf, ggrecv, ggall, selsend, selall, gates, gates_all,
                losssend, lossall, one_v, c_v, e_v, probs_v, dlog_v,
                ld_sem, w_sem, out_sem, send_sem, recv_sem):
    me = lax.axis_index('ep')
    peers = [flip(me, k) for k in ORDER]
    core, chip, twin = me % 2, me // 2, flip(me, 1)
    others = [flip(me, k) for k in ORDER if k % 2 == 0]

    def load(src, dst, i):
        return pltpu.make_async_copy(src, dst, ld_sem.at[i])

    def weight1(e, slot):
        return pltpu.make_async_copy(up_hbm.at[e], w1.at[slot], w_sem.at[0, slot])

    def weight2(e, slot):
        return pltpu.make_async_copy(dn_hbm.at[e], w2.at[slot], w_sem.at[1, slot])

    def push(src, dst, peer, i):
        return pltpu.make_async_remote_copy(src_ref=src, dst_ref=dst, send_sem=send_sem.at[i], recv_sem=recv_sem.at[i],
                                            device_id=(peer,), device_id_type=MESH)

    def wait_recv(buf, i, n=N - 1):
        part = buf.at[pl.ds(0, n)]
        pltpu.make_async_copy(part, part, recv_sem.at[i]).wait()

    def wait_send(buf, i, n=N - 1):
        part = buf.at[pl.ds(0, n)]
        pltpu.make_async_copy(part, part, send_sem.at[i]).wait()

    cp_x = load(x_hbm, x_v, 0)
    cp_g = load(gw_hbm, gw_v, 1)
    cp_r = load(r_hbm, r_v, 2)
    cp_x.start()
    cp_g.start()
    cp_r.start()

    sel = sel_ref[...]
    selsend[...] = jnp.zeros_like(selsend)
    selsend[0:LE, :] = sel
    selall[pl.ds(me, 1)] = selsend[...].reshape(1, 8, CAP)

    barrier = pltpu.get_barrier_semaphore()
    for p in peers:
        pl.semaphore_signal(barrier, inc=1, device_id=(p,), device_id_type=MESH)
    pl.semaphore_wait(barrier, N - 1)

    for p in peers:
        push(selsend, selall.at[me], p, 0).start()
    for e in range(3):
        weight1(e, e).start()
        weight2(e, e).start()

    cp_g.wait()
    cp_x.wait()
    logits = dot(x_v[...], gw_v[...], 1, 1)
    ex = jnp.exp(logits - jnp.max(logits, axis=1, keepdims=True))
    probs = ex / jnp.sum(ex, axis=1, keepdims=True)
    probs_v[...] = probs

    below = ones_where(iota((TOK, TOK), 1) < iota((TOK, TOK), 0))
    slot_lane = (iota((TOK, TOK), 1) % 16).astype(F32)

    tok_row = iota((TOK, CAP), 0)
    same = iota((CAP, TOK), 0) // 8 == iota((CAP, TOK), 1) // 16
    fold = ones_where(same)
    base = (iota((1, CAP), 1) // 8) * TOK
    hits = [ones_where(tok_row == sel[l:l + 1, :] - base) for l in range(LE)]
    count = dot(hits[0], fold)
    for l in range(1, LE):
        count = count + dot(hits[l], fold)
    pres = count > 0.5
    rank = dot(below, ones_where(pres))
    pick_of = jnp.where(pres, jnp.where(rank == slot_lane, 1.0, 0.0), 0.0).astype(BF)
    for l in range(LE):
        e_v[l] = jnp.where(same, dot(hits[l], pick_of, 0, 0), 0.0).astype(BF)

    for_wait = selall.at[pl.ds(0, N - 1)]
    pltpu.make_async_copy(for_wait, for_wait, recv_sem.at[0]).wait()
    everyone = selall[...].reshape(8 * N, CAP)
    mine = jnp.where(iota((8 * N, CAP), 1) // 8 == me, everyone - me * TOK, 0).astype(F32).astype(BF)
    place = ones_where(iota((CAP, 512), 0) % 8 == iota((CAP, 512), 1) % 8)
    spread = dot(mine, place)
    lane = iota((8 * N, 512), 1)
    want = ((lane % 256) // 16) * 8 + 2 * (lane // 256) + (lane % 16) // 8
    ids = jnp.sum(jnp.where(iota((8 * N, 512), 0) == want, spread, 0.0), axis=0, keepdims=True)
    one = jnp.where(iota((TOK, 512), 0).astype(F32) == ids, 1.0, 0.0)
    one_v[...] = one.astype(BF)
    fold2 = ones_where((iota((512, TOK), 0) % 256) // 16 == iota((512, TOK), 1) // 16)
    pres2 = dot(one_v[...], fold2) > 0.5
    rank2 = dot(below, ones_where(pres2))
    give = jnp.where(pres2, jnp.where(rank2 == slot_lane, 1.0, 0.0), 0.0).astype(BF)
    give_t = give.T

    def gather(src, dst):
        def step(c, carry):
            cols = pl.ds(pl.multiple_of(c * CH, CH), CH)
            dst[:, :, cols] = dot(give_t, src[:, cols]).astype(BF).reshape(N, 16, CH)
            return carry
        lax.fori_loop(0, NCH, step, 0)

    gather(x_v, xsend)
    for p in peers:
        push(xsend.at[p], xrecv.at[me], p, 1).start()
    xrecv[pl.ds(me, 1)] = xsend[pl.ds(me, 1)]

    rep = ones_where(iota((64, 512), 0) == 4 * ((iota((64, 512), 1) % 256) // 16) + 2 * (iota((64, 512), 1) // 256)
                     + (iota((64, 512), 1) % 16) // 8)
    wide = 0.0
    for term in split3(probs_v[...]):
        wide = wide + dot(term, rep)
    comb = wide * one
    for i, term in enumerate(split3(comb)):
        c_v[i] = term
    gates[...] = jnp.sum(comb, axis=0, keepdims=True)
    for p in peers:
        push(gates, gates_all.at[me], p, 2).start()
    gates_all[pl.ds(me, 1)] = gates[...].reshape(1, 1, 512)

    cp_r.wait()
    gather(r_v, rsend)
    for p in peers:
        push(rsend.at[p], rrecv.at[me], p, 3).start()
    rrecv[pl.ds(me, 1)] = rsend[pl.ds(me, 1)]

    wait_recv(xrecv, 1)

    def fwd(q, carry):
        for j in range(2):
            e = 2 * q + j
            slot = e % 3
            xl = dot(e_v[e], xrecv[...].reshape(TOK, HID)).astype(BF)
            xl_v[e] = xl
            weight1(e, slot).wait()
            a = dot(xl_v[e], w1[slot])
            if j == 0:
                @pl.when(q == 0)
                def _():
                    weight1(3, 0).start()
            k0 = math.sqrt(2.0 / math.pi)
            t = jnp.tanh(k0 * (a + 0.044715 * (a * a * a)))
            u_v[e] = (0.5 * a * (1.0 + t)).astype(BF)
            gp_v[e] = 0.5 * (1.0 + t) + 0.5 * a * (1.0 - t * t) * (k0 * (1.0 + 3.0 * 0.044715 * (a * a)))
        weight2(2 * q, (2 * q) % 3).wait()
        weight2(2 * q + 1, (2 * q + 1) % 3).wait()

        def step(c, carry):
            cols = pl.ds(pl.multiple_of(c * CH, CH), CH)
            outs = [dot(u_v[2 * q + j], w2[(2 * q + j) % 3, :, cols]).reshape(N, 8, CH) for j in range(2)]
            hsend[q, :, :, cols] = jnp.concatenate(outs, axis=1).astype(BF)
            return carry
        lax.fori_loop(0, NCH, step, 0)

        @pl.when(q == 0)
        def _():
            weight2(3, 0).start()
        for p in peers:
            push(hsend.at[q, p], hrecv.at[q, me], p, 4 + q).start()
        hrecv[q, pl.ds(me, 1)] = hsend[q, pl.ds(me, 1)]
        return carry
    lax.fori_loop(0, 2, fwd, 0)
    pltpu.make_async_copy(xl_v, xl_out, out_sem.at[0]).start()
    pltpu.make_async_copy(u_v, u_out, out_sem.at[1]).start()

    wait_recv(gates_all, 2)
    wait_recv(rrecv, 3)

    def send_now(c):
        cols = pl.ds(c * CH, CH)
        for p in peers:
            push(gsend.at[1, p, :, cols], gnow_out.at[me, :, cols], p, 6 + c).start()
        pltpu.make_async_copy(gsend.at[1, me, :, cols], gnow_out.at[me, :, cols], out_sem.at[7 + c]).start()

    def bwd(q, carry):
        for j in range(2):
            e = 2 * (1 - q) + j
            slot = (1 - q) * (2 - 2 * j) + q * (2 - j)
            if j == 0:
                @pl.when(q == 1)
                def _():
                    weight1(0, 2).wait()
                    weight2(0, 2).wait()
            rows = jnp.broadcast_to(gates_all[...], (N, 8, 512)).reshape(CAP, 512)
            here = iota((CAP, 512), 1) == (1 - q) * 256 + me * 16 + j * 8 + iota((CAP, 512), 0) % 8
            gcol = jnp.sum(jnp.where(here, rows, 0.0), axis=1, keepdims=True)

            def rstep(c, carry):
                cols = pl.ds(pl.multiple_of(c * CH, CH), CH)
                rl = dot(e_v[e], rrecv[:, :, cols].reshape(TOK, CH))
                dh_v[e, :, cols] = (gcol * (rl * scale)).astype(BF)
                return carry
            lax.fori_loop(0, NCH, rstep, 0)
            du = dot(dh_v[e], w2[slot], 1, 1).astype(BF).astype(F32)
            if j == 0:
                @pl.when(q == 0)
                def _():
                    weight2(0, 2).start()
            da_v[e] = (gp_v[e] * du).astype(BF)

        def step(c, carry):
            cols = pl.ds(pl.multiple_of(c * CH, CH), CH)
            outs = []
            for j in range(2):
                slot = (1 - q) * (2 - 2 * j) + q * (2 - j)
                outs.append(dot(da_v[2 * (1 - q) + j], w1[slot, cols, :], 1, 1).reshape(N, 8, CH))
            gsend[1 - q, :, :, cols] = jnp.concatenate(outs, axis=1).astype(BF)
            return carry
        lax.fori_loop(0, NCH, step, 0)

        @pl.when(q == 0)
        def _():
            weight1(0, 2).start()
        @pl.when(q == 0)
        def _():
            send_now(0)
        return carry
    lax.fori_loop(0, 2, bwd, 0)
    later = [pltpu.make_async_copy(gsend.at[0], glater_out.at[:, :, pl.ds(0, HID)], out_sem.at[5]),
             pltpu.make_async_copy(gsend.at[1, :, :, pl.ds(NOW * CH, HID - NOW * CH)],
                                   glater_out.at[:, :, pl.ds(HID, HID - NOW * CH)], out_sem.at[9])]
    for cp in later:
        cp.start()
    pltpu.make_async_copy(dh_v, dh_out, out_sem.at[2]).start()
    pltpu.make_async_copy(da_v, da_out, out_sem.at[3]).start()

    wait_recv(hrecv.at[0], 4)
    wait_recv(hrecv.at[1], 5)
    inner = dot(r_v[...], hrecv[...].reshape(512, HID), 1, 1)
    masked = inner * one_v[...].astype(F32)
    gather_e = ones_where(iota((512, 64), 1) == 4 * ((iota((512, 64), 0) % 256) // 16) + 2 * (iota((512, 64), 0) // 256)
                          + (iota((512, 64), 0) % 16) // 8)
    ds = 0.0
    for term in split3(masked):
        ds = ds + dot(term, gather_e)
    ds = ds * scale
    probs = probs_v[...]
    dlog = (probs * (ds - jnp.sum(probs * ds, axis=1, keepdims=True))).astype(BF)
    dlog_v[...] = dlog
    dlog_t = dlog.astype(F32).T.astype(BF)
    for c in range(NCH):
        part = dot(dlog_t, x_v[:, c * CH:(c + 1) * CH])
        for i in range(CH // 128):
            ggpart[c // 2, (c % 2) * (CH // 128) + i] = part[:, i * 128:(i + 1) * 128]
    push(ggpart.at[1 - core], ggpair, twin, 8).start()
    cp_dlog = pltpu.make_async_copy(dlog_v, dlog_out, out_sem.at[10])
    cp_dlog.start()
    cp_one = pltpu.make_async_copy(one_v, one_out, out_sem.at[11])
    cp_one.start()
    push(ggpart.at[1 - core], ggpair, twin, 8).wait_recv()
    gghalf[...] = ggpart[core] + ggpair[...]
    for p in others:
        push(gghalf.at[p // 2], ggrecv.at[chip], p, 10).start()
    ggrecv[pl.ds(chip, 1)] = gghalf[pl.ds(chip, 1)]
    send_now(1)

    wait_send(xsend, 1)

    def ystep(c, acc):
        cols = pl.ds(pl.multiple_of(c * CH, CH), CH)
        h = hrecv[:, :, :, cols].reshape(512, CH)
        tot = x_v[:, cols].astype(F32) + (dot(c_v[0], h) + dot(c_v[1], h) + dot(c_v[2], h))
        y = tot.astype(BF)
        xsend[:, :, cols] = y.reshape(N, 16, CH)
        return acc + jnp.sum(y.astype(F32) * r_v[:, cols].astype(F32), axis=0, keepdims=True)
    losssend[...] = lax.fori_loop(0, NCH, ystep, jnp.zeros((1, CH), F32))
    cp_y = pltpu.make_async_copy(xsend, y_out, out_sem.at[4])
    cp_y.start()
    for p in peers:
        push(losssend, lossall.at[me], p, 9).start()
    lossall[pl.ds(me, 1)] = losssend[...].reshape(1, 1, CH)

    wait_recv(ggrecv, 10, 7)
    total = ggrecv[0]
    for i in range(1, 8):
        total = total + ggrecv[i]
    ggall[core, pl.ds(chip, 1)] = total.reshape(1, 64, 128)
    for p in others:
        push(ggall.at[core, chip], ggall.at[core, chip], p, 11).start()
    wait_recv(lossall, 9)
    loss_out[0, 0] = jnp.sum(lossall[...]) * scale
    wait_recv(ggall.at[core], 11, 7)
    across = push(ggall.at[core], ggall.at[core], twin, 12)
    across.start()
    across.wait_recv()
    cp_gg = [pltpu.make_async_copy(ggall.at[i // 8, i % 8], gg_out.at[:, pl.ds(i * 128, 128)], out_sem.at[6]) for i in range(N)]
    for cp in cp_gg:
        cp.start()
    for c in range(NOW):
        cols = pl.ds(c * CH, CH)
        part = gnow_out.at[pl.ds(0, N - 1), :, cols]
        pltpu.make_async_copy(part, part, recv_sem.at[6 + c]).wait()

    wait_send(selall, 0)
    wait_send(gates_all, 2)
    wait_send(hsend.at[0], 4)
    wait_send(hsend.at[1], 5)
    for c in range(NOW):
        cols = pl.ds(c * CH, CH)
        part = gsend.at[1, pl.ds(0, N - 1), :, cols]
        pltpu.make_async_copy(part, part, send_sem.at[6 + c]).wait()
        pltpu.make_async_copy(gsend.at[1, me, :, cols], gnow_out.at[me, :, cols], out_sem.at[7 + c]).wait()
    wait_send(rsend, 3)
    wait_send(lossall, 9)
    push(ggpart.at[1 - core], ggpair, twin, 8).wait_send()
    wait_send(gghalf, 10, 7)
    wait_send(ggall.at[core], 11, 7)
    across.wait_send()
    for cp in later:
        cp.wait()
    cp_dlog.wait()
    cp_one.wait()
    pltpu.make_async_copy(xl_v, xl_out, out_sem.at[0]).wait()
    pltpu.make_async_copy(u_v, u_out, out_sem.at[1]).wait()
    pltpu.make_async_copy(dh_v, dh_out, out_sem.at[2]).wait()
    pltpu.make_async_copy(da_v, da_out, out_sem.at[3]).wait()
    cp_y.wait()
    for cp in cp_gg:
        cp.wait()


def comm_call(sel, x, gw, up, dn, r, scale):
    any_ = pl.BlockSpec(memory_space=pl.ANY)
    vmem = pl.BlockSpec(memory_space=pltpu.VMEM)
    V = pltpu.VMEM
    shape = jax.ShapeDtypeStruct
    return pl.pallas_call(
        functools.partial(comm_kernel, scale),
        out_shape=[shape((N, 16, HID), BF), shape((N, 16, NOW * CH), BF), shape((N, 16, 2 * HID - NOW * CH), BF), shape((TOK, 512), BF),
                   shape((TOK, 64), BF), shape((64, HID), F32), shape((1, 1), F32),
                   shape((LE, CAP, HID), BF), shape((LE, CAP, FF), BF), shape((LE, CAP, HID), BF), shape((LE, CAP, FF), BF)],
        in_specs=[vmem, any_, any_, any_, any_, any_],
        out_specs=[any_, any_, any_, any_, any_, any_, pl.BlockSpec(memory_space=pltpu.SMEM), any_, any_, any_, any_],
        scratch_shapes=[
            V((TOK, HID), BF), V((TOK, HID), BF), V((64, HID), BF),
            V((3, HID, FF), BF), V((3, FF, HID), BF),
            V((N, 16, HID), BF), V((N, 16, HID), BF), V((N, 16, HID), BF), V((N, 16, HID), BF),
            V((2, N, 16, HID), BF), V((2, N, 16, HID), BF), V((2, N, 16, HID), BF),
            V((LE, CAP, HID), BF), V((LE, CAP, HID), BF), V((LE, CAP, FF), BF), V((LE, CAP, FF), F32), V((LE, CAP, FF), BF),
            V((2, 8, 64, 128), F32), V((8, 64, 128), F32), V((8, 64, 128), F32), V((8, 64, 128), F32), V((2, 8, 64, 128), F32),
            V((8, CAP), jnp.int32), V((N, 8, CAP), jnp.int32), V((1, 512), F32), V((N, 1, 512), F32),
            V((1, CH), F32), V((N, 1, CH), F32),
            V((TOK, 512), BF), V((3, TOK, 512), BF), V((LE, CAP, TOK), BF), V((TOK, 64), F32), V((TOK, 64), BF),
            pltpu.SemaphoreType.DMA((3,)), pltpu.SemaphoreType.DMA((2, 3)), pltpu.SemaphoreType.DMA((12,)),
            pltpu.SemaphoreType.DMA((13,)), pltpu.SemaphoreType.DMA((13,)),
        ],
        compiler_params=pltpu.CompilerParams(collective_id=0, has_side_effects=True, vmem_limit_bytes=67043328),
        name='exchange',
    )(sel, x, gw, up, dn, r)


def wgrad_kernel(xl_in, u_in, dh_in, da_in, y_in, gg_in, loss_in, g1, g2, y, gg, loss,
                 xl_v, u_v, dh_v, da_v, y_v, gg_v, t1, t2, in_sem, out_sem):
    def loads(e):
        return [pltpu.make_async_copy(src.at[e], dst.at[e], in_sem.at[e])
                for src, dst in ((xl_in, xl_v), (da_in, da_v), (u_in, u_v), (dh_in, dh_v))]

    def stores(i):
        e, c = i // NCH, i % NCH
        cols = pl.ds(pl.multiple_of(c * CH, CH), CH)
        return [pltpu.make_async_copy(t1.at[i], g1.at[e, cols, :], out_sem.at[0]),
                pltpu.make_async_copy(t2.at[i], g2.at[e, :, cols], out_sem.at[1])]

    for e in range(LE):
        for cp in loads(e):
            cp.start()
    cp_y = pltpu.make_async_copy(y_in, y_v, in_sem.at[LE])
    cp_gg = pltpu.make_async_copy(gg_in, gg_v, in_sem.at[LE + 1])
    cp_y.start()
    cp_gg.start()
    loss[0, 0] = loss_in[0, 0]

    def step(i, carry):
        e, c = i // NCH, i % NCH

        @pl.when(c == 0)
        def _():
            for cp in loads(e):
                cp.wait()
        cols = pl.ds(pl.multiple_of(c * CH, CH), CH)
        t1[i] = dot(xl_v[e, :, cols], da_v[e], 0, 0).astype(BF)
        t2[i] = dot(u_v[e], dh_v[e, :, cols], 0, 0).astype(BF)
        for cp in stores(i):
            cp.start()
        return carry
    lax.fori_loop(0, LE * NCH, step, 0)
    cp_y.wait()
    cp_gg.wait()
    out_y = pltpu.make_async_copy(y_v, y, in_sem.at[LE])
    out_gg = pltpu.make_async_copy(gg_v, gg, in_sem.at[LE + 1])
    out_y.start()
    out_gg.start()
    out_y.wait()
    out_gg.wait()

    def finish(i, carry):
        for cp in stores(i):
            cp.wait()
        return carry
    lax.fori_loop(0, LE * NCH, finish, 0)


def wgrad_call(xl, u, dh, da, y, gg, loss):
    shape = jax.ShapeDtypeStruct
    any_ = pl.BlockSpec(memory_space=pl.ANY)
    smem = pl.BlockSpec(memory_space=pltpu.SMEM)
    V = pltpu.VMEM
    return pl.pallas_call(
        wgrad_kernel,
        in_specs=[any_] * 6 + [smem],
        out_specs=[any_] * 4 + [smem],
        out_shape=[shape((LE, HID, FF), BF), shape((LE, FF, HID), BF), shape((N, 16, HID), BF), shape((64, HID), F32), shape((1, 1), F32)],
        scratch_shapes=[V((LE, CAP, HID), BF), V((LE, CAP, FF), BF), V((LE, CAP, HID), BF), V((LE, CAP, FF), BF),
                        V((N, 16, HID), BF), V((64, HID), F32), V((LE * NCH, CH, FF), BF), V((LE * NCH, FF, CH), BF),
                        pltpu.SemaphoreType.DMA((LE + 2,)), pltpu.SemaphoreType.DMA((2,))],
        compiler_params=pltpu.CompilerParams(vmem_limit_bytes=67043328),
        cost_estimate=pl.CostEstimate(flops=4 * LE * CAP * HID * FF, bytes_accessed=64 * 1024 * 1024, transcendentals=0),
        name='weight_grads',
    )(xl, u, dh, da, y, gg, loss)


def gradx_kernel(scale, r, one, dlog, gw, g_first, g_now, g_late, gx):
    tot = r[...].astype(F32) * scale + dot(one[:, :256], g_first[...].reshape(256, CH))
    tot = tot + dot(dlog[...], gw[...])

    @pl.when(pl.program_id(0) < NOW)
    def _():
        gx[...] = (tot + dot(one[:, 256:], g_now[...].reshape(256, CH))).astype(BF)

    @pl.when(pl.program_id(0) >= NOW)
    def _():
        gx[...] = (tot + dot(one[:, 256:], g_late[...].reshape(256, CH))).astype(BF)


def gradx_call(r, one, dlog, gw, now, later, scale):
    whole = lambda c: (0, 0)
    return pl.pallas_call(
        functools.partial(gradx_kernel, scale),
        grid=(NCH,),
        in_specs=[pl.BlockSpec((TOK, CH), lambda c: (0, c)), pl.BlockSpec((TOK, 512), whole), pl.BlockSpec((TOK, 64), whole),
                  pl.BlockSpec((64, CH), lambda c: (0, c)),
                  pl.BlockSpec((N, 16, CH), lambda c: (0, 0, c)),
                  pl.BlockSpec((N, 16, CH), lambda c: (0, 0, jnp.minimum(c, NOW - 1))),
                  pl.BlockSpec((N, 16, CH), lambda c: (0, 0, NCH + jnp.maximum(c - NOW, 0)))],
        out_specs=pl.BlockSpec((TOK, CH), lambda c: (0, c)),
        out_shape=jax.ShapeDtypeStruct((TOK, HID), BF),
        name='grad_x',
    )(r, one, dlog, gw, later, now, later)


def solution(mesh):
    def device_step(x, gate_w, up_w, down_w, expert_picks, loss_w):
        scale = 1.0 / math.sqrt(TOK * N * HID)
        gate_t = gate_w.T
        y, now, later, one, dlog, gg, loss, xl, u, dh, da = comm_call(expert_picks, x, gate_t, up_w, down_w, loss_w, scale)
        later = lax.all_to_all(later, 'ep', 0, 0, tiled=True)
        grad_up, grad_down, y, gg, loss = wgrad_call(xl, u, dh, da, y, gg, loss)
        grad_x = gradx_call(loss_w, one, dlog, gate_t, now, later, scale)
        return y.reshape(TOK, HID), loss[0, 0], grad_x, grad_up, grad_down, gg.T

    return jax.shard_map(device_step, mesh=mesh,
                         in_specs=(P('ep'), P(), P('ep'), P('ep'), P('ep'), P('ep')),
                         out_specs=(P('ep'), P(), P('ep'), P('ep'), P('ep'), P()),
                         check_vma=False)
```

```python
import functools
import math
import jax
import jax.numpy as jnp
from jax import lax
from jax.experimental import pallas as pl
from jax.experimental.pallas import tpu as pltpu
from jax.sharding import PartitionSpec as P

BF = jnp.bfloat16
F32 = jnp.float32
MESH = pl.DeviceIdType.MESH
N = 16
TOK = 256
LE = 4
CAP = 128
HID = 2048
FF = 1408
CH = 512
NCH = HID // CH
FIRST = 3
NOW = 4
ORDER = (14, 15, 6, 10, 12, 7, 11, 13, 2, 4, 8, 3, 5, 9, 1)


def dot(a, b, ca=1, cb=0):
    return lax.dot_general(a, b, (((ca,), (cb,)), ((), ())), preferred_element_type=F32)


def iota(shape, dim):
    return lax.broadcasted_iota(jnp.int32, shape, dim)


def ones_where(cond):
    return jnp.where(cond, 1.0, 0.0).astype(BF)


def split3(v):
    hi = v.astype(BF)
    rest = v - hi.astype(F32)
    mid = rest.astype(BF)
    low = (rest - mid.astype(F32)).astype(BF)
    return hi, mid, low


def flip(me, k):
    out = 0
    for b in range(4):
        bit = (me // (1 << b)) % 2
        if (k >> b) & 1:
            bit = 1 - bit
        out = out + bit * (1 << b)
    return out


def comm_kernel(scale, sel_ref, x_hbm, gw_hbm, up_hbm, dn_hbm, r_hbm,
                y_out, gnow_out, glater_out, one_out, dlog_out, gg_out, loss_out, xl_out, u_out, dh_out, da_out,
                x_v, r_v, gw_v, w1, w2, xsend, rsend, xrecv, rrecv, hsend, hrecv, gsend,
                xl_v, dh_v, u_v, gp_v, da_v, ggpart, ggpair, gghalf, ggrecv, ggall, selsend, selall, gates, gates_all,
                losssend, lossall, one_v, c_v, e_v, probs_v, dlog_v,
                ld_sem, w_sem, out_sem, send_sem, recv_sem):
    me = lax.axis_index('ep')
    peers = [flip(me, k) for k in ORDER]
    core, chip, twin = me % 2, me // 2, flip(me, 1)
    others = [flip(me, k) for k in ORDER if k % 2 == 0]

    def load(src, dst, i):
        return pltpu.make_async_copy(src, dst, ld_sem.at[i])

    def weight1(e, slot):
        return pltpu.make_async_copy(up_hbm.at[e], w1.at[slot], w_sem.at[0, slot])

    def weight2(e, slot):
        return pltpu.make_async_copy(dn_hbm.at[e], w2.at[slot], w_sem.at[1, slot])

    def push(src, dst, peer, i):
        return pltpu.make_async_remote_copy(src_ref=src, dst_ref=dst, send_sem=send_sem.at[i], recv_sem=recv_sem.at[i],
                                            device_id=(peer,), device_id_type=MESH)

    def wait_recv(buf, i, n=N - 1):
        part = buf.at[pl.ds(0, n)]
        pltpu.make_async_copy(part, part, recv_sem.at[i]).wait()

    def wait_send(buf, i, n=N - 1):
        part = buf.at[pl.ds(0, n)]
        pltpu.make_async_copy(part, part, send_sem.at[i]).wait()

    cp_x = load(x_hbm, x_v, 0)
    cp_g = load(gw_hbm, gw_v, 1)
    cp_r = load(r_hbm, r_v, 2)
    cp_x.start()
    cp_g.start()
    cp_r.start()

    sel = sel_ref[...]
    selsend[...] = jnp.zeros_like(selsend)
    selsend[0:LE, :] = sel
    selall[pl.ds(me, 1)] = selsend[...].reshape(1, 8, CAP)

    barrier = pltpu.get_barrier_semaphore()
    for p in peers:
        pl.semaphore_signal(barrier, inc=1, device_id=(p,), device_id_type=MESH)
    pl.semaphore_wait(barrier, N - 1)

    for p in peers:
        push(selsend, selall.at[me], p, 0).start()
    for e in range(3):
        weight1(e, e).start()
        weight2(e, e).start()

    cp_g.wait()
    cp_x.wait()
    logits = dot(x_v[...], gw_v[...], 1, 1)
    ex = jnp.exp(logits - jnp.max(logits, axis=1, keepdims=True))
    probs = ex / jnp.sum(ex, axis=1, keepdims=True)
    probs_v[...] = probs

    below = ones_where(iota((TOK, TOK), 1) < iota((TOK, TOK), 0))
    slot_lane = (iota((TOK, TOK), 1) % 16).astype(F32)

    tok_row = iota((TOK, CAP), 0)
    same = iota((CAP, TOK), 0) // 8 == iota((CAP, TOK), 1) // 16
    fold = ones_where(same)
    base = (iota((1, CAP), 1) // 8) * TOK
    hits = [ones_where(tok_row == sel[l:l + 1, :] - base) for l in range(LE)]
    count = dot(hits[0], fold)
    for l in range(1, LE):
        count = count + dot(hits[l], fold)
    pres = count > 0.5
    rank = dot(below, ones_where(pres))
    pick_of = jnp.where(pres, jnp.where(rank == slot_lane, 1.0, 0.0), 0.0).astype(BF)
    for l in range(LE):
        e_v[l] = jnp.where(same, dot(hits[l], pick_of, 0, 0), 0.0).astype(BF)

    for_wait = selall.at[pl.ds(0, N - 1)]
    pltpu.make_async_copy(for_wait, for_wait, recv_sem.at[0]).wait()
    everyone = selall[...].reshape(8 * N, CAP)
    mine = jnp.where(iota((8 * N, CAP), 1) // 8 == me, everyone - me * TOK, 0).astype(F32).astype(BF)
    place = ones_where(iota((CAP, 512), 0) % 8 == iota((CAP, 512), 1) % 8)
    spread = dot(mine, place)
    lane = iota((8 * N, 512), 1)
    want = ((lane % 256) // 16) * 8 + 2 * (lane // 256) + (lane % 16) // 8
    ids = jnp.sum(jnp.where(iota((8 * N, 512), 0) == want, spread, 0.0), axis=0, keepdims=True)
    one = jnp.where(iota((TOK, 512), 0).astype(F32) == ids, 1.0, 0.0)
    one_v[...] = one.astype(BF)
    fold2 = ones_where((iota((512, TOK), 0) % 256) // 16 == iota((512, TOK), 1) // 16)
    pres2 = dot(one_v[...], fold2) > 0.5
    rank2 = dot(below, ones_where(pres2))
    give = jnp.where(pres2, jnp.where(rank2 == slot_lane, 1.0, 0.0), 0.0).astype(BF)
    give_t = give.T

    def gather(src, dst):
        def step(c, carry):
            cols = pl.ds(pl.multiple_of(c * CH, CH), CH)
            dst[:, :, cols] = dot(give_t, src[:, cols]).astype(BF).reshape(N, 16, CH)
            return carry
        lax.fori_loop(0, NCH, step, 0)

    gather(x_v, xsend)
    for p in peers:
        push(xsend.at[p], xrecv.at[me], p, 1).start()
    xrecv[pl.ds(me, 1)] = xsend[pl.ds(me, 1)]

    rep = ones_where(iota((64, 512), 0) == 4 * ((iota((64, 512), 1) % 256) // 16) + 2 * (iota((64, 512), 1) // 256)
                     + (iota((64, 512), 1) % 16) // 8)
    wide = 0.0
    for term in split3(probs_v[...]):
        wide = wide + dot(term, rep)
    comb = wide * one
    for i, term in enumerate(split3(comb)):
        c_v[i] = term
    gates[...] = jnp.sum(comb, axis=0, keepdims=True)
    for p in peers:
        push(gates, gates_all.at[me], p, 2).start()
    gates_all[pl.ds(me, 1)] = gates[...].reshape(1, 1, 512)

    cp_r.wait()
    gather(r_v, rsend)
    for p in peers:
        push(rsend.at[p], rrecv.at[me], p, 3).start()
    rrecv[pl.ds(me, 1)] = rsend[pl.ds(me, 1)]

    wait_recv(xrecv, 1)

    def fwd(q, carry):
        for j in range(2):
            e = 2 * q + j
            slot = e % 3
            xl = dot(e_v[e], xrecv[...].reshape(TOK, HID)).astype(BF)
            xl_v[e] = xl
            weight1(e, slot).wait()
            a = dot(xl_v[e], w1[slot])
            if j == 0:
                @pl.when(q == 0)
                def _():
                    weight1(3, 0).start()
            k0 = math.sqrt(2.0 / math.pi)
            t = jnp.tanh(k0 * (a + 0.044715 * (a * a * a)))
            u_v[e] = (0.5 * a * (1.0 + t)).astype(BF)
            gp_v[e] = 0.5 * (1.0 + t) + 0.5 * a * (1.0 - t * t) * (k0 * (1.0 + 3.0 * 0.044715 * (a * a)))
        weight2(2 * q, (2 * q) % 3).wait()
        weight2(2 * q + 1, (2 * q + 1) % 3).wait()

        def step(c, carry):
            cols = pl.ds(pl.multiple_of(c * CH, CH), CH)
            outs = [dot(u_v[2 * q + j], w2[(2 * q + j) % 3, :, cols]).reshape(N, 8, CH) for j in range(2)]
            hsend[q, :, :, cols] = jnp.concatenate(outs, axis=1).astype(BF)
            return carry
        lax.fori_loop(0, NCH, step, 0)

        @pl.when(q == 0)
        def _():
            weight2(3, 0).start()
        for p in peers:
            push(hsend.at[q, p], hrecv.at[q, me], p, 4 + q).start()
        hrecv[q, pl.ds(me, 1)] = hsend[q, pl.ds(me, 1)]
        return carry
    lax.fori_loop(0, 2, fwd, 0)
    pltpu.make_async_copy(xl_v, xl_out, out_sem.at[0]).start()
    pltpu.make_async_copy(u_v, u_out, out_sem.at[1]).start()

    wait_recv(gates_all, 2)
    wait_recv(rrecv, 3)

    def send_now(c):
        cols = pl.ds(c * CH, CH)
        for p in peers:
            push(gsend.at[1, p, :, cols], gnow_out.at[me, :, cols], p, 13 + c).start()
        pltpu.make_async_copy(gsend.at[1, me, :, cols], gnow_out.at[me, :, cols], out_sem.at[12 + c]).start()

    def bwd(q, carry):
        for j in range(2):
            e = 2 * (1 - q) + j
            slot = (1 - q) * (2 - 2 * j) + q * (2 - j)
            if j == 0:
                @pl.when(q == 1)
                def _():
                    weight1(0, 2).wait()
                    weight2(0, 2).wait()
            rows = jnp.broadcast_to(gates_all[...], (N, 8, 512)).reshape(CAP, 512)
            here = iota((CAP, 512), 1) == (1 - q) * 256 + me * 16 + j * 8 + iota((CAP, 512), 0) % 8
            gcol = jnp.sum(jnp.where(here, rows, 0.0), axis=1, keepdims=True)

            def rstep(c, carry):
                cols = pl.ds(pl.multiple_of(c * CH, CH), CH)
                rl = dot(e_v[e], rrecv[:, :, cols].reshape(TOK, CH))
                dh_v[e, :, cols] = (gcol * (rl * scale)).astype(BF)
                return carry
            lax.fori_loop(0, NCH, rstep, 0)
            du = dot(dh_v[e], w2[slot], 1, 1).astype(BF).astype(F32)
            if j == 0:
                @pl.when(q == 0)
                def _():
                    weight2(0, 2).start()
            da_v[e] = (gp_v[e] * du).astype(BF)

        def step(c, carry):
            cols = pl.ds(pl.multiple_of(c * CH, CH), CH)
            outs = []
            for j in range(2):
                slot = (1 - q) * (2 - 2 * j) + q * (2 - j)
                outs.append(dot(da_v[2 * (1 - q) + j], w1[slot, cols, :], 1, 1).reshape(N, 8, CH))
            gsend[1 - q, :, :, cols] = jnp.concatenate(outs, axis=1).astype(BF)
            return carry
        lax.fori_loop(0, NCH, step, 0)

        @pl.when(q == 0)
        def _():
            weight1(0, 2).start()
        @pl.when(q == 0)
        def _():
            send_now(0)
        return carry
    lax.fori_loop(0, 2, bwd, 0)
    later = [pltpu.make_async_copy(gsend.at[0], glater_out.at[:, :, pl.ds(0, HID)], out_sem.at[5])]
    if NOW < NCH:
        later.append(pltpu.make_async_copy(gsend.at[1, :, :, pl.ds(NOW * CH, HID - NOW * CH)],
                                           glater_out.at[:, :, pl.ds(HID, HID - NOW * CH)], out_sem.at[9]))
    for cp in later:
        cp.start()
    pltpu.make_async_copy(dh_v, dh_out, out_sem.at[2]).start()
    pltpu.make_async_copy(da_v, da_out, out_sem.at[3]).start()

    wait_recv(hrecv.at[0], 4)
    wait_recv(hrecv.at[1], 5)
    inner = dot(r_v[...], hrecv[...].reshape(512, HID), 1, 1)
    masked = inner * one_v[...].astype(F32)
    gather_e = ones_where(iota((512, 64), 1) == 4 * ((iota((512, 64), 0) % 256) // 16) + 2 * (iota((512, 64), 0) // 256)
                          + (iota((512, 64), 0) % 16) // 8)
    ds = 0.0
    for term in split3(masked):
        ds = ds + dot(term, gather_e)
    ds = ds * scale
    probs = probs_v[...]
    dlog = (probs * (ds - jnp.sum(probs * ds, axis=1, keepdims=True))).astype(BF)
    dlog_v[...] = dlog
    dlog_t = dlog.astype(F32).T.astype(BF)
    for c in range(NCH):
        part = dot(dlog_t, x_v[:, c * CH:(c + 1) * CH])
        for i in range(CH // 128):
            ggpart[c // 2, (c % 2) * (CH // 128) + i] = part[:, i * 128:(i + 1) * 128]
    push(ggpart.at[1 - core], ggpair, twin, 8).start()
    cp_dlog = pltpu.make_async_copy(dlog_v, dlog_out, out_sem.at[10])
    cp_dlog.start()
    cp_one = pltpu.make_async_copy(one_v, one_out, out_sem.at[11])
    cp_one.start()
    push(ggpart.at[1 - core], ggpair, twin, 8).wait_recv()
    gghalf[...] = ggpart[core] + ggpair[...]
    for p in others:
        push(gghalf.at[p // 2], ggrecv.at[chip], p, 10).start()
    ggrecv[pl.ds(chip, 1)] = gghalf[pl.ds(chip, 1)]
    send_now(1)

    wait_send(xsend, 1)

    def ystep(c, acc):
        cols = pl.ds(pl.multiple_of(c * CH, CH), CH)
        h = hrecv[:, :, :, cols].reshape(512, CH)
        tot = x_v[:, cols].astype(F32) + (dot(c_v[0], h) + dot(c_v[1], h) + dot(c_v[2], h))
        y = tot.astype(BF)
        xsend[:, :, cols] = y.reshape(N, 16, CH)
        return acc + jnp.sum(y.astype(F32) * r_v[:, cols].astype(F32), axis=0, keepdims=True)
    losssend[...] = lax.fori_loop(0, NCH, ystep, jnp.zeros((1, CH), F32))
    cp_y = pltpu.make_async_copy(xsend, y_out, out_sem.at[4])
    cp_y.start()
    for p in peers:
        push(losssend, lossall.at[me], p, 9).start()
    lossall[pl.ds(me, 1)] = losssend[...].reshape(1, 1, CH)

    wait_recv(ggrecv, 10, 7)
    total = ggrecv[0]
    for i in range(1, 8):
        total = total + ggrecv[i]
    ggall[core, pl.ds(chip, 1)] = total.reshape(1, 64, 128)
    for p in others:
        push(ggall.at[core, chip], ggall.at[core, chip], p, 11).start()
    for c in range(2, NOW):
        send_now(c)
    wait_recv(lossall, 9)
    loss_out[0, 0] = jnp.sum(lossall[...]) * scale
    wait_recv(ggall.at[core], 11, 7)
    across = push(ggall.at[core], ggall.at[core], twin, 12)
    across.start()
    across.wait_recv()
    cp_gg = [pltpu.make_async_copy(ggall.at[i // 8, i % 8], gg_out.at[:, pl.ds(i * 128, 128)], out_sem.at[6]) for i in range(N)]
    for cp in cp_gg:
        cp.start()
    for c in range(NOW):
        cols = pl.ds(c * CH, CH)
        part = gnow_out.at[pl.ds(0, N - 1), :, cols]
        pltpu.make_async_copy(part, part, recv_sem.at[13 + c]).wait()

    wait_send(selall, 0)
    wait_send(gates_all, 2)
    wait_send(hsend.at[0], 4)
    wait_send(hsend.at[1], 5)
    for c in range(NOW):
        cols = pl.ds(c * CH, CH)
        part = gsend.at[1, pl.ds(0, N - 1), :, cols]
        pltpu.make_async_copy(part, part, send_sem.at[13 + c]).wait()
        pltpu.make_async_copy(gsend.at[1, me, :, cols], gnow_out.at[me, :, cols], out_sem.at[12 + c]).wait()
    wait_send(rsend, 3)
    wait_send(lossall, 9)
    push(ggpart.at[1 - core], ggpair, twin, 8).wait_send()
    wait_send(gghalf, 10, 7)
    wait_send(ggall.at[core], 11, 7)
    across.wait_send()
    for cp in later:
        cp.wait()
    cp_dlog.wait()
    cp_one.wait()
    pltpu.make_async_copy(xl_v, xl_out, out_sem.at[0]).wait()
    pltpu.make_async_copy(u_v, u_out, out_sem.at[1]).wait()
    pltpu.make_async_copy(dh_v, dh_out, out_sem.at[2]).wait()
    pltpu.make_async_copy(da_v, da_out, out_sem.at[3]).wait()
    cp_y.wait()
    for cp in cp_gg:
        cp.wait()


def comm_call(sel, x, gw, up, dn, r, scale):
    any_ = pl.BlockSpec(memory_space=pl.ANY)
    vmem = pl.BlockSpec(memory_space=pltpu.VMEM)
    V = pltpu.VMEM
    shape = jax.ShapeDtypeStruct
    return pl.pallas_call(
        functools.partial(comm_kernel, scale),
        out_shape=[shape((N, 16, HID), BF), shape((N, 16, NOW * CH), BF), shape((N, 16, 2 * HID - NOW * CH), BF), shape((TOK, 512), BF),
                   shape((TOK, 64), BF), shape((64, HID), F32), shape((1, 1), F32),
                   shape((LE, CAP, HID), BF), shape((LE, CAP, FF), BF), shape((LE, CAP, HID), BF), shape((LE, CAP, FF), BF)],
        in_specs=[vmem, any_, any_, any_, any_, any_],
        out_specs=[any_, any_, any_, any_, any_, any_, pl.BlockSpec(memory_space=pltpu.SMEM), any_, any_, any_, any_],
        scratch_shapes=[
            V((TOK, HID), BF), V((TOK, HID), BF), V((64, HID), BF),
            V((3, HID, FF), BF), V((3, FF, HID), BF),
            V((N, 16, HID), BF), V((N, 16, HID), BF), V((N, 16, HID), BF), V((N, 16, HID), BF),
            V((2, N, 16, HID), BF), V((2, N, 16, HID), BF), V((2, N, 16, HID), BF),
            V((LE, CAP, HID), BF), V((LE, CAP, HID), BF), V((LE, CAP, FF), BF), V((LE, CAP, FF), F32), V((LE, CAP, FF), BF),
            V((2, 8, 64, 128), F32), V((8, 64, 128), F32), V((8, 64, 128), F32), V((8, 64, 128), F32), V((2, 8, 64, 128), F32),
            V((8, CAP), jnp.int32), V((N, 8, CAP), jnp.int32), V((1, 512), F32), V((N, 1, 512), F32),
            V((1, CH), F32), V((N, 1, CH), F32),
            V((TOK, 512), BF), V((3, TOK, 512), BF), V((LE, CAP, TOK), BF), V((TOK, 64), F32), V((TOK, 64), BF),
            pltpu.SemaphoreType.DMA((3,)), pltpu.SemaphoreType.DMA((2, 3)), pltpu.SemaphoreType.DMA((16,)),
            pltpu.SemaphoreType.DMA((17,)), pltpu.SemaphoreType.DMA((17,)),
        ],
        compiler_params=pltpu.CompilerParams(collective_id=0, has_side_effects=True, vmem_limit_bytes=67043328),
        name='exchange',
    )(sel, x, gw, up, dn, r)


def tile_tools(ins, bufs, outs, tiles, in_sem, out_sem, first):
    def loads(e):
        return [pltpu.make_async_copy(src.at[e], dst.at[e - first], in_sem.at[e - first]) for src, dst in zip(ins, bufs)]

    def stores(i):
        e, c = i // NCH, i % NCH
        cols = pl.ds(pl.multiple_of(c * CH, CH), CH)
        return [pltpu.make_async_copy(tiles[0].at[i - first * NCH], outs[0].at[e, cols, :], out_sem.at[0]),
                pltpu.make_async_copy(tiles[1].at[i - first * NCH], outs[1].at[e, :, cols], out_sem.at[1])]

    def step(i, carry):
        e, c = i // NCH, i % NCH
        xl_v, da_v, u_v, dh_v = bufs
        cols = pl.ds(pl.multiple_of(c * CH, CH), CH)
        tiles[0][i - first * NCH] = dot(xl_v[e - first, :, cols], da_v[e - first], 0, 0).astype(BF)
        tiles[1][i - first * NCH] = dot(u_v[e - first], dh_v[e - first, :, cols], 0, 0).astype(BF)
        for cp in stores(i):
            cp.start()
        return carry

    def finish(i, carry):
        for cp in stores(i):
            cp.wait()
        return carry
    return loads, step, finish


def wgrad1_kernel(xl_in, da_in, u_in, dh_in, y_in, gg_in, loss_in, g1, g2, y, gg, loss,
                  xl_v, da_v, u_v, dh_v, y_v, gg_v, t1, t2, in_sem, out_sem):
    loads, step, finish = tile_tools((xl_in, da_in, u_in, dh_in), (xl_v, da_v, u_v, dh_v), (g1, g2), (t1, t2), in_sem, out_sem, 0)
    cp_y = pltpu.make_async_copy(y_in, y_v, in_sem.at[LE])
    cp_gg = pltpu.make_async_copy(gg_in, gg_v, in_sem.at[LE + 1])
    for cp in loads(0):
        cp.start()
    loss[0, 0] = loss_in[0, 0]

    def expert(e, carry):
        for cp in loads(e):
            cp.wait()

        @pl.when(e + 1 < FIRST)
        def _():
            for cp in loads(e + 1):
                cp.start()

        @pl.when(e == 0)
        def _():
            cp_y.start()
            cp_gg.start()
        lax.fori_loop(e * NCH, (e + 1) * NCH, step, 0)
        return carry
    lax.fori_loop(0, FIRST, expert, 0)
    cp_y.wait()
    cp_gg.wait()
    out_y = pltpu.make_async_copy(y_v, y, in_sem.at[LE])
    out_gg = pltpu.make_async_copy(gg_v, gg, in_sem.at[LE + 1])
    out_y.start()
    out_gg.start()
    out_y.wait()
    out_gg.wait()
    lax.fori_loop(0, FIRST * NCH, finish, 0)


def wgrad1_call(xl, da, u, dh, y, gg, loss):
    shape = jax.ShapeDtypeStruct
    any_ = pl.BlockSpec(memory_space=pl.ANY)
    smem = pl.BlockSpec(memory_space=pltpu.SMEM)
    V = pltpu.VMEM
    return pl.pallas_call(
        wgrad1_kernel,
        in_specs=[any_] * 6 + [smem],
        out_specs=[any_] * 4 + [smem],
        out_shape=[shape((LE, HID, FF), BF), shape((LE, FF, HID), BF), shape((N, 16, HID), BF), shape((64, HID), F32), shape((1, 1), F32)],
        scratch_shapes=[V((FIRST, CAP, HID), BF), V((FIRST, CAP, FF), BF), V((FIRST, CAP, FF), BF), V((FIRST, CAP, HID), BF),
                        V((N, 16, HID), BF), V((64, HID), F32), V((FIRST * NCH, CH, FF), BF), V((FIRST * NCH, FF, CH), BF),
                        pltpu.SemaphoreType.DMA((LE + 2,)), pltpu.SemaphoreType.DMA((2,))],
        compiler_params=pltpu.CompilerParams(vmem_limit_bytes=67043328),
        cost_estimate=pl.CostEstimate(flops=FIRST * 4 * CAP * HID * FF, bytes_accessed=48 * 1024 * 1024, transcendentals=0),
        name='weight_grads_a',
    )(xl, da, u, dh, y, gg, loss)


def wgrad2_kernel(scale, g1_in, g2_in, xl_in, da_in, u_in, dh_in, r_in, one_in, dlog_in, gw_in, now_in, late_in, g1, g2, gx,
                  xl_v, da_v, u_v, dh_v, r_v, one_v, dlog_v, gw_v, now_v, late_v, gx_v, t1, t2, in_sem, out_sem):
    rest = LE - FIRST
    loads, step, finish = tile_tools((xl_in, da_in, u_in, dh_in), (xl_v, da_v, u_v, dh_v), (g1, g2), (t1, t2), in_sem, out_sem, FIRST)
    for cp in loads(FIRST):
        cp.start()
    small = [pltpu.make_async_copy(src, dst, in_sem.at[rest]) for src, dst in
             ((r_in, r_v), (one_in, one_v), (dlog_in, dlog_v), (gw_in, gw_v), (now_in, now_v), (late_in, late_v))]
    for cp in small:
        cp.start()
    for e in range(FIRST, LE):
        for cp in loads(e):
            cp.wait()
        if e + 1 < LE:
            for cp in loads(e + 1):
                cp.start()
        lax.fori_loop(e * NCH, (e + 1) * NCH, step, 0)
        if e == FIRST:
            for cp in small:
                cp.wait()

            def gstep(c, carry):
                cols = pl.ds(pl.multiple_of(c * CH, CH), CH)
                tot = r_v[:, cols].astype(F32) * scale + dot(one_v[:, 0:256], late_v[:, :, cols].reshape(256, CH))
                tot = tot + dot(one_v[:, 256:512], now_v[:, :, cols].reshape(256, CH))
                gx_v[:, cols] = (tot + dot(dlog_v[...], gw_v[:, cols])).astype(BF)
                return carry
            lax.fori_loop(0, NCH, gstep, 0)
            pltpu.make_async_copy(gx_v, gx, in_sem.at[rest]).start()
    pltpu.make_async_copy(gx_v, gx, in_sem.at[rest]).wait()
    lax.fori_loop(FIRST * NCH, LE * NCH, finish, 0)


def wgrad2_call(g1, g2, xl, da, u, dh, r, one, dlog, gw, now, late, scale):
    shape = jax.ShapeDtypeStruct
    any_ = pl.BlockSpec(memory_space=pl.ANY)
    V = pltpu.VMEM
    rest = LE - FIRST
    return pl.pallas_call(
        functools.partial(wgrad2_kernel, scale),
        in_specs=[any_] * 12,
        out_specs=[any_] * 3,
        out_shape=[shape((LE, HID, FF), BF), shape((LE, FF, HID), BF), shape((TOK, HID), BF)],
        scratch_shapes=[V((rest, CAP, HID), BF), V((rest, CAP, FF), BF), V((rest, CAP, FF), BF), V((rest, CAP, HID), BF),
                        V((TOK, HID), BF), V((TOK, 512), BF), V((TOK, 64), BF), V((64, HID), BF), V((N, 16, HID), BF), V((N, 16, HID), BF),
                        V((TOK, HID), BF), V((rest * NCH, CH, FF), BF), V((rest * NCH, FF, CH), BF),
                        pltpu.SemaphoreType.DMA((rest + 1,)), pltpu.SemaphoreType.DMA((2,))],
        input_output_aliases={0: 0, 1: 1},
        compiler_params=pltpu.CompilerParams(vmem_limit_bytes=67043328),
        name='weight_grads_b',
    )(g1, g2, xl, da, u, dh, r, one, dlog, gw, now, late)


def solution(mesh):
    def device_step(x, gate_w, up_w, down_w, expert_picks, loss_w):
        scale = 1.0 / math.sqrt(TOK * N * HID)
        gate_t = gate_w.T
        y, now, later, one, dlog, gg, loss, xl, u, dh, da = comm_call(expert_picks, x, gate_t, up_w, down_w, loss_w, scale)
        later = lax.all_to_all(later, 'ep', 0, 0, tiled=True)
        grad_up, grad_down, y, gg, loss = wgrad1_call(xl, da, u, dh, y, gg, loss)
        grad_up, grad_down, grad_x = wgrad2_call(grad_up, grad_down, xl, da, u, dh, loss_w, one, dlog, gate_t, now, later, scale)
        return y.reshape(TOK, HID), loss[0, 0], grad_x, grad_up, grad_down, gg.T

    return jax.shard_map(device_step, mesh=mesh,
                         in_specs=(P('ep'), P(), P('ep'), P('ep'), P('ep'), P('ep')),
                         out_specs=(P('ep'), P(), P('ep'), P('ep'), P('ep'), P()),
                         check_vma=False)
```

```python
import functools
import math
import jax
import jax.numpy as jnp
from jax import lax
from jax.experimental import pallas as pl
from jax.experimental.pallas import tpu as pltpu
from jax.sharding import PartitionSpec as P

BF = jnp.bfloat16
F32 = jnp.float32
MESH = pl.DeviceIdType.MESH
N = 16
TOK = 256
LE = 4
CAP = 128
HID = 2048
FF = 1408
CH = 512
NCH = HID // CH
FIRST = 4
HALF = HID // 2
NOW = 2
ORDER = (14, 15, 6, 10, 12, 7, 11, 13, 2, 4, 8, 3, 5, 9, 1)


def dot(a, b, ca=1, cb=0):
    return lax.dot_general(a, b, (((ca,), (cb,)), ((), ())), preferred_element_type=F32)


def iota(shape, dim):
    return lax.broadcasted_iota(jnp.int32, shape, dim)


def ones_where(cond):
    return jnp.where(cond, 1.0, 0.0).astype(BF)


def split3(v):
    hi = v.astype(BF)
    rest = v - hi.astype(F32)
    mid = rest.astype(BF)
    low = (rest - mid.astype(F32)).astype(BF)
    return hi, mid, low


def flip(me, k):
    out = 0
    for b in range(4):
        bit = (me // (1 << b)) % 2
        if (k >> b) & 1:
            bit = 1 - bit
        out = out + bit * (1 << b)
    return out


def comm_kernel(scale, sel_ref, x_hbm, gw_hbm, up_hbm, dn_hbm, r_hbm,
                y_out, gnow_out, glater_out, one_out, dlog_out, gg_out, loss_out, xl_out, u_out, dh_out, da_out,
                x_v, r_v, gw_v, w1, w2, xsend, rsend, xrecv, rrecv, hsend, hrecv, gsend,
                xl_v, dh_v, u_v, gp_v, da_v, ggpart, ggpair, gghalf, ggrecv, ggall, selsend, selall, gates, gates_all,
                losssend, lossall, dgsend, dgall, one_v, c_v, e_v, probs_v, dlog_v,
                ld_sem, w_sem, out_sem, send_sem, recv_sem):
    open_ = []

    def phase(name):
        if open_:
            open_.pop().__exit__(None, None, None)
        if name:
            open_.append(jax.named_scope(name))
            open_[-1].__enter__()
    me = lax.axis_index('ep')
    peers = [flip(me, k) for k in ORDER]
    core, chip, twin = me % 2, me // 2, flip(me, 1)
    others = [flip(me, k) for k in ORDER if k % 2 == 0]

    def load(src, dst, i):
        return pltpu.make_async_copy(src, dst, ld_sem.at[i])

    def weight1(e, slot):
        return pltpu.make_async_copy(up_hbm.at[e], w1.at[slot], w_sem.at[0, slot])

    def weight2(e, slot):
        return pltpu.make_async_copy(dn_hbm.at[e], w2.at[slot], w_sem.at[1, slot])

    def push(src, dst, peer, i):
        return pltpu.make_async_remote_copy(src_ref=src, dst_ref=dst, send_sem=send_sem.at[i], recv_sem=recv_sem.at[i],
                                            device_id=(peer,), device_id_type=MESH)

    def wait_recv(buf, i, n=N - 1):
        part = buf.at[pl.ds(0, n)]
        pltpu.make_async_copy(part, part, recv_sem.at[i]).wait()

    def wait_send(buf, i, n=N - 1):
        part = buf.at[pl.ds(0, n)]
        pltpu.make_async_copy(part, part, send_sem.at[i]).wait()

    phase('p00_start')
    cp_x = load(x_hbm, x_v, 0)
    cp_g = load(gw_hbm, gw_v, 1)
    cp_r = load(r_hbm, r_v, 2)
    cp_x.start()
    cp_g.start()
    cp_r.start()

    sel = sel_ref[...]
    selsend[...] = jnp.zeros_like(selsend)
    selsend[0:LE, :] = sel
    selall[pl.ds(me, 1)] = selsend[...].reshape(1, 8, CAP)

    phase('p01_barrier')
    barrier = pltpu.get_barrier_semaphore()
    for p in peers:
        pl.semaphore_signal(barrier, inc=1, device_id=(p,), device_id_type=MESH)
    pl.semaphore_wait(barrier, N - 1)

    for p in peers:
        push(selsend, selall.at[me], p, 0).start()
    for e in range(3):
        weight1(e, e).start()
        weight2(e, e).start()

    phase('p02_logits')
    cp_g.wait()
    cp_x.wait()
    logits = dot(x_v[...], gw_v[...], 1, 1)
    ex = jnp.exp(logits - jnp.max(logits, axis=1, keepdims=True))
    probs = ex / jnp.sum(ex, axis=1, keepdims=True)
    probs_v[...] = probs

    phase('p03_ownpicks')
    below = ones_where(iota((TOK, TOK), 1) < iota((TOK, TOK), 0))
    slot_lane = (iota((TOK, TOK), 1) % 16).astype(F32)

    tok_row = iota((TOK, CAP), 0)
    same = iota((CAP, TOK), 0) // 8 == iota((CAP, TOK), 1) // 16
    fold = ones_where(same)
    base = (iota((1, CAP), 1) // 8) * TOK
    hits = [ones_where(tok_row == sel[l:l + 1, :] - base) for l in range(LE)]
    count = dot(hits[0], fold)
    for l in range(1, LE):
        count = count + dot(hits[l], fold)
    pres = count > 0.5
    rank = dot(below, ones_where(pres))
    pick_of = jnp.where(pres, jnp.where(rank == slot_lane, 1.0, 0.0), 0.0).astype(BF)
    for l in range(LE):
        e_v[l] = jnp.where(same, dot(hits[l], pick_of, 0, 0), 0.0).astype(BF)

    phase('p04_waitsel')
    for_wait = selall.at[pl.ds(0, N - 1)]
    pltpu.make_async_copy(for_wait, for_wait, recv_sem.at[0]).wait()
    phase('p05_give')
    everyone = selall[...].reshape(8 * N, CAP)
    mine = jnp.where(iota((8 * N, CAP), 1) // 8 == me, everyone - me * TOK, 0).astype(F32).astype(BF)
    place = ones_where(iota((CAP, 512), 0) % 8 == iota((CAP, 512), 1) % 8)
    spread = dot(mine, place)
    lane = iota((8 * N, 512), 1)
    want = ((lane % 256) // 16) * 8 + 2 * (lane // 256) + (lane % 16) // 8
    ids = jnp.sum(jnp.where(iota((8 * N, 512), 0) == want, spread, 0.0), axis=0, keepdims=True)
    one = jnp.where(iota((TOK, 512), 0).astype(F32) == ids, 1.0, 0.0)
    one_v[...] = one.astype(BF)
    fold2 = ones_where((iota((512, TOK), 0) % 256) // 16 == iota((512, TOK), 1) // 16)
    pres2 = dot(one_v[...], fold2) > 0.5
    rank2 = dot(below, ones_where(pres2))
    give = jnp.where(pres2, jnp.where(rank2 == slot_lane, 1.0, 0.0), 0.0).astype(BF)
    give_t = give.T

    def gather(src, dst):
        def step(c, carry):
            cols = pl.ds(pl.multiple_of(c * CH, CH), CH)
            dst[:, :, cols] = dot(give_t, src[:, cols]).astype(BF).reshape(N, 16, CH)
            return carry
        lax.fori_loop(0, NCH, step, 0)

    phase('p06_gatherx')
    gather(x_v, xsend)
    for p in peers:
        push(xsend.at[p], xrecv.at[me], p, 1).start()
    xrecv[pl.ds(me, 1)] = xsend[pl.ds(me, 1)]

    phase('p07_gates')
    rep = ones_where(iota((64, 512), 0) == 4 * ((iota((64, 512), 1) % 256) // 16) + 2 * (iota((64, 512), 1) // 256)
                     + (iota((64, 512), 1) % 16) // 8)
    wide = 0.0
    for term in split3(probs_v[...]):
        wide = wide + dot(term, rep)
    comb = wide * one
    for i, term in enumerate(split3(comb)):
        c_v[i] = term
    gates[...] = jnp.sum(comb, axis=0, keepdims=True)
    for p in peers:
        push(gates, gates_all.at[me], p, 2).start()
    gates_all[pl.ds(me, 1)] = gates[...].reshape(1, 1, 512)

    phase('p08_gatherr')
    cp_r.wait()
    gather(r_v, rsend)
    for p in peers:
        push(rsend.at[p], rrecv.at[me], p, 3).start()
    rrecv[pl.ds(me, 1)] = rsend[pl.ds(me, 1)]

    phase('p09_waitx')
    wait_recv(xrecv, 1)

    def send_h(q, half):
        cols = pl.ds(half * HALF, HALF)
        for p in peers:
            push(hsend.at[q, p, :, cols], hrecv.at[q, me, :, cols], p, 4 + 2 * q + half).start()

    def wait_h(buf, sem):
        for q in range(2):
            for half in range(2):
                part = buf.at[q, pl.ds(0, N - 1), :, pl.ds(half * HALF, HALF)]
                pltpu.make_async_copy(part, part, sem.at[4 + 2 * q + half]).wait()

    phase('p10_fwd')
    def fwd(q, carry):
        for j in range(2):
            e = 2 * q + j
            slot = e % 3
            xl = dot(e_v[e], xrecv[...].reshape(TOK, HID)).astype(BF)
            xl_v[e] = xl
            weight1(e, slot).wait()
            a = dot(xl_v[e], w1[slot])
            if j == 0:
                @pl.when(q == 0)
                def _():
                    weight1(3, 0).start()
            k0 = math.sqrt(2.0 / math.pi)
            t = jnp.tanh(k0 * (a + 0.044715 * (a * a * a)))
            u_v[e] = (0.5 * a * (1.0 + t)).astype(BF)
            gp_v[e] = 0.5 * (1.0 + t) + 0.5 * a * (1.0 - t * t) * (k0 * (1.0 + 3.0 * 0.044715 * (a * a)))
        weight2(2 * q, (2 * q) % 3).wait()
        weight2(2 * q + 1, (2 * q + 1) % 3).wait()

        def step(c, carry):
            cols = pl.ds(pl.multiple_of(c * CH, CH), CH)
            outs = [dot(u_v[2 * q + j], w2[(2 * q + j) % 3, :, cols]).reshape(N, 8, CH) for j in range(2)]
            hsend[q, :, :, cols] = jnp.concatenate(outs, axis=1).astype(BF)
            return carry
        lax.fori_loop(0, NCH, step, 0)

        @pl.when(q == 0)
        def _():
            weight2(3, 0).start()
        hrecv[q, pl.ds(me, 1)] = hsend[q, pl.ds(me, 1)]

        @pl.when(q == 0)
        def _():
            send_h(0, 0)
        return carry
    lax.fori_loop(0, 2, fwd, 0)
    pltpu.make_async_copy(xl_v, xl_out, out_sem.at[0]).start()
    pltpu.make_async_copy(u_v, u_out, out_sem.at[1]).start()

    phase('p11_waitr')
    wait_recv(gates_all, 2)
    wait_recv(rrecv, 3)

    def send_now(c):
        cols = pl.ds(c * CH, CH)
        for p in peers:
            push(gsend.at[1, p, :, cols], gnow_out.at[me, :, cols], p, 13 + c).start()
        pltpu.make_async_copy(gsend.at[1, me, :, cols], gnow_out.at[me, :, cols], out_sem.at[12 + c]).start()

    phase('p11b_pre')
    lane128 = iota((CAP, 128), 1)
    rows = jnp.broadcast_to(gates_all[...], (N, 8, 512)).reshape(CAP, 512)

    def pre(q, table):
        for j in range(2):
            e = 2 * q + j
            here = iota((CAP, 512), 1) == q * 256 + me * 16 + j * 8 + iota((CAP, 512), 0) % 8
            gcol = jnp.sum(jnp.where(here, rows, 0.0), axis=1, keepdims=True)

            def rstep(c, acc):
                cols = pl.ds(pl.multiple_of(c * CH, CH), CH)
                rl = dot(e_v[e], rrecv[:, :, cols].reshape(TOK, CH))
                dh_v[e, :, cols] = (gcol * (rl * scale)).astype(BF)
                hj = hsend[q, :, :, cols].astype(F32)[:, 8 * j:8 * j + 8, :].reshape(CAP, CH)
                prod = rl * hj
                return acc + ((prod[:, 0:128] + prod[:, 128:256]) + (prod[:, 256:384] + prod[:, 384:512]))
            acc = lax.fori_loop(0, NCH, rstep, jnp.zeros((CAP, 128), F32))
            table = table + jnp.where(lane128 == e, jnp.sum(acc, axis=1, keepdims=True) * scale, 0.0)
        return table
    dgsend[...] = lax.fori_loop(0, 2, pre, jnp.zeros((CAP, 128), F32)).reshape(N, 8, 128)
    for p in peers:
        push(dgsend.at[p], dgall.at[me], p, 8).start()
    dgall[pl.ds(me, 1)] = dgsend[pl.ds(me, 1)]
    send_h(0, 1)

    def gate_grads():
        with jax.named_scope('w_gate_grads'):
            gate_grads_wait()
        with jax.named_scope('c_gate_grads'):
            gate_grads_rest()

    def gate_grads_wait():
        wait_recv(dgall, 8)

    def gate_grads_rest():
        mine_of = []
        for l in range(LE):
            col = jnp.sum(jnp.where(iota((N, 8, 128), 2) == l, dgall[...], 0.0), axis=2, keepdims=True).reshape(CAP, 1)
            mine_of.append(jnp.where(iota((CAP, 64), 1) == 4 * (iota((CAP, 64), 0) // 8) + l, col, 0.0).reshape(N, 8, 64))
        spread_g = jnp.concatenate([jnp.concatenate(mine_of[2 * q:2 * q + 2], axis=1).reshape(256, 64) for q in range(2)], axis=0)
        ds = 0.0
        for term in split3(spread_g):
            ds = ds + dot(one_v[...], term)
        probs = probs_v[...]
        dlog = (probs * (ds - jnp.sum(probs * ds, axis=1, keepdims=True))).astype(BF)
        dlog_v[...] = dlog
        dlog_t = dlog.astype(F32).T.astype(BF)
        for c in range(NCH):
            part = dot(dlog_t, x_v[:, c * CH:(c + 1) * CH])
            for i in range(CH // 128):
                ggpart[c // 2, (c % 2) * (CH // 128) + i] = part[:, i * 128:(i + 1) * 128]
        push(ggpart.at[1 - core], ggpair, twin, 17).start()
        send_h(1, 0)

    def gate_scatter():
        with jax.named_scope('w_gate_scatter'):
            gate_scatter_wait()
        with jax.named_scope('c_gate_scatter'):
            gate_scatter_rest()

    def gate_scatter_wait():
        push(ggpart.at[1 - core], ggpair, twin, 17).wait_recv()

    def gate_scatter_rest():
        gghalf[...] = ggpart[core] + ggpair[...]
        for p in others:
            push(gghalf.at[p // 2], ggrecv.at[chip], p, 10).start()
        ggrecv[pl.ds(chip, 1)] = gghalf[pl.ds(chip, 1)]
        send_h(1, 1)

    def gate_gather():
        with jax.named_scope('w_gate_gather'):
            gate_gather_wait()
        with jax.named_scope('c_gate_gather'):
            gate_gather_rest()

    def gate_gather_wait():
        wait_recv(ggrecv, 10, 7)

    def gate_gather_rest():
        total = ggrecv[0]
        for i in range(1, 8):
            total = total + ggrecv[i]
        ggall[core, pl.ds(chip, 1)] = total.reshape(1, 64, 128)
        for p in others:
            push(ggall.at[core, chip], ggall.at[core, chip], p, 11).start()
        for c in range(NOW):
            send_now(c)

    phase('p12_bwd')
    def bwd(q, carry):
        for j in range(2):
            e = 2 * (1 - q) + j
            slot = (1 - q) * (2 - 2 * j) + q * (2 - j)
            if j == 0:
                @pl.when(q == 1)
                def _():
                    weight1(0, 2).wait()
                    weight2(0, 2).wait()
            du = dot(dh_v[e], w2[slot], 1, 1).astype(BF).astype(F32)
            if j == 0:
                @pl.when(q == 0)
                def _():
                    weight2(0, 2).start()
            da_v[e] = (gp_v[e] * du).astype(BF)
            if j == 0:
                pl.when(q == 0)(gate_grads)
                pl.when(q == 1)(gate_gather)

        def step(c, carry):
            cols = pl.ds(pl.multiple_of(c * CH, CH), CH)
            outs = []
            for j in range(2):
                slot = (1 - q) * (2 - 2 * j) + q * (2 - j)
                outs.append(dot(da_v[2 * (1 - q) + j], w1[slot, cols, :], 1, 1).reshape(N, 8, CH))
            gsend[1 - q, :, :, cols] = jnp.concatenate(outs, axis=1).astype(BF)
            return carry
        lax.fori_loop(0, NCH, step, 0)

        @pl.when(q == 0)
        def _():
            weight1(0, 2).start()
            gate_scatter()
        return carry
    lax.fori_loop(0, 2, bwd, 0)
    phase('p12b_later')
    later = [pltpu.make_async_copy(gsend.at[0], glater_out.at[:, :, pl.ds(0, HID)], out_sem.at[5])]
    if NOW < NCH:
        later.append(pltpu.make_async_copy(gsend.at[1, :, :, pl.ds(NOW * CH, HID - NOW * CH)],
                                           glater_out.at[:, :, pl.ds(HID, HID - NOW * CH)], out_sem.at[9]))
    for cp in later:
        cp.start()
    pltpu.make_async_copy(dh_v, dh_out, out_sem.at[2]).start()
    pltpu.make_async_copy(da_v, da_out, out_sem.at[3]).start()

    cp_dlog = pltpu.make_async_copy(dlog_v, dlog_out, out_sem.at[10])
    cp_dlog.start()
    cp_one = pltpu.make_async_copy(one_v, one_out, out_sem.at[11])
    cp_one.start()

    phase('p13_waith')
    wait_h(hrecv, recv_sem)
    wait_send(xsend, 1)

    phase('p15_y')
    def ystep(c, acc):
        cols = pl.ds(pl.multiple_of(c * CH, CH), CH)
        h = hrecv[:, :, :, cols].reshape(512, CH)
        tot = x_v[:, cols].astype(F32) + (dot(c_v[0], h) + dot(c_v[1], h) + dot(c_v[2], h))
        y = tot.astype(BF)
        xsend[:, :, cols] = y.reshape(N, 16, CH)
        return acc + jnp.sum(y.astype(F32) * r_v[:, cols].astype(F32), axis=0, keepdims=True)
    losssend[...] = lax.fori_loop(0, NCH, ystep, jnp.zeros((1, CH), F32))
    cp_y = pltpu.make_async_copy(xsend, y_out, out_sem.at[4])
    cp_y.start()
    for p in peers:
        push(losssend, lossall.at[me], p, 9).start()
    lossall[pl.ds(me, 1)] = losssend[...].reshape(1, 1, CH)

    phase('p20_loss')
    wait_recv(lossall, 9)
    loss_out[0, 0] = jnp.sum(lossall[...]) * scale
    phase('p21_waitgg')
    wait_recv(ggall.at[core], 11, 7)
    across = push(ggall.at[core], ggall.at[core], twin, 12)
    across.start()
    across.wait_recv()
    cp_gg = [pltpu.make_async_copy(ggall.at[i // 8, i % 8], gg_out.at[:, pl.ds(i * 128, 128)], out_sem.at[6]) for i in range(N)]
    for cp in cp_gg:
        cp.start()
    phase('p21b_waitg')
    for c in range(NOW):
        cols = pl.ds(c * CH, CH)
        part = gnow_out.at[pl.ds(0, N - 1), :, cols]
        pltpu.make_async_copy(part, part, recv_sem.at[13 + c]).wait()

    phase('p22_drain')
    wait_send(selall, 0)
    wait_send(gates_all, 2)
    wait_h(hsend, send_sem)
    wait_send(dgall, 8)
    for c in range(NOW):
        cols = pl.ds(c * CH, CH)
        part = gsend.at[1, pl.ds(0, N - 1), :, cols]
        pltpu.make_async_copy(part, part, send_sem.at[13 + c]).wait()
        pltpu.make_async_copy(gsend.at[1, me, :, cols], gnow_out.at[me, :, cols], out_sem.at[12 + c]).wait()
    wait_send(rsend, 3)
    wait_send(lossall, 9)
    push(ggpart.at[1 - core], ggpair, twin, 17).wait_send()
    wait_send(gghalf, 10, 7)
    wait_send(ggall.at[core], 11, 7)
    across.wait_send()
    for cp in later:
        cp.wait()
    cp_dlog.wait()
    cp_one.wait()
    pltpu.make_async_copy(xl_v, xl_out, out_sem.at[0]).wait()
    pltpu.make_async_copy(u_v, u_out, out_sem.at[1]).wait()
    pltpu.make_async_copy(dh_v, dh_out, out_sem.at[2]).wait()
    pltpu.make_async_copy(da_v, da_out, out_sem.at[3]).wait()
    cp_y.wait()
    for cp in cp_gg:
        cp.wait()
    phase(None)


def comm_call(sel, x, gw, up, dn, r, scale):
    any_ = pl.BlockSpec(memory_space=pl.ANY)
    vmem = pl.BlockSpec(memory_space=pltpu.VMEM)
    V = pltpu.VMEM
    shape = jax.ShapeDtypeStruct
    return pl.pallas_call(
        functools.partial(comm_kernel, scale),
        out_shape=[shape((N, 16, HID), BF), shape((N, 16, NOW * CH), BF), shape((N, 16, 2 * HID - NOW * CH), BF), shape((TOK, 512), BF),
                   shape((TOK, 64), BF), shape((64, HID), F32), shape((1, 1), F32),
                   shape((LE, CAP, HID), BF), shape((LE, CAP, FF), BF), shape((LE, CAP, HID), BF), shape((LE, CAP, FF), BF)],
        in_specs=[vmem, any_, any_, any_, any_, any_],
        out_specs=[any_, any_, any_, any_, any_, any_, pl.BlockSpec(memory_space=pltpu.SMEM), any_, any_, any_, any_],
        scratch_shapes=[
            V((TOK, HID), BF), V((TOK, HID), BF), V((64, HID), BF),
            V((3, HID, FF), BF), V((3, FF, HID), BF),
            V((N, 16, HID), BF), V((N, 16, HID), BF), V((N, 16, HID), BF), V((N, 16, HID), BF),
            V((2, N, 16, HID), BF), V((2, N, 16, HID), BF), V((2, N, 16, HID), BF),
            V((LE, CAP, HID), BF), V((LE, CAP, HID), BF), V((LE, CAP, FF), BF), V((LE, CAP, FF), F32), V((LE, CAP, FF), BF),
            V((2, 8, 64, 128), F32), V((8, 64, 128), F32), V((8, 64, 128), F32), V((8, 64, 128), F32), V((2, 8, 64, 128), F32),
            V((8, CAP), jnp.int32), V((N, 8, CAP), jnp.int32), V((1, 512), F32), V((N, 1, 512), F32),
            V((1, CH), F32), V((N, 1, CH), F32), V((N, 8, 128), F32), V((N, 8, 128), F32),
            V((TOK, 512), BF), V((3, TOK, 512), BF), V((LE, CAP, TOK), BF), V((TOK, 64), F32), V((TOK, 64), BF),
            pltpu.SemaphoreType.DMA((3,)), pltpu.SemaphoreType.DMA((2, 3)), pltpu.SemaphoreType.DMA((16,)),
            pltpu.SemaphoreType.DMA((18,)), pltpu.SemaphoreType.DMA((18,)),
        ],
        compiler_params=pltpu.CompilerParams(collective_id=0, has_side_effects=True, vmem_limit_bytes=67043328),
        name='exchange',
    )(sel, x, gw, up, dn, r)


def tile_tools(ins, bufs, outs, tiles, in_sem, out_sem, first):
    def loads(e):
        return [pltpu.make_async_copy(src.at[e], dst.at[e - first], in_sem.at[e - first]) for src, dst in zip(ins, bufs)]

    def stores(i):
        e, c = i // NCH, i % NCH
        cols = pl.ds(pl.multiple_of(c * CH, CH), CH)
        return [pltpu.make_async_copy(tiles[0].at[i - first * NCH], outs[0].at[e, cols, :], out_sem.at[0]),
                pltpu.make_async_copy(tiles[1].at[i - first * NCH], outs[1].at[e, :, cols], out_sem.at[1])]

    def step(i, carry):
        e, c = i // NCH, i % NCH
        xl_v, da_v, u_v, dh_v = bufs
        cols = pl.ds(pl.multiple_of(c * CH, CH), CH)
        tiles[0][i - first * NCH] = dot(xl_v[e - first, :, cols], da_v[e - first], 0, 0).astype(BF)
        tiles[1][i - first * NCH] = dot(u_v[e - first], dh_v[e - first, :, cols], 0, 0).astype(BF)
        for cp in stores(i):
            cp.start()
        return carry

    def finish(i, carry):
        for cp in stores(i):
            cp.wait()
        return carry
    return loads, step, finish


def wgrad1_kernel(xl_in, da_in, u_in, dh_in, y_in, gg_in, loss_in, g1, g2, y, gg, loss,
                  xl_v, da_v, u_v, dh_v, y_v, gg_v, t1, t2, in_sem, out_sem):
    loads, step, finish = tile_tools((xl_in, da_in, u_in, dh_in), (xl_v, da_v, u_v, dh_v), (g1, g2), (t1, t2), in_sem, out_sem, 0)
    cp_y = pltpu.make_async_copy(y_in, y_v, in_sem.at[LE])
    cp_gg = pltpu.make_async_copy(gg_in, gg_v, in_sem.at[LE + 1])
    for cp in loads(0):
        cp.start()
    loss[0, 0] = loss_in[0, 0]

    def expert(e, carry):
        for cp in loads(e):
            cp.wait()

        @pl.when(e + 1 < FIRST)
        def _():
            for cp in loads(e + 1):
                cp.start()

        @pl.when(e == 0)
        def _():
            cp_y.start()
            cp_gg.start()
        lax.fori_loop(e * NCH, (e + 1) * NCH, step, 0)
        return carry
    lax.fori_loop(0, FIRST, expert, 0)
    cp_y.wait()
    cp_gg.wait()
    out_y = pltpu.make_async_copy(y_v, y, in_sem.at[LE])
    out_gg = pltpu.make_async_copy(gg_v, gg, in_sem.at[LE + 1])
    out_y.start()
    out_gg.start()
    out_y.wait()
    out_gg.wait()
    lax.fori_loop(0, FIRST * NCH, finish, 0)


def wgrad1_call(xl, da, u, dh, y, gg, loss):
    shape = jax.ShapeDtypeStruct
    any_ = pl.BlockSpec(memory_space=pl.ANY)
    smem = pl.BlockSpec(memory_space=pltpu.SMEM)
    V = pltpu.VMEM
    return pl.pallas_call(
        wgrad1_kernel,
        in_specs=[any_] * 6 + [smem],
        out_specs=[any_] * 4 + [smem],
        out_shape=[shape((LE, HID, FF), BF), shape((LE, FF, HID), BF), shape((N, 16, HID), BF), shape((64, HID), F32), shape((1, 1), F32)],
        scratch_shapes=[V((FIRST, CAP, HID), BF), V((FIRST, CAP, FF), BF), V((FIRST, CAP, FF), BF), V((FIRST, CAP, HID), BF),
                        V((N, 16, HID), BF), V((64, HID), F32), V((FIRST * NCH, CH, FF), BF), V((FIRST * NCH, FF, CH), BF),
                        pltpu.SemaphoreType.DMA((LE + 2,)), pltpu.SemaphoreType.DMA((2,))],
        compiler_params=pltpu.CompilerParams(vmem_limit_bytes=67043328),
        cost_estimate=pl.CostEstimate(flops=FIRST * 4 * CAP * HID * FF, bytes_accessed=48 * 1024 * 1024, transcendentals=0),
        name='weight_grads_a',
    )(xl, da, u, dh, y, gg, loss)


def gradx_kernel(scale, late_in, now_in, r_in, one_in, dlog_in, gw_in, gx, late_v, now_v, r_v, one_v, dlog_v, gw_v, gx_v, in_sem, out_sem):
    def pieces(c):
        cols = pl.ds(c * CH, CH)
        out = [pltpu.make_async_copy(late_in.at[:, :, cols], late_v.at[:, :, cols], in_sem.at[c])]
        out.append(pltpu.make_async_copy(r_in.at[:, cols], r_v.at[:, cols], in_sem.at[c]))
        if c < NOW:
            out.append(pltpu.make_async_copy(now_in.at[:, :, cols], now_v.at[:, :, cols], in_sem.at[c]))
        else:
            more = pl.ds((NCH + c - NOW) * CH, CH)
            out.append(pltpu.make_async_copy(late_in.at[:, :, more], now_v.at[:, :, cols], in_sem.at[c]))
        return out
    first = [pltpu.make_async_copy(src, dst, in_sem.at[NCH]) for src, dst in ((one_in, one_v), (dlog_in, dlog_v), (gw_in, gw_v))]
    for cp in first:
        cp.start()
    for c in range(NCH):
        for cp in pieces(c):
            cp.start()
    for cp in first:
        cp.wait()
    for c in range(NCH):
        cols = pl.ds(c * CH, CH)
        for cp in pieces(c):
            cp.wait()
        tot = r_v[:, cols].astype(F32) * scale + dot(one_v[:, 0:256], late_v[:, :, cols].reshape(256, CH))
        tot = tot + dot(one_v[:, 256:512], now_v[:, :, cols].reshape(256, CH))
        gx_v[:, cols] = (tot + dot(dlog_v[...], gw_v[:, cols])).astype(BF)
        pltpu.make_async_copy(gx_v.at[:, cols], gx.at[:, cols], out_sem).start()
    for c in range(NCH):
        cols = pl.ds(c * CH, CH)
        pltpu.make_async_copy(gx_v.at[:, cols], gx.at[:, cols], out_sem).wait()


def gradx_call(late, now, r, one, dlog, gw, scale):
    any_ = pl.BlockSpec(memory_space=pl.ANY)
    V = pltpu.VMEM
    return pl.pallas_call(
        functools.partial(gradx_kernel, scale),
        in_specs=[any_] * 6,
        out_specs=any_,
        out_shape=jax.ShapeDtypeStruct((TOK, HID), BF),
        scratch_shapes=[V((N, 16, HID), BF), V((N, 16, HID), BF), V((TOK, HID), BF), V((TOK, 512), BF), V((TOK, 64), BF), V((64, HID), BF),
                        V((TOK, HID), BF), pltpu.SemaphoreType.DMA((NCH + 1,)), pltpu.SemaphoreType.DMA],
        compiler_params=pltpu.CompilerParams(vmem_limit_bytes=67043328),
        name='grad_x',
    )(late, now, r, one, dlog, gw)


def solution(mesh):
    def device_step(x, gate_w, up_w, down_w, expert_picks, loss_w):
        scale = 1.0 / math.sqrt(TOK * N * HID)
        gate_t = gate_w.T
        y, now, later, one, dlog, gg, loss, xl, u, dh, da = comm_call(expert_picks, x, gate_t, up_w, down_w, loss_w, scale)
        later = lax.all_to_all(later, 'ep', 0, 0, tiled=True)
        grad_up, grad_down, y, gg, loss = wgrad1_call(xl, da, u, dh, y, gg, loss)
        grad_x = gradx_call(later, now, loss_w, one, dlog, gate_t, scale)
        return y.reshape(TOK, HID), loss[0, 0], grad_x, grad_up, grad_down, gg.T

    return jax.shard_map(device_step, mesh=mesh,
                         in_specs=(P('ep'), P(), P('ep'), P('ep'), P('ep'), P('ep')),
                         out_specs=(P('ep'), P(), P('ep'), P('ep'), P('ep'), P()),
                         check_vma=False)
```

```python
import functools
import math
import jax
import jax.numpy as jnp
from jax import lax
from jax.experimental import pallas as pl
from jax.experimental.pallas import tpu as pltpu
from jax.sharding import PartitionSpec as P

BF = jnp.bfloat16
F32 = jnp.float32
MESH = pl.DeviceIdType.MESH
N = 16
TOK = 256
LE = 4
CAP = 128
HID = 2048
FF = 1408
CH = 512
NCH = HID // CH
FIRST = 4
HALF = HID // 2
NOW = 2
ORDER = (14, 15, 6, 10, 12, 7, 11, 13, 2, 4, 8, 3, 5, 9, 1)


def dot(a, b, ca=1, cb=0):
    return lax.dot_general(a, b, (((ca,), (cb,)), ((), ())), preferred_element_type=F32)


def iota(shape, dim):
    return lax.broadcasted_iota(jnp.int32, shape, dim)


def ones_where(cond):
    return jnp.where(cond, 1.0, 0.0).astype(BF)


def split3(v):
    hi = v.astype(BF)
    rest = v - hi.astype(F32)
    mid = rest.astype(BF)
    low = (rest - mid.astype(F32)).astype(BF)
    return hi, mid, low


def flip(me, k):
    out = 0
    for b in range(4):
        bit = (me // (1 << b)) % 2
        if (k >> b) & 1:
            bit = 1 - bit
        out = out + bit * (1 << b)
    return out


def comm_kernel(scale, sel_ref, x_hbm, gw_hbm, up_hbm, dn_hbm, r_hbm,
                y_out, gnow_out, glater_out, one_out, dlog_out, gg_out, loss_out, xl_out, u_out, dh_out, da_out,
                x_v, r_v, gw_v, w1, w2, xsend, rsend, xrecv, rrecv, hsend, hrecv, gsend,
                xl_v, dh_v, u_v, gp_v, da_v, ggpart, ggpair, gghalf, ggrecv, ggall, selsend, selall, gates, gates_all,
                losssend, lossall, dgsend, dgall, one_v, c_v, e_v, probs_v, dlog_v,
                ld_sem, w_sem, out_sem, send_sem, recv_sem):
    open_ = []

    def phase(name):
        if open_:
            open_.pop().__exit__(None, None, None)
        if name:
            open_.append(jax.named_scope(name))
            open_[-1].__enter__()
    me = lax.axis_index('ep')
    peers = [flip(me, k) for k in ORDER]
    core, chip, twin = me % 2, me // 2, flip(me, 1)
    others = [flip(me, k) for k in ORDER if k % 2 == 0]

    def load(src, dst, i):
        return pltpu.make_async_copy(src, dst, ld_sem.at[i])

    def weight1(e, slot):
        return pltpu.make_async_copy(up_hbm.at[e], w1.at[slot], w_sem.at[0, slot])

    def weight2(e, slot):
        return pltpu.make_async_copy(dn_hbm.at[e], w2.at[slot], w_sem.at[1, slot])

    def push(src, dst, peer, i):
        return pltpu.make_async_remote_copy(src_ref=src, dst_ref=dst, send_sem=send_sem.at[i], recv_sem=recv_sem.at[i],
                                            device_id=(peer,), device_id_type=MESH)

    def wait_recv(buf, i, n=N - 1):
        part = buf.at[pl.ds(0, n)]
        pltpu.make_async_copy(part, part, recv_sem.at[i]).wait()

    def wait_send(buf, i, n=N - 1):
        part = buf.at[pl.ds(0, n)]
        pltpu.make_async_copy(part, part, send_sem.at[i]).wait()

    phase('p00_start')
    cp_x = load(x_hbm, x_v, 0)
    cp_g = load(gw_hbm, gw_v, 1)
    cp_r = load(r_hbm, r_v, 2)
    cp_x.start()
    cp_g.start()
    cp_r.start()

    sel = sel_ref[...]
    selsend[...] = jnp.zeros_like(selsend)
    selsend[0:LE, :] = sel
    selall[pl.ds(me, 1)] = selsend[...].reshape(1, 8, CAP)

    phase('p01_barrier')
    barrier = pltpu.get_barrier_semaphore()
    for p in peers:
        pl.semaphore_signal(barrier, inc=1, device_id=(p,), device_id_type=MESH)
    pl.semaphore_wait(barrier, N - 1)

    for p in peers:
        push(selsend, selall.at[me], p, 0).start()
    for e in range(3):
        weight1(e, e).start()
        weight2(e, e).start()

    phase('p02_logits')
    cp_g.wait()
    cp_x.wait()
    logits = dot(x_v[...], gw_v[...], 1, 1)
    ex = jnp.exp(logits - jnp.max(logits, axis=1, keepdims=True))
    probs = ex / jnp.sum(ex, axis=1, keepdims=True)
    probs_v[...] = probs

    phase('p03_ownpicks')
    below = ones_where(iota((TOK, TOK), 1) < iota((TOK, TOK), 0))
    slot_lane = (iota((TOK, TOK), 1) % 16).astype(F32)

    tok_row = iota((TOK, CAP), 0)
    same = iota((CAP, TOK), 0) // 8 == iota((CAP, TOK), 1) // 16
    fold = ones_where(same)
    base = (iota((1, CAP), 1) // 8) * TOK
    hits = [ones_where(tok_row == sel[l:l + 1, :] - base) for l in range(LE)]
    count = dot(hits[0], fold)
    for l in range(1, LE):
        count = count + dot(hits[l], fold)
    pres = count > 0.5
    rank = dot(below, ones_where(pres))
    pick_of = jnp.where(pres, jnp.where(rank == slot_lane, 1.0, 0.0), 0.0).astype(BF)
    for l in range(LE):
        e_v[l] = jnp.where(same, dot(hits[l], pick_of, 0, 0), 0.0).astype(BF)

    phase('p04_waitsel')
    place = ones_where(iota((CAP, 512), 0) % 8 == iota((CAP, 512), 1) % 8)
    fold2 = ones_where((iota((512, TOK), 0) % 256) // 16 == iota((512, TOK), 1) // 16)
    for_wait = selall.at[pl.ds(0, N - 1)]
    pltpu.make_async_copy(for_wait, for_wait, recv_sem.at[0]).wait()
    phase('p05_give')
    everyone = selall[...].reshape(8 * N, CAP)
    mine = jnp.where(iota((8 * N, CAP), 1) // 8 == me, everyone - me * TOK, 0).astype(F32).astype(BF)
    spread = dot(mine, place)
    lane = iota((8 * N, 512), 1)
    want = ((lane % 256) // 16) * 8 + 2 * (lane // 256) + (lane % 16) // 8
    ids = jnp.sum(jnp.where(iota((8 * N, 512), 0) == want, spread, 0.0), axis=0, keepdims=True)
    one = jnp.where(iota((TOK, 512), 0).astype(F32) == ids, 1.0, 0.0)
    one_v[...] = one.astype(BF)
    pres2 = dot(one_v[...], fold2) > 0.5
    rank2 = dot(below, ones_where(pres2))
    give = jnp.where(pres2, jnp.where(rank2 == slot_lane, 1.0, 0.0), 0.0).astype(BF)
    give_t = give.T

    def gather(src, dst):
        def step(c, carry):
            cols = pl.ds(pl.multiple_of(c * CH, CH), CH)
            dst[:, :, cols] = dot(give_t, src[:, cols]).astype(BF).reshape(N, 16, CH)
            return carry
        lax.fori_loop(0, NCH, step, 0)

    phase('p06_gatherx')
    for c in range(NCH):
        cols = pl.ds(c * CH, CH)
        xsend[:, :, cols] = dot(give_t, x_v[:, cols]).astype(BF).reshape(N, 16, CH)
        for p in peers:
            push(xsend.at[p, :, cols], xrecv.at[me, :, cols], p, 1).start()
    xrecv[pl.ds(me, 1)] = xsend[pl.ds(me, 1)]

    phase('p07_gates')
    rep = ones_where(iota((64, 512), 0) == 4 * ((iota((64, 512), 1) % 256) // 16) + 2 * (iota((64, 512), 1) // 256)
                     + (iota((64, 512), 1) % 16) // 8)
    wide = 0.0
    for term in split3(probs_v[...]):
        wide = wide + dot(term, rep)
    comb = wide * one
    for i, term in enumerate(split3(comb)):
        c_v[i] = term
    gates[...] = jnp.sum(comb, axis=0, keepdims=True)
    for p in peers:
        push(gates, gates_all.at[me], p, 2).start()
    gates_all[pl.ds(me, 1)] = gates[...].reshape(1, 1, 512)

    phase('p08_gatherr')
    cp_r.wait()
    gather(r_v, rsend)
    for p in peers:
        push(rsend.at[p], rrecv.at[me], p, 3).start()
    rrecv[pl.ds(me, 1)] = rsend[pl.ds(me, 1)]

    phase('p09_waitx')
    wait_recv(xrecv, 1)

    def send_h(q, half):
        cols = pl.ds(half * HALF, HALF)
        for p in peers:
            push(hsend.at[q, p, :, cols], hrecv.at[q, me, :, cols], p, 4 + 2 * q + half).start()

    def wait_h(buf, sem):
        for q in range(2):
            for half in range(2):
                part = buf.at[q, pl.ds(0, N - 1), :, pl.ds(half * HALF, HALF)]
                pltpu.make_async_copy(part, part, sem.at[4 + 2 * q + half]).wait()

    phase('p10_fwd')
    def fwd(q, carry):
        for j in range(2):
            e = 2 * q + j
            slot = e % 3
            xl = dot(e_v[e], xrecv[...].reshape(TOK, HID)).astype(BF)
            xl_v[e] = xl
            weight1(e, slot).wait()
            a = dot(xl_v[e], w1[slot])
            if j == 0:
                @pl.when(q == 0)
                def _():
                    weight1(3, 0).start()
            k0 = math.sqrt(2.0 / math.pi)
            t = jnp.tanh(k0 * (a + 0.044715 * (a * a * a)))
            u_v[e] = (0.5 * a * (1.0 + t)).astype(BF)
            gp_v[e] = 0.5 * (1.0 + t) + 0.5 * a * (1.0 - t * t) * (k0 * (1.0 + 3.0 * 0.044715 * (a * a)))
        weight2(2 * q, (2 * q) % 3).wait()
        weight2(2 * q + 1, (2 * q + 1) % 3).wait()

        def step(c, carry):
            cols = pl.ds(pl.multiple_of(c * CH, CH), CH)
            outs = [dot(u_v[2 * q + j], w2[(2 * q + j) % 3, :, cols]).reshape(N, 8, CH) for j in range(2)]
            hsend[q, :, :, cols] = jnp.concatenate(outs, axis=1).astype(BF)
            return carry
        lax.fori_loop(0, NCH, step, 0)

        @pl.when(q == 0)
        def _():
            weight2(3, 0).start()
        hrecv[q, pl.ds(me, 1)] = hsend[q, pl.ds(me, 1)]

        @pl.when(q == 0)
        def _():
            send_h(0, 0)
        return carry
    lax.fori_loop(0, 2, fwd, 0)
    pltpu.make_async_copy(xl_v, xl_out, out_sem.at[0]).start()
    pltpu.make_async_copy(u_v, u_out, out_sem.at[1]).start()

    phase('p11_waitr')
    wait_recv(gates_all, 2)
    wait_recv(rrecv, 3)

    def send_now(c):
        cols = pl.ds(c * CH, CH)
        for p in peers:
            push(gsend.at[1, p, :, cols], gnow_out.at[me, :, cols], p, 13 + c).start()
        pltpu.make_async_copy(gsend.at[1, me, :, cols], gnow_out.at[me, :, cols], out_sem.at[12 + c]).start()

    phase('p11b_pre')
    lane128 = iota((CAP, 128), 1)
    rows = jnp.broadcast_to(gates_all[...], (N, 8, 512)).reshape(CAP, 512)

    def pre(q, table):
        for j in range(2):
            e = 2 * q + j
            here = iota((CAP, 512), 1) == q * 256 + me * 16 + j * 8 + iota((CAP, 512), 0) % 8
            gcol = jnp.sum(jnp.where(here, rows, 0.0), axis=1, keepdims=True)

            def rstep(c, acc):
                cols = pl.ds(pl.multiple_of(c * CH, CH), CH)
                rl = dot(e_v[e], rrecv[:, :, cols].reshape(TOK, CH))
                dh_v[e, :, cols] = (gcol * (rl * scale)).astype(BF)
                hj = hsend[q, :, :, cols].astype(F32)[:, 8 * j:8 * j + 8, :].reshape(CAP, CH)
                prod = rl * hj
                return acc + ((prod[:, 0:128] + prod[:, 128:256]) + (prod[:, 256:384] + prod[:, 384:512]))
            acc = lax.fori_loop(0, NCH, rstep, jnp.zeros((CAP, 128), F32))
            table = table + jnp.where(lane128 == e, jnp.sum(acc, axis=1, keepdims=True) * scale, 0.0)
        return table
    dgsend[...] = lax.fori_loop(0, 2, pre, jnp.zeros((CAP, 128), F32)).reshape(N, 8, 128)
    for p in peers:
        push(dgsend.at[p], dgall.at[me], p, 8).start()
    dgall[pl.ds(me, 1)] = dgsend[pl.ds(me, 1)]
    send_h(0, 1)
    send_h(1, 0)

    def gate_grads():
        with jax.named_scope('w_gate_grads'):
            gate_grads_wait()
        with jax.named_scope('c_gate_grads'):
            gate_grads_rest()

    def gate_grads_wait():
        wait_recv(dgall, 8)

    def gate_grads_rest():
        mine_of = []
        for l in range(LE):
            col = jnp.sum(jnp.where(iota((N, 8, 128), 2) == l, dgall[...], 0.0), axis=2, keepdims=True).reshape(CAP, 1)
            mine_of.append(jnp.where(iota((CAP, 64), 1) == 4 * (iota((CAP, 64), 0) // 8) + l, col, 0.0).reshape(N, 8, 64))
        spread_g = jnp.concatenate([jnp.concatenate(mine_of[2 * q:2 * q + 2], axis=1).reshape(256, 64) for q in range(2)], axis=0)
        ds = 0.0
        for term in split3(spread_g):
            ds = ds + dot(one_v[...], term)
        probs = probs_v[...]
        dlog = (probs * (ds - jnp.sum(probs * ds, axis=1, keepdims=True))).astype(BF)
        dlog_v[...] = dlog
        dlog_t = dlog.astype(F32).T.astype(BF)
        for c in range(NCH):
            part = dot(dlog_t, x_v[:, c * CH:(c + 1) * CH])
            for i in range(CH // 128):
                ggpart[c // 2, (c % 2) * (CH // 128) + i] = part[:, i * 128:(i + 1) * 128]
        push(ggpart.at[1 - core], ggpair, twin, 17).start()

    def gate_scatter():
        with jax.named_scope('w_gate_scatter'):
            gate_scatter_wait()
        with jax.named_scope('c_gate_scatter'):
            gate_scatter_rest()

    def gate_scatter_wait():
        push(ggpart.at[1 - core], ggpair, twin, 17).wait_recv()

    def gate_scatter_rest():
        gghalf[...] = ggpart[core] + ggpair[...]
        for p in others:
            push(gghalf.at[p // 2], ggrecv.at[chip], p, 10).start()
        ggrecv[pl.ds(chip, 1)] = gghalf[pl.ds(chip, 1)]
        send_now(0)

    def gate_gather():
        with jax.named_scope('w_gate_gather'):
            gate_gather_wait()
        with jax.named_scope('c_gate_gather'):
            gate_gather_rest()

    def gate_gather_wait():
        wait_recv(ggrecv, 10, 7)

    def gate_gather_rest():
        total = ggrecv[0]
        for i in range(1, 8):
            total = total + ggrecv[i]
        ggall[core, pl.ds(chip, 1)] = total.reshape(1, 64, 128)
        for p in others:
            push(ggall.at[core, chip], ggall.at[core, chip], p, 11).start()
        for c in range(1, NOW):
            send_now(c)

    phase('p12_bwd')
    def bwd(q, carry):
        for j in range(2):
            e = 2 * (1 - q) + j
            slot = (1 - q) * (2 - 2 * j) + q * (2 - j)
            if j == 0:
                @pl.when(q == 1)
                def _():
                    weight1(0, 2).wait()
                    weight2(0, 2).wait()
            du = dot(dh_v[e], w2[slot], 1, 1).astype(BF).astype(F32)
            if j == 0:
                @pl.when(q == 0)
                def _():
                    weight2(0, 2).start()
            da_v[e] = (gp_v[e] * du).astype(BF)
            if j == 0:
                pl.when(q == 1)(gate_scatter)

        def step(c, carry):
            cols = pl.ds(pl.multiple_of(c * CH, CH), CH)
            outs = []
            for j in range(2):
                slot = (1 - q) * (2 - 2 * j) + q * (2 - j)
                outs.append(dot(da_v[2 * (1 - q) + j], w1[slot, cols, :], 1, 1).reshape(N, 8, CH))
            gsend[1 - q, :, :, cols] = jnp.concatenate(outs, axis=1).astype(BF)
            return carry
        lax.fori_loop(0, NCH, step, 0)

        @pl.when(q == 0)
        def _():
            weight1(0, 2).start()
            send_h(1, 1)
            gate_grads()
        return carry
    lax.fori_loop(0, 2, bwd, 0)
    phase('p12b_later')
    later = [pltpu.make_async_copy(gsend.at[0], glater_out.at[:, :, pl.ds(0, HID)], out_sem.at[5])]
    if NOW < NCH:
        later.append(pltpu.make_async_copy(gsend.at[1, :, :, pl.ds(NOW * CH, HID - NOW * CH)],
                                           glater_out.at[:, :, pl.ds(HID, HID - NOW * CH)], out_sem.at[9]))
    for cp in later:
        cp.start()
    pltpu.make_async_copy(dh_v, dh_out, out_sem.at[2]).start()
    pltpu.make_async_copy(da_v, da_out, out_sem.at[3]).start()

    cp_dlog = pltpu.make_async_copy(dlog_v, dlog_out, out_sem.at[10])
    cp_dlog.start()
    cp_one = pltpu.make_async_copy(one_v, one_out, out_sem.at[11])
    cp_one.start()

    phase('p13_waith')
    wait_h(hrecv, recv_sem)
    wait_send(xsend, 1)

    phase('p15_y')
    def ystep(c, acc):
        cols = pl.ds(pl.multiple_of(c * CH, CH), CH)
        h = hrecv[:, :, :, cols].reshape(512, CH)
        tot = x_v[:, cols].astype(F32) + (dot(c_v[0], h) + dot(c_v[1], h) + dot(c_v[2], h))
        y = tot.astype(BF)
        xsend[:, :, cols] = y.reshape(N, 16, CH)
        return acc + jnp.sum(y.astype(F32) * r_v[:, cols].astype(F32), axis=0, keepdims=True)
    losssend[...] = lax.fori_loop(0, NCH, ystep, jnp.zeros((1, CH), F32))
    cp_y = pltpu.make_async_copy(xsend, y_out, out_sem.at[4])
    cp_y.start()
    for p in peers:
        push(losssend, lossall.at[me], p, 9).start()
    lossall[pl.ds(me, 1)] = losssend[...].reshape(1, 1, CH)
    phase('p19_gather')
    gate_gather()

    phase('p20_waitgg')
    wait_recv(ggall.at[core], 11, 7)
    across = push(ggall.at[core], ggall.at[core], twin, 12)
    across.start()
    phase('p21_loss')
    wait_recv(lossall, 9)
    loss_out[0, 0] = jnp.sum(lossall[...]) * scale
    across.wait_recv()
    cp_gg = [pltpu.make_async_copy(ggall.at[i // 8, i % 8], gg_out.at[:, pl.ds(i * 128, 128)], out_sem.at[6]) for i in range(N)]
    for cp in cp_gg:
        cp.start()
    phase('p21b_waitg')
    for c in range(NOW):
        cols = pl.ds(c * CH, CH)
        part = gnow_out.at[pl.ds(0, N - 1), :, cols]
        pltpu.make_async_copy(part, part, recv_sem.at[13 + c]).wait()

    phase('p22_drain')
    wait_send(selall, 0)
    wait_send(gates_all, 2)
    wait_h(hsend, send_sem)
    wait_send(dgall, 8)
    for c in range(NOW):
        cols = pl.ds(c * CH, CH)
        part = gsend.at[1, pl.ds(0, N - 1), :, cols]
        pltpu.make_async_copy(part, part, send_sem.at[13 + c]).wait()
        pltpu.make_async_copy(gsend.at[1, me, :, cols], gnow_out.at[me, :, cols], out_sem.at[12 + c]).wait()
    wait_send(rsend, 3)
    wait_send(lossall, 9)
    push(ggpart.at[1 - core], ggpair, twin, 17).wait_send()
    wait_send(gghalf, 10, 7)
    wait_send(ggall.at[core], 11, 7)
    across.wait_send()
    for cp in later:
        cp.wait()
    cp_dlog.wait()
    cp_one.wait()
    pltpu.make_async_copy(xl_v, xl_out, out_sem.at[0]).wait()
    pltpu.make_async_copy(u_v, u_out, out_sem.at[1]).wait()
    pltpu.make_async_copy(dh_v, dh_out, out_sem.at[2]).wait()
    pltpu.make_async_copy(da_v, da_out, out_sem.at[3]).wait()
    cp_y.wait()
    for cp in cp_gg:
        cp.wait()
    phase(None)


def comm_call(sel, x, gw, up, dn, r, scale):
    any_ = pl.BlockSpec(memory_space=pl.ANY)
    vmem = pl.BlockSpec(memory_space=pltpu.VMEM)
    V = pltpu.VMEM
    shape = jax.ShapeDtypeStruct
    return pl.pallas_call(
        functools.partial(comm_kernel, scale),
        out_shape=[shape((N, 16, HID), BF), shape((N, 16, NOW * CH), BF), shape((N, 16, 2 * HID - NOW * CH), BF), shape((TOK, 512), BF),
                   shape((TOK, 64), BF), shape((64, HID), F32), shape((1, 1), F32),
                   shape((LE, CAP, HID), BF), shape((LE, CAP, FF), BF), shape((LE, CAP, HID), BF), shape((LE, CAP, FF), BF)],
        in_specs=[vmem, any_, any_, any_, any_, any_],
        out_specs=[any_, any_, any_, any_, any_, any_, pl.BlockSpec(memory_space=pltpu.SMEM), any_, any_, any_, any_],
        scratch_shapes=[
            V((TOK, HID), BF), V((TOK, HID), BF), V((64, HID), BF),
            V((3, HID, FF), BF), V((3, FF, HID), BF),
            V((N, 16, HID), BF), V((N, 16, HID), BF), V((N, 16, HID), BF), V((N, 16, HID), BF),
            V((2, N, 16, HID), BF), V((2, N, 16, HID), BF), V((2, N, 16, HID), BF),
            V((LE, CAP, HID), BF), V((LE, CAP, HID), BF), V((LE, CAP, FF), BF), V((LE, CAP, FF), F32), V((LE, CAP, FF), BF),
            V((2, 8, 64, 128), F32), V((8, 64, 128), F32), V((8, 64, 128), F32), V((8, 64, 128), F32), V((2, 8, 64, 128), F32),
            V((8, CAP), jnp.int32), V((N, 8, CAP), jnp.int32), V((1, 512), F32), V((N, 1, 512), F32),
            V((1, CH), F32), V((N, 1, CH), F32), V((N, 8, 128), F32), V((N, 8, 128), F32),
            V((TOK, 512), BF), V((3, TOK, 512), BF), V((LE, CAP, TOK), BF), V((TOK, 64), F32), V((TOK, 64), BF),
            pltpu.SemaphoreType.DMA((3,)), pltpu.SemaphoreType.DMA((2, 3)), pltpu.SemaphoreType.DMA((16,)),
            pltpu.SemaphoreType.DMA((18,)), pltpu.SemaphoreType.DMA((18,)),
        ],
        compiler_params=pltpu.CompilerParams(collective_id=0, has_side_effects=True, vmem_limit_bytes=67043328),
        name='exchange',
    )(sel, x, gw, up, dn, r)


def tile_tools(ins, bufs, outs, tiles, in_sem, out_sem, first):
    def loads(e):
        return [pltpu.make_async_copy(src.at[e], dst.at[e - first], in_sem.at[e - first]) for src, dst in zip(ins, bufs)]

    def stores(i):
        e, c = i // NCH, i % NCH
        cols = pl.ds(pl.multiple_of(c * CH, CH), CH)
        return [pltpu.make_async_copy(tiles[0].at[i - first * NCH], outs[0].at[e, cols, :], out_sem.at[0]),
                pltpu.make_async_copy(tiles[1].at[i - first * NCH], outs[1].at[e, :, cols], out_sem.at[1])]

    def step(i, carry):
        e, c = i // NCH, i % NCH
        xl_v, da_v, u_v, dh_v = bufs
        cols = pl.ds(pl.multiple_of(c * CH, CH), CH)
        tiles[0][i - first * NCH] = dot(xl_v[e - first, :, cols], da_v[e - first], 0, 0).astype(BF)
        tiles[1][i - first * NCH] = dot(u_v[e - first], dh_v[e - first, :, cols], 0, 0).astype(BF)
        for cp in stores(i):
            cp.start()
        return carry

    def finish(i, carry):
        for cp in stores(i):
            cp.wait()
        return carry
    return loads, step, finish


def wgrad1_kernel(xl_in, da_in, u_in, dh_in, y_in, gg_in, loss_in, g1, g2, y, gg, loss,
                  xl_v, da_v, u_v, dh_v, y_v, gg_v, t1, t2, in_sem, out_sem):
    loads, step, finish = tile_tools((xl_in, da_in, u_in, dh_in), (xl_v, da_v, u_v, dh_v), (g1, g2), (t1, t2), in_sem, out_sem, 0)
    cp_y = pltpu.make_async_copy(y_in, y_v, in_sem.at[LE])
    cp_gg = pltpu.make_async_copy(gg_in, gg_v, in_sem.at[LE + 1])
    for cp in loads(0):
        cp.start()
    loss[0, 0] = loss_in[0, 0]

    def expert(e, carry):
        for cp in loads(e):
            cp.wait()

        @pl.when(e + 1 < FIRST)
        def _():
            for cp in loads(e + 1):
                cp.start()

        @pl.when(e == 0)
        def _():
            cp_y.start()
            cp_gg.start()
        lax.fori_loop(e * NCH, (e + 1) * NCH, step, 0)
        return carry
    lax.fori_loop(0, FIRST, expert, 0)
    cp_y.wait()
    cp_gg.wait()
    out_y = pltpu.make_async_copy(y_v, y, in_sem.at[LE])
    out_gg = pltpu.make_async_copy(gg_v, gg, in_sem.at[LE + 1])
    out_y.start()
    out_gg.start()
    out_y.wait()
    out_gg.wait()
    lax.fori_loop(0, FIRST * NCH, finish, 0)


def wgrad1_call(xl, da, u, dh, y, gg, loss):
    shape = jax.ShapeDtypeStruct
    any_ = pl.BlockSpec(memory_space=pl.ANY)
    smem = pl.BlockSpec(memory_space=pltpu.SMEM)
    V = pltpu.VMEM
    return pl.pallas_call(
        wgrad1_kernel,
        in_specs=[any_] * 6 + [smem],
        out_specs=[any_] * 4 + [smem],
        out_shape=[shape((LE, HID, FF), BF), shape((LE, FF, HID), BF), shape((N, 16, HID), BF), shape((64, HID), F32), shape((1, 1), F32)],
        scratch_shapes=[V((FIRST, CAP, HID), BF), V((FIRST, CAP, FF), BF), V((FIRST, CAP, FF), BF), V((FIRST, CAP, HID), BF),
                        V((N, 16, HID), BF), V((64, HID), F32), V((FIRST * NCH, CH, FF), BF), V((FIRST * NCH, FF, CH), BF),
                        pltpu.SemaphoreType.DMA((LE + 2,)), pltpu.SemaphoreType.DMA((2,))],
        compiler_params=pltpu.CompilerParams(vmem_limit_bytes=67043328),
        cost_estimate=pl.CostEstimate(flops=FIRST * 4 * CAP * HID * FF, bytes_accessed=48 * 1024 * 1024, transcendentals=0),
        name='weight_grads_a',
    )(xl, da, u, dh, y, gg, loss)


def gradx_kernel(scale, late_in, now_in, r_in, one_in, dlog_in, gw_in, gx, late_v, now_v, r_v, one_v, dlog_v, gw_v, gx_v, in_sem, out_sem):
    def pieces(c):
        cols = pl.ds(c * CH, CH)
        out = [pltpu.make_async_copy(late_in.at[:, :, cols], late_v.at[:, :, cols], in_sem.at[c])]
        out.append(pltpu.make_async_copy(r_in.at[:, cols], r_v.at[:, cols], in_sem.at[c]))
        if c < NOW:
            out.append(pltpu.make_async_copy(now_in.at[:, :, cols], now_v.at[:, :, cols], in_sem.at[c]))
        else:
            more = pl.ds((NCH + c - NOW) * CH, CH)
            out.append(pltpu.make_async_copy(late_in.at[:, :, more], now_v.at[:, :, cols], in_sem.at[c]))
        return out
    first = [pltpu.make_async_copy(src, dst, in_sem.at[NCH]) for src, dst in ((one_in, one_v), (dlog_in, dlog_v), (gw_in, gw_v))]
    for cp in first:
        cp.start()
    for c in range(NCH):
        for cp in pieces(c):
            cp.start()
    for cp in first:
        cp.wait()
    for c in range(NCH):
        cols = pl.ds(c * CH, CH)
        for cp in pieces(c):
            cp.wait()
        tot = r_v[:, cols].astype(F32) * scale + dot(one_v[:, 0:256], late_v[:, :, cols].reshape(256, CH))
        tot = tot + dot(one_v[:, 256:512], now_v[:, :, cols].reshape(256, CH))
        gx_v[:, cols] = (tot + dot(dlog_v[...], gw_v[:, cols])).astype(BF)
        pltpu.make_async_copy(gx_v.at[:, cols], gx.at[:, cols], out_sem).start()
    for c in range(NCH):
        cols = pl.ds(c * CH, CH)
        pltpu.make_async_copy(gx_v.at[:, cols], gx.at[:, cols], out_sem).wait()


def gradx_call(late, now, r, one, dlog, gw, scale):
    any_ = pl.BlockSpec(memory_space=pl.ANY)
    V = pltpu.VMEM
    return pl.pallas_call(
        functools.partial(gradx_kernel, scale),
        in_specs=[any_] * 6,
        out_specs=any_,
        out_shape=jax.ShapeDtypeStruct((TOK, HID), BF),
        scratch_shapes=[V((N, 16, HID), BF), V((N, 16, HID), BF), V((TOK, HID), BF), V((TOK, 512), BF), V((TOK, 64), BF), V((64, HID), BF),
                        V((TOK, HID), BF), pltpu.SemaphoreType.DMA((NCH + 1,)), pltpu.SemaphoreType.DMA],
        compiler_params=pltpu.CompilerParams(vmem_limit_bytes=67043328),
        name='grad_x',
    )(late, now, r, one, dlog, gw)


def solution(mesh):
    def device_step(x, gate_w, up_w, down_w, expert_picks, loss_w):
        scale = 1.0 / math.sqrt(TOK * N * HID)
        gate_t = gate_w.T
        y, now, later, one, dlog, gg, loss, xl, u, dh, da = comm_call(expert_picks, x, gate_t, up_w, down_w, loss_w, scale)
        later = lax.all_to_all(later, 'ep', 0, 0, tiled=True)
        grad_up, grad_down, y, gg, loss = wgrad1_call(xl, da, u, dh, y, gg, loss)
        grad_x = gradx_call(later, now, loss_w, one, dlog, gate_t, scale)
        return y.reshape(TOK, HID), loss[0, 0], grad_x, grad_up, grad_down, gg.T

    return jax.shard_map(device_step, mesh=mesh,
                         in_specs=(P('ep'), P(), P('ep'), P('ep'), P('ep'), P('ep')),
                         out_specs=(P('ep'), P(), P('ep'), P('ep'), P('ep'), P()),
                         check_vma=False)
```

```python
import functools
import math
import jax
import jax.numpy as jnp
from jax import lax
from jax.experimental import pallas as pl
from jax.experimental.pallas import tpu as pltpu
from jax.sharding import PartitionSpec as P

BF = jnp.bfloat16
F32 = jnp.float32
MESH = pl.DeviceIdType.MESH
N = 16
TOK = 256
LE = 4
CAP = 128
HID = 2048
FF = 1408
CH = 512
NCH = HID // CH
FIRST = 4
HALF = HID // 2
NOW = 2
ORDER = (14, 15, 6, 10, 12, 7, 11, 13, 2, 4, 8, 3, 5, 9, 1)


def dot(a, b, ca=1, cb=0):
    return lax.dot_general(a, b, (((ca,), (cb,)), ((), ())), preferred_element_type=F32)


def iota(shape, dim):
    return lax.broadcasted_iota(jnp.int32, shape, dim)


def ones_where(cond):
    return jnp.where(cond, 1.0, 0.0).astype(BF)


def split3(v):
    hi = v.astype(BF)
    rest = v - hi.astype(F32)
    mid = rest.astype(BF)
    low = (rest - mid.astype(F32)).astype(BF)
    return hi, mid, low


def flip(me, k):
    out = 0
    for b in range(4):
        bit = (me // (1 << b)) % 2
        if (k >> b) & 1:
            bit = 1 - bit
        out = out + bit * (1 << b)
    return out


def comm_kernel(scale, sel_ref, x_hbm, gw_hbm, up_hbm, dn_hbm, r_hbm,
                y_out, gnow_out, glater_out, one_out, dlog_out, gg_out, loss_out, xl_out, u_out, dh_out, da_out,
                x_v, r_v, gw_v, w1, w2, xsend, rsend, xrecv, rrecv, hsend, hrecv, gsend,
                xl_v, dh_v, u_v, gp_v, da_v, ggpart, ggpair, gghalf, ggrecv, ggall, selsend, selall, gates, gates_all,
                losssend, lossall, dgsend, dgall, one_v, c_v, e_v, probs_v, dlog_v,
                ld_sem, w_sem, out_sem, send_sem, recv_sem):
    open_ = []

    def phase(name):
        if open_:
            open_.pop().__exit__(None, None, None)
        if name:
            open_.append(jax.named_scope(name))
            open_[-1].__enter__()
    me = lax.axis_index('ep')
    peers = [flip(me, k) for k in ORDER]
    core, chip, twin = me % 2, me // 2, flip(me, 1)
    others = [flip(me, k) for k in ORDER if k % 2 == 0]

    def load(src, dst, i):
        return pltpu.make_async_copy(src, dst, ld_sem.at[i])

    def weight1(e, slot):
        return pltpu.make_async_copy(up_hbm.at[e], w1.at[slot], w_sem.at[0, slot])

    def weight2(e, slot):
        return pltpu.make_async_copy(dn_hbm.at[e], w2.at[slot], w_sem.at[1, slot])

    def push(src, dst, peer, i):
        return pltpu.make_async_remote_copy(src_ref=src, dst_ref=dst, send_sem=send_sem.at[i], recv_sem=recv_sem.at[i],
                                            device_id=(peer,), device_id_type=MESH)

    def wait_recv(buf, i, n=N - 1):
        part = buf.at[pl.ds(0, n)]
        pltpu.make_async_copy(part, part, recv_sem.at[i]).wait()

    def wait_send(buf, i, n=N - 1):
        part = buf.at[pl.ds(0, n)]
        pltpu.make_async_copy(part, part, send_sem.at[i]).wait()

    phase('p00_start')
    cp_x = load(x_hbm, x_v, 0)
    cp_g = load(gw_hbm, gw_v, 1)
    cp_r = load(r_hbm, r_v, 2)
    cp_x.start()
    cp_g.start()
    cp_r.start()

    sel = sel_ref[...]
    selsend[...] = jnp.zeros_like(selsend)
    selsend[0:LE, :] = sel
    selall[pl.ds(me, 1)] = selsend[...].reshape(1, 8, CAP)

    phase('p01_barrier')
    barrier = pltpu.get_barrier_semaphore()
    for p in peers:
        pl.semaphore_signal(barrier, inc=1, device_id=(p,), device_id_type=MESH)
    pl.semaphore_wait(barrier, N - 1)

    for p in peers:
        push(selsend, selall.at[me], p, 0).start()
    for e in range(3):
        weight1(e, e).start()
        weight2(e, e).start()

    phase('p02_logits')
    cp_g.wait()
    cp_x.wait()
    logits = dot(x_v[...], gw_v[...], 1, 1)
    ex = jnp.exp(logits - jnp.max(logits, axis=1, keepdims=True))
    probs = ex / jnp.sum(ex, axis=1, keepdims=True)
    probs_v[...] = probs

    phase('p03_ownpicks')
    below = ones_where(iota((TOK, TOK), 1) < iota((TOK, TOK), 0))
    slot_lane = (iota((TOK, TOK), 1) % 16).astype(F32)

    tok_row = iota((TOK, CAP), 0)
    same = iota((CAP, TOK), 0) // 8 == iota((CAP, TOK), 1) // 16
    fold = ones_where(same)
    base = (iota((1, CAP), 1) // 8) * TOK
    hits = [ones_where(tok_row == sel[l:l + 1, :] - base) for l in range(LE)]
    count = dot(hits[0], fold)
    for l in range(1, LE):
        count = count + dot(hits[l], fold)
    pres = count > 0.5
    rank = dot(below, ones_where(pres))
    pick_of = jnp.where(pres, jnp.where(rank == slot_lane, 1.0, 0.0), 0.0).astype(BF)
    for l in range(LE):
        e_v[l] = jnp.where(same, dot(hits[l], pick_of, 0, 0), 0.0).astype(BF)

    phase('p04_waitsel')
    place = ones_where(iota((CAP, 512), 0) % 8 == iota((CAP, 512), 1) % 8)
    fold2 = ones_where((iota((512, TOK), 0) % 256) // 16 == iota((512, TOK), 1) // 16)
    for_wait = selall.at[pl.ds(0, N - 1)]
    pltpu.make_async_copy(for_wait, for_wait, recv_sem.at[0]).wait()
    phase('p05_give')
    everyone = selall[...].reshape(8 * N, CAP)
    mine = jnp.where(iota((8 * N, CAP), 1) // 8 == me, everyone - me * TOK, 0).astype(F32).astype(BF)
    spread = dot(mine, place)
    lane = iota((8 * N, 512), 1)
    want = ((lane % 256) // 16) * 8 + 2 * (lane // 256) + (lane % 16) // 8
    ids = jnp.sum(jnp.where(iota((8 * N, 512), 0) == want, spread, 0.0), axis=0, keepdims=True)
    one = jnp.where(iota((TOK, 512), 0).astype(F32) == ids, 1.0, 0.0)
    one_v[...] = one.astype(BF)
    pres2 = dot(one_v[...], fold2) > 0.5
    rank2 = dot(below, ones_where(pres2))
    give = jnp.where(pres2, jnp.where(rank2 == slot_lane, 1.0, 0.0), 0.0).astype(BF)
    give_t = give.T

    def gather(src, dst):
        def step(c, carry):
            cols = pl.ds(pl.multiple_of(c * CH, CH), CH)
            dst[:, :, cols] = dot(give_t, src[:, cols]).astype(BF).reshape(N, 16, CH)
            return carry
        lax.fori_loop(0, NCH, step, 0)

    phase('p06_gatherx')
    for c in range(NCH):
        cols = pl.ds(c * CH, CH)
        xsend[:, :, cols] = dot(give_t, x_v[:, cols]).astype(BF).reshape(N, 16, CH)
        for p in peers:
            push(xsend.at[p, :, cols], xrecv.at[me, :, cols], p, 1).start()
    xrecv[pl.ds(me, 1)] = xsend[pl.ds(me, 1)]

    phase('p07_gates')
    rep = ones_where(iota((64, 512), 0) == 4 * ((iota((64, 512), 1) % 256) // 16) + 2 * (iota((64, 512), 1) // 256)
                     + (iota((64, 512), 1) % 16) // 8)
    wide = 0.0
    for term in split3(probs_v[...]):
        wide = wide + dot(term, rep)
    comb = wide * one
    for i, term in enumerate(split3(comb)):
        c_v[i] = term
    gates[...] = jnp.sum(comb, axis=0, keepdims=True)
    for p in peers:
        push(gates, gates_all.at[me], p, 2).start()
    gates_all[pl.ds(me, 1)] = gates[...].reshape(1, 1, 512)

    phase('p08_gatherr')
    cp_r.wait()
    gather(r_v, rsend)
    for p in peers:
        push(rsend.at[p], rrecv.at[me], p, 3).start()
    rrecv[pl.ds(me, 1)] = rsend[pl.ds(me, 1)]

    phase('p09_waitx')
    wait_recv(xrecv, 1)

    def send_h(q, half):
        cols = pl.ds(half * HALF, HALF)
        for p in peers:
            push(hsend.at[q, p, :, cols], hrecv.at[q, me, :, cols], p, 4 + 2 * q + half).start()

    def wait_h(buf, sem):
        for q in range(2):
            for half in range(2):
                part = buf.at[q, pl.ds(0, N - 1), :, pl.ds(half * HALF, HALF)]
                pltpu.make_async_copy(part, part, sem.at[4 + 2 * q + half]).wait()

    phase('p10_fwd')
    def fwd(q, carry):
        for j in range(2):
            e = 2 * q + j
            slot = e % 3
            xl = dot(e_v[e], xrecv[...].reshape(TOK, HID)).astype(BF)
            xl_v[e] = xl
            weight1(e, slot).wait()
            a = dot(xl_v[e], w1[slot])
            if j == 0:
                @pl.when(q == 0)
                def _():
                    weight1(3, 0).start()
            k0 = math.sqrt(2.0 / math.pi)
            t = jnp.tanh(k0 * (a + 0.044715 * (a * a * a)))
            u_v[e] = (0.5 * a * (1.0 + t)).astype(BF)
            gp_v[e] = 0.5 * (1.0 + t) + 0.5 * a * (1.0 - t * t) * (k0 * (1.0 + 3.0 * 0.044715 * (a * a)))
        weight2(2 * q, (2 * q) % 3).wait()
        weight2(2 * q + 1, (2 * q + 1) % 3).wait()

        def step(c, carry):
            cols = pl.ds(pl.multiple_of(c * CH, CH), CH)
            outs = [dot(u_v[2 * q + j], w2[(2 * q + j) % 3, :, cols]).reshape(N, 8, CH) for j in range(2)]
            hsend[q, :, :, cols] = jnp.concatenate(outs, axis=1).astype(BF)
            return carry
        lax.fori_loop(0, NCH, step, 0)

        @pl.when(q == 0)
        def _():
            weight2(3, 0).start()
        hrecv[q, pl.ds(me, 1)] = hsend[q, pl.ds(me, 1)]

        @pl.when(q == 0)
        def _():
            send_h(0, 0)
        return carry
    lax.fori_loop(0, 2, fwd, 0)
    pltpu.make_async_copy(xl_v, xl_out, out_sem.at[0]).start()
    pltpu.make_async_copy(u_v, u_out, out_sem.at[1]).start()

    phase('p11_waitr')
    wait_recv(gates_all, 2)
    wait_recv(rrecv, 3)

    def send_now(c):
        cols = pl.ds(c * CH, CH)
        for p in peers:
            push(gsend.at[1, p, :, cols], gnow_out.at[me, :, cols], p, 13 + c).start()
        pltpu.make_async_copy(gsend.at[1, me, :, cols], gnow_out.at[me, :, cols], out_sem.at[12 + c]).start()

    phase('p11b_pre')
    lane128 = iota((CAP, 128), 1)
    rows = jnp.broadcast_to(gates_all[...], (N, 8, 512)).reshape(CAP, 512)

    def pre(q, table):
        for j in range(2):
            e = 2 * q + j
            here = iota((CAP, 512), 1) == q * 256 + me * 16 + j * 8 + iota((CAP, 512), 0) % 8
            gcol = jnp.sum(jnp.where(here, rows, 0.0), axis=1, keepdims=True)

            def rstep(c, acc):
                cols = pl.ds(pl.multiple_of(c * CH, CH), CH)
                rl = dot(e_v[e], rrecv[:, :, cols].reshape(TOK, CH))
                dh_v[e, :, cols] = (gcol * (rl * scale)).astype(BF)
                hj = hsend[q, :, :, cols].astype(F32)[:, 8 * j:8 * j + 8, :].reshape(CAP, CH)
                prod = rl * hj
                return acc + ((prod[:, 0:128] + prod[:, 128:256]) + (prod[:, 256:384] + prod[:, 384:512]))
            acc = lax.fori_loop(0, NCH, rstep, jnp.zeros((CAP, 128), F32))
            table = table + jnp.where(lane128 == e, jnp.sum(acc, axis=1, keepdims=True) * scale, 0.0)
        return table
    dgsend[...] = lax.fori_loop(0, 2, pre, jnp.zeros((CAP, 128), F32)).reshape(N, 8, 128)
    for p in peers:
        push(dgsend.at[p], dgall.at[me], p, 8).start()
    dgall[pl.ds(me, 1)] = dgsend[pl.ds(me, 1)]

    def gate_grads():
        with jax.named_scope('w_gate_grads'):
            gate_grads_wait()
        with jax.named_scope('c_gate_grads'):
            gate_grads_rest()

    def gate_grads_wait():
        wait_recv(dgall, 8)

    def gate_grads_rest():
        mine_of = []
        for l in range(LE):
            col = jnp.sum(jnp.where(iota((N, 8, 128), 2) == l, dgall[...], 0.0), axis=2, keepdims=True).reshape(CAP, 1)
            mine_of.append(jnp.where(iota((CAP, 64), 1) == 4 * (iota((CAP, 64), 0) // 8) + l, col, 0.0).reshape(N, 8, 64))
        spread_g = jnp.concatenate([jnp.concatenate(mine_of[2 * q:2 * q + 2], axis=1).reshape(256, 64) for q in range(2)], axis=0)
        ds = 0.0
        for term in split3(spread_g):
            ds = ds + dot(one_v[...], term)
        probs = probs_v[...]
        dlog = (probs * (ds - jnp.sum(probs * ds, axis=1, keepdims=True))).astype(BF)
        dlog_v[...] = dlog
        dlog_t = dlog.astype(F32).T.astype(BF)
        for c in range(NCH):
            part = dot(dlog_t, x_v[:, c * CH:(c + 1) * CH])
            for i in range(CH // 128):
                ggpart[c // 2, (c % 2) * (CH // 128) + i] = part[:, i * 128:(i + 1) * 128]
        push(ggpart.at[1 - core], ggpair, twin, 17).start()

    def gate_scatter():
        with jax.named_scope('w_gate_scatter'):
            gate_scatter_wait()
        with jax.named_scope('c_gate_scatter'):
            gate_scatter_rest()

    def gate_scatter_wait():
        push(ggpart.at[1 - core], ggpair, twin, 17).wait_recv()

    def gate_scatter_rest():
        gghalf[...] = ggpart[core] + ggpair[...]
        for p in others:
            push(gghalf.at[p // 2], ggrecv.at[chip], p, 10).start()
        ggrecv[pl.ds(chip, 1)] = gghalf[pl.ds(chip, 1)]

    def gate_gather():
        with jax.named_scope('w_gate_gather'):
            gate_gather_wait()
        with jax.named_scope('c_gate_gather'):
            gate_gather_rest()

    def gate_gather_wait():
        wait_recv(ggrecv, 10, 7)

    def gate_gather_rest():
        total = ggrecv[0]
        for i in range(1, 8):
            total = total + ggrecv[i]
        ggall[core, pl.ds(chip, 1)] = total.reshape(1, 64, 128)
        for p in others:
            push(ggall.at[core, chip], ggall.at[core, chip], p, 11).start()
        for c in range(NOW):
            send_now(c)

    phase('p12_bwd')
    def bwd(q, carry):
        for j in range(2):
            e = 2 * (1 - q) + j
            slot = (1 - q) * (2 - 2 * j) + q * (2 - j)
            if j == 0:
                @pl.when(q == 1)
                def _():
                    weight1(0, 2).wait()
                    weight2(0, 2).wait()
            du = dot(dh_v[e], w2[slot], 1, 1).astype(BF).astype(F32)
            if j == 0:
                @pl.when(q == 0)
                def _():
                    weight2(0, 2).start()
            da_v[e] = (gp_v[e] * du).astype(BF)
            if j == 0:
                @pl.when(q == 0)
                def _():
                    send_h(0, 1)
                    send_h(1, 0)

                @pl.when(q == 1)
                def _():
                    send_h(1, 1)
            else:
                pl.when(q == 0)(gate_grads)

        def step(c, carry):
            cols = pl.ds(pl.multiple_of(c * CH, CH), CH)
            outs = []
            for j in range(2):
                slot = (1 - q) * (2 - 2 * j) + q * (2 - j)
                outs.append(dot(da_v[2 * (1 - q) + j], w1[slot, cols, :], 1, 1).reshape(N, 8, CH))
            gsend[1 - q, :, :, cols] = jnp.concatenate(outs, axis=1).astype(BF)
            return carry
        lax.fori_loop(0, NCH, step, 0)

        @pl.when(q == 0)
        def _():
            weight1(0, 2).start()
            gate_scatter()
        return carry
    lax.fori_loop(0, 2, bwd, 0)
    phase('p19_gather')
    gate_gather()
    phase('p12b_later')
    later = [pltpu.make_async_copy(gsend.at[0], glater_out.at[:, :, pl.ds(0, HID)], out_sem.at[5])]
    if NOW < NCH:
        later.append(pltpu.make_async_copy(gsend.at[1, :, :, pl.ds(NOW * CH, HID - NOW * CH)],
                                           glater_out.at[:, :, pl.ds(HID, HID - NOW * CH)], out_sem.at[9]))
    for cp in later:
        cp.start()
    pltpu.make_async_copy(dh_v, dh_out, out_sem.at[2]).start()
    pltpu.make_async_copy(da_v, da_out, out_sem.at[3]).start()

    cp_dlog = pltpu.make_async_copy(dlog_v, dlog_out, out_sem.at[10])
    cp_dlog.start()
    cp_one = pltpu.make_async_copy(one_v, one_out, out_sem.at[11])
    cp_one.start()

    phase('p13_waith')
    wait_h(hrecv, recv_sem)
    wait_send(xsend, 1)

    phase('p15_y')
    def ystep(c, acc):
        cols = pl.ds(pl.multiple_of(c * CH, CH), CH)
        h = hrecv[:, :, :, cols].reshape(512, CH)
        tot = x_v[:, cols].astype(F32) + (dot(c_v[0], h) + dot(c_v[1], h) + dot(c_v[2], h))
        y = tot.astype(BF)
        xsend[:, :, cols] = y.reshape(N, 16, CH)
        return acc + jnp.sum(y.astype(F32) * r_v[:, cols].astype(F32), axis=0, keepdims=True)
    losssend[...] = lax.fori_loop(0, NCH, ystep, jnp.zeros((1, CH), F32))
    cp_y = pltpu.make_async_copy(xsend, y_out, out_sem.at[4])
    cp_y.start()
    for p in peers:
        push(losssend, lossall.at[me], p, 9).start()
    lossall[pl.ds(me, 1)] = losssend[...].reshape(1, 1, CH)

    phase('p20_waitgg')
    wait_recv(ggall.at[core], 11, 7)
    across = push(ggall.at[core], ggall.at[core], twin, 12)
    across.start()
    phase('p21_loss')
    wait_recv(lossall, 9)
    loss_out[0, 0] = jnp.sum(lossall[...]) * scale
    across.wait_recv()
    cp_gg = [pltpu.make_async_copy(ggall.at[i // 8, i % 8], gg_out.at[:, pl.ds(i * 128, 128)], out_sem.at[6]) for i in range(N)]
    for cp in cp_gg:
        cp.start()
    phase('p21b_waitg')
    for c in range(NOW):
        cols = pl.ds(c * CH, CH)
        part = gnow_out.at[pl.ds(0, N - 1), :, cols]
        pltpu.make_async_copy(part, part, recv_sem.at[13 + c]).wait()

    phase('p22_drain')
    wait_send(selall, 0)
    wait_send(gates_all, 2)
    wait_h(hsend, send_sem)
    wait_send(dgall, 8)
    for c in range(NOW):
        cols = pl.ds(c * CH, CH)
        part = gsend.at[1, pl.ds(0, N - 1), :, cols]
        pltpu.make_async_copy(part, part, send_sem.at[13 + c]).wait()
        pltpu.make_async_copy(gsend.at[1, me, :, cols], gnow_out.at[me, :, cols], out_sem.at[12 + c]).wait()
    wait_send(rsend, 3)
    wait_send(lossall, 9)
    push(ggpart.at[1 - core], ggpair, twin, 17).wait_send()
    wait_send(gghalf, 10, 7)
    wait_send(ggall.at[core], 11, 7)
    across.wait_send()
    for cp in later:
        cp.wait()
    cp_dlog.wait()
    cp_one.wait()
    pltpu.make_async_copy(xl_v, xl_out, out_sem.at[0]).wait()
    pltpu.make_async_copy(u_v, u_out, out_sem.at[1]).wait()
    pltpu.make_async_copy(dh_v, dh_out, out_sem.at[2]).wait()
    pltpu.make_async_copy(da_v, da_out, out_sem.at[3]).wait()
    cp_y.wait()
    for cp in cp_gg:
        cp.wait()
    phase(None)


def comm_call(sel, x, gw, up, dn, r, scale):
    any_ = pl.BlockSpec(memory_space=pl.ANY)
    vmem = pl.BlockSpec(memory_space=pltpu.VMEM)
    V = pltpu.VMEM
    shape = jax.ShapeDtypeStruct
    return pl.pallas_call(
        functools.partial(comm_kernel, scale),
        out_shape=[shape((N, 16, HID), BF), shape((N, 16, NOW * CH), BF), shape((N, 16, 2 * HID - NOW * CH), BF), shape((TOK, 512), BF),
                   shape((TOK, 64), BF), shape((64, HID), F32), shape((1, 1), F32),
                   shape((LE, CAP, HID), BF), shape((LE, CAP, FF), BF), shape((LE, CAP, HID), BF), shape((LE, CAP, FF), BF)],
        in_specs=[vmem, any_, any_, any_, any_, any_],
        out_specs=[any_, any_, any_, any_, any_, any_, pl.BlockSpec(memory_space=pltpu.SMEM), any_, any_, any_, any_],
        scratch_shapes=[
            V((TOK, HID), BF), V((TOK, HID), BF), V((64, HID), BF),
            V((3, HID, FF), BF), V((3, FF, HID), BF),
            V((N, 16, HID), BF), V((N, 16, HID), BF), V((N, 16, HID), BF), V((N, 16, HID), BF),
            V((2, N, 16, HID), BF), V((2, N, 16, HID), BF), V((2, N, 16, HID), BF),
            V((LE, CAP, HID), BF), V((LE, CAP, HID), BF), V((LE, CAP, FF), BF), V((LE, CAP, FF), F32), V((LE, CAP, FF), BF),
            V((2, 8, 64, 128), F32), V((8, 64, 128), F32), V((8, 64, 128), F32), V((8, 64, 128), F32), V((2, 8, 64, 128), F32),
            V((8, CAP), jnp.int32), V((N, 8, CAP), jnp.int32), V((1, 512), F32), V((N, 1, 512), F32),
            V((1, CH), F32), V((N, 1, CH), F32), V((N, 8, 128), F32), V((N, 8, 128), F32),
            V((TOK, 512), BF), V((3, TOK, 512), BF), V((LE, CAP, TOK), BF), V((TOK, 64), F32), V((TOK, 64), BF),
            pltpu.SemaphoreType.DMA((3,)), pltpu.SemaphoreType.DMA((2, 3)), pltpu.SemaphoreType.DMA((16,)),
            pltpu.SemaphoreType.DMA((18,)), pltpu.SemaphoreType.DMA((18,)),
        ],
        compiler_params=pltpu.CompilerParams(collective_id=0, has_side_effects=True, vmem_limit_bytes=67043328),
        name='exchange',
    )(sel, x, gw, up, dn, r)


def tile_tools(ins, bufs, outs, tiles, in_sem, out_sem, first):
    def loads(e):
        return [pltpu.make_async_copy(src.at[e], dst.at[e - first], in_sem.at[e - first]) for src, dst in zip(ins, bufs)]

    def stores(i):
        e, c = i // NCH, i % NCH
        cols = pl.ds(pl.multiple_of(c * CH, CH), CH)
        return [pltpu.make_async_copy(tiles[0].at[i - first * NCH], outs[0].at[e, cols, :], out_sem.at[0]),
                pltpu.make_async_copy(tiles[1].at[i - first * NCH], outs[1].at[e, :, cols], out_sem.at[1])]

    def step(i, carry):
        e, c = i // NCH, i % NCH
        xl_v, da_v, u_v, dh_v = bufs
        cols = pl.ds(pl.multiple_of(c * CH, CH), CH)
        tiles[0][i - first * NCH] = dot(xl_v[e - first, :, cols], da_v[e - first], 0, 0).astype(BF)
        tiles[1][i - first * NCH] = dot(u_v[e - first], dh_v[e - first, :, cols], 0, 0).astype(BF)
        for cp in stores(i):
            cp.start()
        return carry

    def finish(i, carry):
        for cp in stores(i):
            cp.wait()
        return carry
    return loads, step, finish


def wgrad1_kernel(xl_in, da_in, u_in, dh_in, y_in, gg_in, loss_in, g1, g2, y, gg, loss,
                  xl_v, da_v, u_v, dh_v, y_v, gg_v, t1, t2, in_sem, out_sem):
    loads, step, finish = tile_tools((xl_in, da_in, u_in, dh_in), (xl_v, da_v, u_v, dh_v), (g1, g2), (t1, t2), in_sem, out_sem, 0)
    cp_y = pltpu.make_async_copy(y_in, y_v, in_sem.at[LE])
    cp_gg = pltpu.make_async_copy(gg_in, gg_v, in_sem.at[LE + 1])
    for cp in loads(0):
        cp.start()
    loss[0, 0] = loss_in[0, 0]

    def expert(e, carry):
        for cp in loads(e):
            cp.wait()

        @pl.when(e + 1 < FIRST)
        def _():
            for cp in loads(e + 1):
                cp.start()

        @pl.when(e == 0)
        def _():
            cp_y.start()
            cp_gg.start()
        lax.fori_loop(e * NCH, (e + 1) * NCH, step, 0)
        return carry
    lax.fori_loop(0, FIRST, expert, 0)
    cp_y.wait()
    cp_gg.wait()
    out_y = pltpu.make_async_copy(y_v, y, in_sem.at[LE])
    out_gg = pltpu.make_async_copy(gg_v, gg, in_sem.at[LE + 1])
    out_y.start()
    out_gg.start()
    out_y.wait()
    out_gg.wait()
    lax.fori_loop(0, FIRST * NCH, finish, 0)


def wgrad1_call(xl, da, u, dh, y, gg, loss):
    shape = jax.ShapeDtypeStruct
    any_ = pl.BlockSpec(memory_space=pl.ANY)
    smem = pl.BlockSpec(memory_space=pltpu.SMEM)
    V = pltpu.VMEM
    return pl.pallas_call(
        wgrad1_kernel,
        in_specs=[any_] * 6 + [smem],
        out_specs=[any_] * 4 + [smem],
        out_shape=[shape((LE, HID, FF), BF), shape((LE, FF, HID), BF), shape((N, 16, HID), BF), shape((64, HID), F32), shape((1, 1), F32)],
        scratch_shapes=[V((FIRST, CAP, HID), BF), V((FIRST, CAP, FF), BF), V((FIRST, CAP, FF), BF), V((FIRST, CAP, HID), BF),
                        V((N, 16, HID), BF), V((64, HID), F32), V((FIRST * NCH, CH, FF), BF), V((FIRST * NCH, FF, CH), BF),
                        pltpu.SemaphoreType.DMA((LE + 2,)), pltpu.SemaphoreType.DMA((2,))],
        compiler_params=pltpu.CompilerParams(vmem_limit_bytes=67043328),
        cost_estimate=pl.CostEstimate(flops=FIRST * 4 * CAP * HID * FF, bytes_accessed=48 * 1024 * 1024, transcendentals=0),
        name='weight_grads_a',
    )(xl, da, u, dh, y, gg, loss)


def gradx_kernel(scale, late_in, now_in, r_in, one_in, dlog_in, gw_in, gx, late_v, now_v, r_v, one_v, dlog_v, gw_v, gx_v, in_sem, out_sem):
    def pieces(c):
        cols = pl.ds(c * CH, CH)
        out = [pltpu.make_async_copy(late_in.at[:, :, cols], late_v.at[:, :, cols], in_sem.at[c])]
        out.append(pltpu.make_async_copy(r_in.at[:, cols], r_v.at[:, cols], in_sem.at[c]))
        if c < NOW:
            out.append(pltpu.make_async_copy(now_in.at[:, :, cols], now_v.at[:, :, cols], in_sem.at[c]))
        else:
            more = pl.ds((NCH + c - NOW) * CH, CH)
            out.append(pltpu.make_async_copy(late_in.at[:, :, more], now_v.at[:, :, cols], in_sem.at[c]))
        return out
    first = [pltpu.make_async_copy(src, dst, in_sem.at[NCH]) for src, dst in ((one_in, one_v), (dlog_in, dlog_v), (gw_in, gw_v))]
    for cp in first:
        cp.start()
    for c in range(NCH):
        for cp in pieces(c):
            cp.start()
    for cp in first:
        cp.wait()
    for c in range(NCH):
        cols = pl.ds(c * CH, CH)
        for cp in pieces(c):
            cp.wait()
        tot = r_v[:, cols].astype(F32) * scale + dot(one_v[:, 0:256], late_v[:, :, cols].reshape(256, CH))
        tot = tot + dot(one_v[:, 256:512], now_v[:, :, cols].reshape(256, CH))
        gx_v[:, cols] = (tot + dot(dlog_v[...], gw_v[:, cols])).astype(BF)
        pltpu.make_async_copy(gx_v.at[:, cols], gx.at[:, cols], out_sem).start()
    for c in range(NCH):
        cols = pl.ds(c * CH, CH)
        pltpu.make_async_copy(gx_v.at[:, cols], gx.at[:, cols], out_sem).wait()


def gradx_call(late, now, r, one, dlog, gw, scale):
    any_ = pl.BlockSpec(memory_space=pl.ANY)
    V = pltpu.VMEM
    return pl.pallas_call(
        functools.partial(gradx_kernel, scale),
        in_specs=[any_] * 6,
        out_specs=any_,
        out_shape=jax.ShapeDtypeStruct((TOK, HID), BF),
        scratch_shapes=[V((N, 16, HID), BF), V((N, 16, HID), BF), V((TOK, HID), BF), V((TOK, 512), BF), V((TOK, 64), BF), V((64, HID), BF),
                        V((TOK, HID), BF), pltpu.SemaphoreType.DMA((NCH + 1,)), pltpu.SemaphoreType.DMA],
        compiler_params=pltpu.CompilerParams(vmem_limit_bytes=67043328),
        name='grad_x',
    )(late, now, r, one, dlog, gw)


def solution(mesh):
    def device_step(x, gate_w, up_w, down_w, expert_picks, loss_w):
        scale = 1.0 / math.sqrt(TOK * N * HID)
        gate_t = gate_w.T
        y, now, later, one, dlog, gg, loss, xl, u, dh, da = comm_call(expert_picks, x, gate_t, up_w, down_w, loss_w, scale)
        later = lax.all_to_all(later, 'ep', 0, 0, tiled=True)
        grad_up, grad_down, y, gg, loss = wgrad1_call(xl, da, u, dh, y, gg, loss)
        grad_x = gradx_call(later, now, loss_w, one, dlog, gate_t, scale)
        return y.reshape(TOK, HID), loss[0, 0], grad_x, grad_up, grad_down, gg.T

    return jax.shard_map(device_step, mesh=mesh,
                         in_specs=(P('ep'), P(), P('ep'), P('ep'), P('ep'), P('ep')),
                         out_specs=(P('ep'), P(), P('ep'), P('ep'), P('ep'), P()),
                         check_vma=False)
```

```python
import functools
import math
import jax
import jax.numpy as jnp
from jax import lax
from jax.experimental import pallas as pl
from jax.experimental.pallas import tpu as pltpu
from jax.sharding import PartitionSpec as P

BF = jnp.bfloat16
F32 = jnp.float32
MESH = pl.DeviceIdType.MESH
N = 16
TOK = 256
LE = 4
CAP = 128
HID = 2048
FF = 1408
CH = 512
NCH = HID // CH
FIRST = 4
HALF = HID // 2
NOW = 2
ORDER = (14, 15, 6, 10, 12, 7, 11, 13, 2, 4, 8, 3, 5, 9, 1)


def dot(a, b, ca=1, cb=0):
    return lax.dot_general(a, b, (((ca,), (cb,)), ((), ())), preferred_element_type=F32)


def iota(shape, dim):
    return lax.broadcasted_iota(jnp.int32, shape, dim)


def ones_where(cond):
    return jnp.where(cond, 1.0, 0.0).astype(BF)


def split3(v):
    hi = v.astype(BF)
    rest = v - hi.astype(F32)
    mid = rest.astype(BF)
    low = (rest - mid.astype(F32)).astype(BF)
    return hi, mid, low


def flip(me, k):
    out = 0
    for b in range(4):
        bit = (me // (1 << b)) % 2
        if (k >> b) & 1:
            bit = 1 - bit
        out = out + bit * (1 << b)
    return out


def comm_kernel(scale, sel_ref, x_hbm, gw_hbm, up_hbm, dn_hbm, r_hbm,
                y_out, gnow_out, glater_out, one_out, dlog_out, gg_out, loss_out, xl_out, u_out, dh_out, da_out,
                x_v, r_v, gw_v, w1, w2, xsend, rsend, xrecv, rrecv, hsend, hrecv, gsend,
                xl_v, dh_v, u_v, gp_v, da_v, ggpart, ggpair, gghalf, ggrecv, ggall, selsend, selall, gates, gates_all,
                losssend, lossall, dgsend, dgall, one_v, c_v, e_v, probs_v, dlog_v,
                ld_sem, w_sem, out_sem, send_sem, recv_sem):
    open_ = []

    def phase(name):
        if open_:
            open_.pop().__exit__(None, None, None)
        if name:
            open_.append(jax.named_scope(name))
            open_[-1].__enter__()
    me = lax.axis_index('ep')
    peers = [flip(me, k) for k in ORDER]
    core, chip, twin = me % 2, me // 2, flip(me, 1)
    others = [flip(me, k) for k in ORDER if k % 2 == 0]

    def load(src, dst, i):
        return pltpu.make_async_copy(src, dst, ld_sem.at[i])

    def weight1(e, slot):
        return pltpu.make_async_copy(up_hbm.at[e], w1.at[slot], w_sem.at[0, slot])

    def weight2(e, slot):
        return pltpu.make_async_copy(dn_hbm.at[e], w2.at[slot], w_sem.at[1, slot])

    def push(src, dst, peer, i):
        return pltpu.make_async_remote_copy(src_ref=src, dst_ref=dst, send_sem=send_sem.at[i], recv_sem=recv_sem.at[i],
                                            device_id=(peer,), device_id_type=MESH)

    def wait_recv(buf, i, n=N - 1):
        part = buf.at[pl.ds(0, n)]
        pltpu.make_async_copy(part, part, recv_sem.at[i]).wait()

    def wait_send(buf, i, n=N - 1):
        part = buf.at[pl.ds(0, n)]
        pltpu.make_async_copy(part, part, send_sem.at[i]).wait()

    phase('p00_start')
    cp_x = load(x_hbm, x_v, 0)
    cp_g = load(gw_hbm, gw_v, 1)
    cp_r = load(r_hbm, r_v, 2)
    cp_x.start()
    cp_g.start()
    cp_r.start()

    sel = sel_ref[...]
    selsend[...] = jnp.zeros_like(selsend)
    selsend[0:LE, :] = sel
    selall[pl.ds(me, 1)] = selsend[...].reshape(1, 8, CAP)

    phase('p01_barrier')
    barrier = pltpu.get_barrier_semaphore()
    for p in peers:
        pl.semaphore_signal(barrier, inc=1, device_id=(p,), device_id_type=MESH)
    pl.semaphore_wait(barrier, N - 1)

    for p in peers:
        push(selsend, selall.at[me], p, 0).start()
    for e in range(3):
        weight1(e, e).start()
        weight2(e, e).start()

    phase('p02_logits')
    cp_g.wait()
    cp_x.wait()
    logits = dot(x_v[...], gw_v[...], 1, 1)
    ex = jnp.exp(logits - jnp.max(logits, axis=1, keepdims=True))
    probs = ex / jnp.sum(ex, axis=1, keepdims=True)
    probs_v[...] = probs

    phase('p03_ownpicks')
    below = ones_where(iota((TOK, TOK), 1) < iota((TOK, TOK), 0))
    slot_lane = (iota((TOK, TOK), 1) % 16).astype(F32)

    tok_row = iota((TOK, CAP), 0)
    same = iota((CAP, TOK), 0) // 8 == iota((CAP, TOK), 1) // 16
    fold = ones_where(same)
    base = (iota((1, CAP), 1) // 8) * TOK
    hits = [ones_where(tok_row == sel[l:l + 1, :] - base) for l in range(LE)]
    count = dot(hits[0], fold)
    for l in range(1, LE):
        count = count + dot(hits[l], fold)
    pres = count > 0.5
    rank = dot(below, ones_where(pres))
    pick_of = jnp.where(pres, jnp.where(rank == slot_lane, 1.0, 0.0), 0.0).astype(BF)
    for l in range(LE):
        e_v[l] = jnp.where(same, dot(hits[l], pick_of, 0, 0), 0.0).astype(BF)

    phase('p04_waitsel')
    place = ones_where(iota((CAP, 512), 0) % 8 == iota((CAP, 512), 1) % 8)
    fold2 = ones_where((iota((512, TOK), 0) % 256) // 16 == iota((512, TOK), 1) // 16)
    for_wait = selall.at[pl.ds(0, N - 1)]
    pltpu.make_async_copy(for_wait, for_wait, recv_sem.at[0]).wait()
    phase('p05_give')
    everyone = selall[...].reshape(8 * N, CAP)
    mine = jnp.where(iota((8 * N, CAP), 1) // 8 == me, everyone - me * TOK, 0).astype(F32).astype(BF)
    spread = dot(mine, place)
    lane = iota((8 * N, 512), 1)
    want = ((lane % 256) // 16) * 8 + 2 * (lane // 256) + (lane % 16) // 8
    ids = jnp.sum(jnp.where(iota((8 * N, 512), 0) == want, spread, 0.0), axis=0, keepdims=True)
    one = jnp.where(iota((TOK, 512), 0).astype(F32) == ids, 1.0, 0.0)
    one_v[...] = one.astype(BF)
    pres2 = dot(one_v[...], fold2) > 0.5
    rank2 = dot(below, ones_where(pres2))
    give = jnp.where(pres2, jnp.where(rank2 == slot_lane, 1.0, 0.0), 0.0).astype(BF)
    give_t = give.T

    def gather(src, dst):
        def step(c, carry):
            cols = pl.ds(pl.multiple_of(c * CH, CH), CH)
            dst[:, :, cols] = dot(give_t, src[:, cols]).astype(BF).reshape(N, 16, CH)
            return carry
        lax.fori_loop(0, NCH, step, 0)

    phase('p06_gatherx')
    for c in range(NCH):
        cols = pl.ds(c * CH, CH)
        xsend[:, :, cols] = dot(give_t, x_v[:, cols]).astype(BF).reshape(N, 16, CH)
        for p in peers:
            push(xsend.at[p, :, cols], xrecv.at[me, :, cols], p, 1).start()
    xrecv[pl.ds(me, 1)] = xsend[pl.ds(me, 1)]

    phase('p07_gates')
    rep = ones_where(iota((64, 512), 0) == 4 * ((iota((64, 512), 1) % 256) // 16) + 2 * (iota((64, 512), 1) // 256)
                     + (iota((64, 512), 1) % 16) // 8)
    wide = 0.0
    for term in split3(probs_v[...]):
        wide = wide + dot(term, rep)
    comb = wide * one
    for i, term in enumerate(split3(comb)):
        c_v[i] = term
    gates[...] = jnp.sum(comb, axis=0, keepdims=True)
    for p in peers:
        push(gates, gates_all.at[me], p, 2).start()
    gates_all[pl.ds(me, 1)] = gates[...].reshape(1, 1, 512)

    phase('p08_gatherr')
    cp_r.wait()
    gather(r_v, rsend)
    for p in peers:
        push(rsend.at[p], rrecv.at[me], p, 3).start()
    rrecv[pl.ds(me, 1)] = rsend[pl.ds(me, 1)]

    phase('p09_waitx')
    wait_recv(xrecv, 1)

    def send_h(q, half):
        cols = pl.ds(half * HALF, HALF)
        for p in peers:
            push(hsend.at[q, p, :, cols], hrecv.at[q, me, :, cols], p, 4 + 2 * q + half).start()

    def wait_h(buf, sem):
        for q in range(2):
            for half in range(2):
                part = buf.at[q, pl.ds(0, N - 1), :, pl.ds(half * HALF, HALF)]
                pltpu.make_async_copy(part, part, sem.at[4 + 2 * q + half]).wait()

    phase('p10_fwd')
    def fwd(q, carry):
        for j in range(2):
            e = 2 * q + j
            slot = e % 3
            xl = dot(e_v[e], xrecv[...].reshape(TOK, HID)).astype(BF)
            xl_v[e] = xl
            weight1(e, slot).wait()
            a = dot(xl_v[e], w1[slot])
            if j == 0:
                @pl.when(q == 0)
                def _():
                    weight1(3, 0).start()
            k0 = math.sqrt(2.0 / math.pi)
            t = jnp.tanh(k0 * (a + 0.044715 * (a * a * a)))
            u_v[e] = (0.5 * a * (1.0 + t)).astype(BF)
            gp_v[e] = 0.5 * (1.0 + t) + 0.5 * a * (1.0 - t * t) * (k0 * (1.0 + 3.0 * 0.044715 * (a * a)))
        weight2(2 * q, (2 * q) % 3).wait()
        weight2(2 * q + 1, (2 * q + 1) % 3).wait()

        def step(c, carry):
            cols = pl.ds(pl.multiple_of(c * CH, CH), CH)
            outs = [dot(u_v[2 * q + j], w2[(2 * q + j) % 3, :, cols]).reshape(N, 8, CH) for j in range(2)]
            hsend[q, :, :, cols] = jnp.concatenate(outs, axis=1).astype(BF)
            return carry
        lax.fori_loop(0, NCH, step, 0)

        @pl.when(q == 0)
        def _():
            weight2(3, 0).start()
        hrecv[q, pl.ds(me, 1)] = hsend[q, pl.ds(me, 1)]

        @pl.when(q == 0)
        def _():
            send_h(0, 0)
        return carry
    lax.fori_loop(0, 2, fwd, 0)
    pltpu.make_async_copy(xl_v, xl_out, out_sem.at[0]).start()
    pltpu.make_async_copy(u_v, u_out, out_sem.at[1]).start()

    phase('p11_waitr')
    wait_recv(gates_all, 2)
    wait_recv(rrecv, 3)

    def send_now(c):
        cols = pl.ds(c * CH, CH)
        for p in peers:
            push(gsend.at[1, p, :, cols], gnow_out.at[me, :, cols], p, 13 + c).start()
        pltpu.make_async_copy(gsend.at[1, me, :, cols], gnow_out.at[me, :, cols], out_sem.at[12 + c]).start()

    phase('p11b_pre')
    lane128 = iota((CAP, 128), 1)
    rows = jnp.broadcast_to(gates_all[...], (N, 8, 512)).reshape(CAP, 512)

    def pre(q, table):
        for j in range(2):
            e = 2 * q + j
            here = iota((CAP, 512), 1) == q * 256 + me * 16 + j * 8 + iota((CAP, 512), 0) % 8
            gcol = jnp.sum(jnp.where(here, rows, 0.0), axis=1, keepdims=True)

            def rstep(c, acc):
                cols = pl.ds(pl.multiple_of(c * CH, CH), CH)
                rl = dot(e_v[e], rrecv[:, :, cols].reshape(TOK, CH))
                dh_v[e, :, cols] = (gcol * (rl * scale)).astype(BF)
                hj = hsend[q, :, :, cols].astype(F32)[:, 8 * j:8 * j + 8, :].reshape(CAP, CH)
                prod = rl * hj
                return acc + ((prod[:, 0:128] + prod[:, 128:256]) + (prod[:, 256:384] + prod[:, 384:512]))
            acc = lax.fori_loop(0, NCH, rstep, jnp.zeros((CAP, 128), F32))
            table = table + jnp.where(lane128 == e, jnp.sum(acc, axis=1, keepdims=True) * scale, 0.0)
        return table
    dgsend[...] = lax.fori_loop(0, 2, pre, jnp.zeros((CAP, 128), F32)).reshape(N, 8, 128)
    for p in peers:
        push(dgsend.at[p], dgall.at[me], p, 8).start()
    dgall[pl.ds(me, 1)] = dgsend[pl.ds(me, 1)]
    send_h(0, 1)
    send_h(1, 0)

    def gate_grads():
        with jax.named_scope('w_gate_grads'):
            gate_grads_wait()
        with jax.named_scope('c_gate_grads'):
            gate_grads_rest()

    def gate_grads_wait():
        wait_recv(dgall, 8)

    def gate_grads_rest():
        mine_of = []
        for l in range(LE):
            col = jnp.sum(jnp.where(iota((N, 8, 128), 2) == l, dgall[...], 0.0), axis=2, keepdims=True).reshape(CAP, 1)
            mine_of.append(jnp.where(iota((CAP, 64), 1) == 4 * (iota((CAP, 64), 0) // 8) + l, col, 0.0).reshape(N, 8, 64))
        spread_g = jnp.concatenate([jnp.concatenate(mine_of[2 * q:2 * q + 2], axis=1).reshape(256, 64) for q in range(2)], axis=0)
        ds = 0.0
        for term in split3(spread_g):
            ds = ds + dot(one_v[...], term)
        probs = probs_v[...]
        dlog = (probs * (ds - jnp.sum(probs * ds, axis=1, keepdims=True))).astype(BF)
        dlog_v[...] = dlog
        dlog_t = dlog.astype(F32).T.astype(BF)
        for c in range(NCH):
            part = dot(dlog_t, x_v[:, c * CH:(c + 1) * CH])
            for i in range(CH // 128):
                ggpart[c // 2, (c % 2) * (CH // 128) + i] = part[:, i * 128:(i + 1) * 128]
        push(ggpart.at[1 - core], ggpair, twin, 17).start()

    def gate_scatter():
        with jax.named_scope('w_gate_scatter'):
            gate_scatter_wait()
        with jax.named_scope('c_gate_scatter'):
            gate_scatter_rest()

    def gate_scatter_wait():
        push(ggpart.at[1 - core], ggpair, twin, 17).wait_recv()

    def gate_scatter_rest():
        gghalf[...] = ggpart[core] + ggpair[...]
        for p in others:
            push(gghalf.at[p // 2], ggrecv.at[chip], p, 10).start()
        ggrecv[pl.ds(chip, 1)] = gghalf[pl.ds(chip, 1)]
        send_h(1, 1)

    def gate_gather():
        with jax.named_scope('w_gate_gather'):
            gate_gather_wait()
        with jax.named_scope('c_gate_gather'):
            gate_gather_rest()

    def gate_gather_wait():
        wait_recv(ggrecv, 10, 7)

    def gate_gather_rest():
        total = ggrecv[0]
        for i in range(1, 8):
            total = total + ggrecv[i]
        ggall[core, pl.ds(chip, 1)] = total.reshape(1, 64, 128)
        for p in others:
            push(ggall.at[core, chip], ggall.at[core, chip], p, 11).start()
        for c in range(NOW):
            send_now(c)

    phase('p12_bwd')
    def bwd(q, carry):
        for j in range(2):
            e = (1 - q) * (2 + j) + q * (1 - j)
            slot = (1 - q) * (2 - 2 * j) + q * (1 + j)
            if j == 1:
                @pl.when(q == 1)
                def _():
                    weight2(0, 2).wait()
            du = dot(dh_v[e], w2[slot], 1, 1).astype(BF).astype(F32)
            da_v[e] = (gp_v[e] * du).astype(BF)
            if j == 0:
                @pl.when(q == 0)
                def _():
                    weight2(0, 2).start()
                pl.when(q == 1)(gate_scatter)

        @pl.when(q == 1)
        def _():
            weight1(0, 2).wait()

        def step(c, carry):
            cols = pl.ds(pl.multiple_of(c * CH, CH), CH)
            outs = []
            for j in range(2):
                slot = (1 - q) * (2 - 2 * j) + q * (2 - j)
                outs.append(dot(da_v[2 * (1 - q) + j], w1[slot, cols, :], 1, 1).reshape(N, 8, CH))
            gsend[1 - q, :, :, cols] = jnp.concatenate(outs, axis=1).astype(BF)
            return carry
        lax.fori_loop(0, NCH, step, 0)

        @pl.when(q == 0)
        def _():
            weight1(0, 2).start()
            gate_grads()
        return carry
    lax.fori_loop(0, 2, bwd, 0)
    phase('p19_gather')
    gate_gather()
    phase('p12b_later')
    later = [pltpu.make_async_copy(gsend.at[0], glater_out.at[:, :, pl.ds(0, HID)], out_sem.at[5])]
    if NOW < NCH:
        later.append(pltpu.make_async_copy(gsend.at[1, :, :, pl.ds(NOW * CH, HID - NOW * CH)],
                                           glater_out.at[:, :, pl.ds(HID, HID - NOW * CH)], out_sem.at[9]))
    for cp in later:
        cp.start()
    pltpu.make_async_copy(dh_v, dh_out, out_sem.at[2]).start()
    pltpu.make_async_copy(da_v, da_out, out_sem.at[3]).start()

    cp_dlog = pltpu.make_async_copy(dlog_v, dlog_out, out_sem.at[10])
    cp_dlog.start()
    cp_one = pltpu.make_async_copy(one_v, one_out, out_sem.at[11])
    cp_one.start()

    phase('p13_waith')
    wait_h(hrecv, recv_sem)
    wait_send(xsend, 1)

    phase('p15_y')
    def ystep(c, acc):
        cols = pl.ds(pl.multiple_of(c * CH, CH), CH)
        h = hrecv[:, :, :, cols].reshape(512, CH)
        tot = x_v[:, cols].astype(F32) + (dot(c_v[0], h) + dot(c_v[1], h) + dot(c_v[2], h))
        y = tot.astype(BF)
        xsend[:, :, cols] = y.reshape(N, 16, CH)
        return acc + jnp.sum(y.astype(F32) * r_v[:, cols].astype(F32), axis=0, keepdims=True)
    losssend[...] = lax.fori_loop(0, NCH, ystep, jnp.zeros((1, CH), F32))
    cp_y = pltpu.make_async_copy(xsend, y_out, out_sem.at[4])
    cp_y.start()
    for p in peers:
        push(losssend, lossall.at[me], p, 9).start()
    lossall[pl.ds(me, 1)] = losssend[...].reshape(1, 1, CH)

    phase('p20_waitgg')
    wait_recv(ggall.at[core], 11, 7)
    across = push(ggall.at[core], ggall.at[core], twin, 12)
    across.start()
    phase('p21_loss')
    wait_recv(lossall, 9)
    loss_out[0, 0] = jnp.sum(lossall[...]) * scale
    across.wait_recv()
    cp_gg = [pltpu.make_async_copy(ggall.at[i // 8, i % 8], gg_out.at[:, pl.ds(i * 128, 128)], out_sem.at[6]) for i in range(N)]
    for cp in cp_gg:
        cp.start()
    phase('p21b_waitg')
    for c in range(NOW):
        cols = pl.ds(c * CH, CH)
        part = gnow_out.at[pl.ds(0, N - 1), :, cols]
        pltpu.make_async_copy(part, part, recv_sem.at[13 + c]).wait()

    phase('p22_drain')
    wait_send(selall, 0)
    wait_send(gates_all, 2)
    wait_h(hsend, send_sem)
    wait_send(dgall, 8)
    for c in range(NOW):
        cols = pl.ds(c * CH, CH)
        part = gsend.at[1, pl.ds(0, N - 1), :, cols]
        pltpu.make_async_copy(part, part, send_sem.at[13 + c]).wait()
        pltpu.make_async_copy(gsend.at[1, me, :, cols], gnow_out.at[me, :, cols], out_sem.at[12 + c]).wait()
    wait_send(rsend, 3)
    wait_send(lossall, 9)
    push(ggpart.at[1 - core], ggpair, twin, 17).wait_send()
    wait_send(gghalf, 10, 7)
    wait_send(ggall.at[core], 11, 7)
    across.wait_send()
    for cp in later:
        cp.wait()
    cp_dlog.wait()
    cp_one.wait()
    pltpu.make_async_copy(xl_v, xl_out, out_sem.at[0]).wait()
    pltpu.make_async_copy(u_v, u_out, out_sem.at[1]).wait()
    pltpu.make_async_copy(dh_v, dh_out, out_sem.at[2]).wait()
    pltpu.make_async_copy(da_v, da_out, out_sem.at[3]).wait()
    cp_y.wait()
    for cp in cp_gg:
        cp.wait()
    phase(None)


def comm_call(sel, x, gw, up, dn, r, scale):
    any_ = pl.BlockSpec(memory_space=pl.ANY)
    vmem = pl.BlockSpec(memory_space=pltpu.VMEM)
    V = pltpu.VMEM
    shape = jax.ShapeDtypeStruct
    return pl.pallas_call(
        functools.partial(comm_kernel, scale),
        out_shape=[shape((N, 16, HID), BF), shape((N, 16, NOW * CH), BF), shape((N, 16, 2 * HID - NOW * CH), BF), shape((TOK, 512), BF),
                   shape((TOK, 64), BF), shape((64, HID), F32), shape((1, 1), F32),
                   shape((LE, CAP, HID), BF), shape((LE, CAP, FF), BF), shape((LE, CAP, HID), BF), shape((LE, CAP, FF), BF)],
        in_specs=[vmem, any_, any_, any_, any_, any_],
        out_specs=[any_, any_, any_, any_, any_, any_, pl.BlockSpec(memory_space=pltpu.SMEM), any_, any_, any_, any_],
        scratch_shapes=[
            V((TOK, HID), BF), V((TOK, HID), BF), V((64, HID), BF),
            V((3, HID, FF), BF), V((3, FF, HID), BF),
            V((N, 16, HID), BF), V((N, 16, HID), BF), V((N, 16, HID), BF), V((N, 16, HID), BF),
            V((2, N, 16, HID), BF), V((2, N, 16, HID), BF), V((2, N, 16, HID), BF),
            V((LE, CAP, HID), BF), V((LE, CAP, HID), BF), V((LE, CAP, FF), BF), V((LE, CAP, FF), F32), V((LE, CAP, FF), BF),
            V((2, 8, 64, 128), F32), V((8, 64, 128), F32), V((8, 64, 128), F32), V((8, 64, 128), F32), V((2, 8, 64, 128), F32),
            V((8, CAP), jnp.int32), V((N, 8, CAP), jnp.int32), V((1, 512), F32), V((N, 1, 512), F32),
            V((1, CH), F32), V((N, 1, CH), F32), V((N, 8, 128), F32), V((N, 8, 128), F32),
            V((TOK, 512), BF), V((3, TOK, 512), BF), V((LE, CAP, TOK), BF), V((TOK, 64), F32), V((TOK, 64), BF),
            pltpu.SemaphoreType.DMA((3,)), pltpu.SemaphoreType.DMA((2, 3)), pltpu.SemaphoreType.DMA((16,)),
            pltpu.SemaphoreType.DMA((18,)), pltpu.SemaphoreType.DMA((18,)),
        ],
        compiler_params=pltpu.CompilerParams(collective_id=0, has_side_effects=True, vmem_limit_bytes=67043328),
        name='exchange',
    )(sel, x, gw, up, dn, r)


def tile_tools(ins, bufs, outs, tiles, in_sem, out_sem, first):
    def loads(e):
        return [pltpu.make_async_copy(src.at[e], dst.at[e - first], in_sem.at[e - first]) for src, dst in zip(ins, bufs)]

    def stores(i):
        e, c = i // NCH, i % NCH
        cols = pl.ds(pl.multiple_of(c * CH, CH), CH)
        return [pltpu.make_async_copy(tiles[0].at[i - first * NCH], outs[0].at[e, cols, :], out_sem.at[0]),
                pltpu.make_async_copy(tiles[1].at[i - first * NCH], outs[1].at[e, :, cols], out_sem.at[1])]

    def step(i, carry):
        e, c = i // NCH, i % NCH
        xl_v, da_v, u_v, dh_v = bufs
        cols = pl.ds(pl.multiple_of(c * CH, CH), CH)
        tiles[0][i - first * NCH] = dot(xl_v[e - first, :, cols], da_v[e - first], 0, 0).astype(BF)
        tiles[1][i - first * NCH] = dot(u_v[e - first], dh_v[e - first, :, cols], 0, 0).astype(BF)
        for cp in stores(i):
            cp.start()
        return carry

    def finish(i, carry):
        for cp in stores(i):
            cp.wait()
        return carry
    return loads, step, finish


def wgrad1_kernel(xl_in, da_in, u_in, dh_in, y_in, gg_in, loss_in, g1, g2, y, gg, loss,
                  xl_v, da_v, u_v, dh_v, y_v, gg_v, t1, t2, in_sem, out_sem):
    loads, step, finish = tile_tools((xl_in, da_in, u_in, dh_in), (xl_v, da_v, u_v, dh_v), (g1, g2), (t1, t2), in_sem, out_sem, 0)
    cp_y = pltpu.make_async_copy(y_in, y_v, in_sem.at[LE])
    cp_gg = pltpu.make_async_copy(gg_in, gg_v, in_sem.at[LE + 1])
    for cp in loads(0):
        cp.start()
    loss[0, 0] = loss_in[0, 0]

    def expert(e, carry):
        for cp in loads(e):
            cp.wait()

        @pl.when(e + 1 < FIRST)
        def _():
            for cp in loads(e + 1):
                cp.start()

        @pl.when(e == 0)
        def _():
            cp_y.start()
            cp_gg.start()
        lax.fori_loop(e * NCH, (e + 1) * NCH, step, 0)
        return carry
    lax.fori_loop(0, FIRST, expert, 0)
    cp_y.wait()
    cp_gg.wait()
    out_y = pltpu.make_async_copy(y_v, y, in_sem.at[LE])
    out_gg = pltpu.make_async_copy(gg_v, gg, in_sem.at[LE + 1])
    out_y.start()
    out_gg.start()
    out_y.wait()
    out_gg.wait()
    lax.fori_loop(0, FIRST * NCH, finish, 0)


def wgrad1_call(xl, da, u, dh, y, gg, loss):
    shape = jax.ShapeDtypeStruct
    any_ = pl.BlockSpec(memory_space=pl.ANY)
    smem = pl.BlockSpec(memory_space=pltpu.SMEM)
    V = pltpu.VMEM
    return pl.pallas_call(
        wgrad1_kernel,
        in_specs=[any_] * 6 + [smem],
        out_specs=[any_] * 4 + [smem],
        out_shape=[shape((LE, HID, FF), BF), shape((LE, FF, HID), BF), shape((N, 16, HID), BF), shape((64, HID), F32), shape((1, 1), F32)],
        scratch_shapes=[V((FIRST, CAP, HID), BF), V((FIRST, CAP, FF), BF), V((FIRST, CAP, FF), BF), V((FIRST, CAP, HID), BF),
                        V((N, 16, HID), BF), V((64, HID), F32), V((FIRST * NCH, CH, FF), BF), V((FIRST * NCH, FF, CH), BF),
                        pltpu.SemaphoreType.DMA((LE + 2,)), pltpu.SemaphoreType.DMA((2,))],
        compiler_params=pltpu.CompilerParams(vmem_limit_bytes=67043328),
        cost_estimate=pl.CostEstimate(flops=FIRST * 4 * CAP * HID * FF, bytes_accessed=48 * 1024 * 1024, transcendentals=0),
        name='weight_grads_a',
    )(xl, da, u, dh, y, gg, loss)


def gradx_kernel(scale, late_in, now_in, r_in, one_in, dlog_in, gw_in, gx, late_v, now_v, r_v, one_v, dlog_v, gw_v, gx_v, in_sem, out_sem):
    def pieces(c):
        cols = pl.ds(c * CH, CH)
        out = [pltpu.make_async_copy(late_in.at[:, :, cols], late_v.at[:, :, cols], in_sem.at[c])]
        out.append(pltpu.make_async_copy(r_in.at[:, cols], r_v.at[:, cols], in_sem.at[c]))
        if c < NOW:
            out.append(pltpu.make_async_copy(now_in.at[:, :, cols], now_v.at[:, :, cols], in_sem.at[c]))
        else:
            more = pl.ds((NCH + c - NOW) * CH, CH)
            out.append(pltpu.make_async_copy(late_in.at[:, :, more], now_v.at[:, :, cols], in_sem.at[c]))
        return out
    first = [pltpu.make_async_copy(src, dst, in_sem.at[NCH]) for src, dst in ((one_in, one_v), (dlog_in, dlog_v), (gw_in, gw_v))]
    for cp in first:
        cp.start()
    for c in range(NCH):
        for cp in pieces(c):
            cp.start()
    for cp in first:
        cp.wait()
    for c in range(NCH):
        cols = pl.ds(c * CH, CH)
        for cp in pieces(c):
            cp.wait()
        tot = r_v[:, cols].astype(F32) * scale + dot(one_v[:, 0:256], late_v[:, :, cols].reshape(256, CH))
        tot = tot + dot(one_v[:, 256:512], now_v[:, :, cols].reshape(256, CH))
        gx_v[:, cols] = (tot + dot(dlog_v[...], gw_v[:, cols])).astype(BF)
        pltpu.make_async_copy(gx_v.at[:, cols], gx.at[:, cols], out_sem).start()
    for c in range(NCH):
        cols = pl.ds(c * CH, CH)
        pltpu.make_async_copy(gx_v.at[:, cols], gx.at[:, cols], out_sem).wait()


def gradx_call(late, now, r, one, dlog, gw, scale):
    any_ = pl.BlockSpec(memory_space=pl.ANY)
    V = pltpu.VMEM
    return pl.pallas_call(
        functools.partial(gradx_kernel, scale),
        in_specs=[any_] * 6,
        out_specs=any_,
        out_shape=jax.ShapeDtypeStruct((TOK, HID), BF),
        scratch_shapes=[V((N, 16, HID), BF), V((N, 16, HID), BF), V((TOK, HID), BF), V((TOK, 512), BF), V((TOK, 64), BF), V((64, HID), BF),
                        V((TOK, HID), BF), pltpu.SemaphoreType.DMA((NCH + 1,)), pltpu.SemaphoreType.DMA],
        compiler_params=pltpu.CompilerParams(vmem_limit_bytes=67043328),
        name='grad_x',
    )(late, now, r, one, dlog, gw)


def solution(mesh):
    def device_step(x, gate_w, up_w, down_w, expert_picks, loss_w):
        scale = 1.0 / math.sqrt(TOK * N * HID)
        gate_t = gate_w.T
        y, now, later, one, dlog, gg, loss, xl, u, dh, da = comm_call(expert_picks, x, gate_t, up_w, down_w, loss_w, scale)
        later = lax.all_to_all(later, 'ep', 0, 0, tiled=True)
        grad_up, grad_down, y, gg, loss = wgrad1_call(xl, da, u, dh, y, gg, loss)
        grad_x = gradx_call(later, now, loss_w, one, dlog, gate_t, scale)
        return y.reshape(TOK, HID), loss[0, 0], grad_x, grad_up, grad_down, gg.T

    return jax.shard_map(device_step, mesh=mesh,
                         in_specs=(P('ep'), P(), P('ep'), P('ep'), P('ep'), P('ep')),
                         out_specs=(P('ep'), P(), P('ep'), P('ep'), P('ep'), P()),
                         check_vma=False)
```

```python
import functools
import math
import jax
import jax.numpy as jnp
from jax import lax
from jax.experimental import pallas as pl
from jax.experimental.pallas import tpu as pltpu
from jax.sharding import PartitionSpec as P

BF = jnp.bfloat16
F32 = jnp.float32
MESH = pl.DeviceIdType.MESH
N = 16
TOK = 256
LE = 4
CAP = 128
HID = 2048
FF = 1408
CH = 512
NCH = HID // CH
FIRST = 4
HALF = HID // 2
NOW = 2
ORDER = (14, 15, 6, 10, 12, 7, 11, 13, 2, 4, 8, 3, 5, 9, 1)


def dot(a, b, ca=1, cb=0):
    return lax.dot_general(a, b, (((ca,), (cb,)), ((), ())), preferred_element_type=F32)


def iota(shape, dim):
    return lax.broadcasted_iota(jnp.int32, shape, dim)


def ones_where(cond):
    return jnp.where(cond, 1.0, 0.0).astype(BF)


def split3(v):
    hi = v.astype(BF)
    rest = v - hi.astype(F32)
    mid = rest.astype(BF)
    low = (rest - mid.astype(F32)).astype(BF)
    return hi, mid, low


def flip(me, k):
    out = 0
    for b in range(4):
        bit = (me // (1 << b)) % 2
        if (k >> b) & 1:
            bit = 1 - bit
        out = out + bit * (1 << b)
    return out


def comm_kernel(scale, sel_ref, x_hbm, gw_hbm, up_hbm, dn_hbm, r_hbm,
                y_out, gnow_out, glater_out, one_out, dlog_out, gg_out, loss_out, xl_out, u_out, dh_out, da_out,
                x_v, r_v, gw_v, w1, w2, xsend, rsend, xrecv, rrecv, hsend, hrecv, gsend,
                xl_v, dh_v, u_v, gp_v, da_v, ggpart, ggpair, gghalf, ggrecv, ggall, selsend, selall, gates, gates_all,
                losssend, lossall, dgsend, dgall, one_v, c_v, e_v, probs_v, dlog_v,
                ld_sem, w_sem, out_sem, send_sem, recv_sem):
    open_ = []

    def phase(name):
        if open_:
            open_.pop().__exit__(None, None, None)
        if name:
            open_.append(jax.named_scope(name))
            open_[-1].__enter__()
    me = lax.axis_index('ep')
    peers = [flip(me, k) for k in ORDER]
    core, chip, twin = me % 2, me // 2, flip(me, 1)
    others = [flip(me, k) for k in ORDER if k % 2 == 0]

    def load(src, dst, i):
        return pltpu.make_async_copy(src, dst, ld_sem.at[i])

    def weight1(e, slot):
        return pltpu.make_async_copy(up_hbm.at[e], w1.at[slot], w_sem.at[0, slot])

    def weight2(e, slot):
        return pltpu.make_async_copy(dn_hbm.at[e], w2.at[slot], w_sem.at[1, slot])

    def push(src, dst, peer, i):
        return pltpu.make_async_remote_copy(src_ref=src, dst_ref=dst, send_sem=send_sem.at[0 if i == 1 else 1], recv_sem=recv_sem.at[i],
                                            device_id=(peer,), device_id_type=MESH)

    def wait_recv(buf, i, n=N - 1):
        part = buf.at[pl.ds(0, n)]
        pltpu.make_async_copy(part, part, recv_sem.at[i]).wait()

    def wait_send(buf, i, n=N - 1):
        part = buf.at[pl.ds(0, n)]
        pltpu.make_async_copy(part, part, send_sem.at[0 if i == 1 else 1]).wait()

    phase('p00_start')
    cp_x = load(x_hbm, x_v, 0)
    cp_g = load(gw_hbm, gw_v, 0)
    cp_r = load(r_hbm, r_v, 1)
    cp_x.start()
    cp_g.start()
    cp_r.start()

    sel = sel_ref[...]
    selsend[...] = jnp.zeros_like(selsend)
    selsend[0:LE, :] = sel
    selall[pl.ds(me, 1)] = selsend[...].reshape(1, 8, CAP)

    phase('p01_barrier')
    barrier = pltpu.get_barrier_semaphore()
    for p in peers:
        pl.semaphore_signal(barrier, inc=1, device_id=(p,), device_id_type=MESH)
    pl.semaphore_wait(barrier, N - 1)

    for p in peers:
        push(selsend, selall.at[me], p, 0).start()
    for e in range(3):
        weight1(e, e).start()
        weight2(e, e).start()

    phase('p02_logits')
    cp_g.wait()
    cp_x.wait()
    logits = dot(x_v[...], gw_v[...], 1, 1)
    ex = jnp.exp(logits - jnp.max(logits, axis=1, keepdims=True))
    probs = ex / jnp.sum(ex, axis=1, keepdims=True)
    probs_v[...] = probs

    phase('p03_ownpicks')
    below = ones_where(iota((TOK, TOK), 1) < iota((TOK, TOK), 0))
    slot_lane = (iota((TOK, TOK), 1) % 16).astype(F32)

    tok_row = iota((TOK, CAP), 0)
    same = iota((CAP, TOK), 0) // 8 == iota((CAP, TOK), 1) // 16
    fold = ones_where(same)
    base = (iota((1, CAP), 1) // 8) * TOK
    hits = [ones_where(tok_row == sel[l:l + 1, :] - base) for l in range(LE)]
    count = dot(hits[0], fold)
    for l in range(1, LE):
        count = count + dot(hits[l], fold)
    pres = count > 0.5
    rank = dot(below, ones_where(pres))
    pick_of = jnp.where(pres, jnp.where(rank == slot_lane, 1.0, 0.0), 0.0).astype(BF)
    for l in range(LE):
        e_v[l] = jnp.where(same, dot(hits[l], pick_of, 0, 0), 0.0).astype(BF)

    phase('p04_waitsel')
    place = ones_where(iota((CAP, 512), 0) % 8 == iota((CAP, 512), 1) % 8)
    fold2 = ones_where((iota((512, TOK), 0) % 256) // 16 == iota((512, TOK), 1) // 16)
    for_wait = selall.at[pl.ds(0, N - 1)]
    pltpu.make_async_copy(for_wait, for_wait, recv_sem.at[0]).wait()
    phase('p05_give')
    everyone = selall[...].reshape(8 * N, CAP)
    mine = jnp.where(iota((8 * N, CAP), 1) // 8 == me, everyone - me * TOK, 0).astype(F32).astype(BF)
    spread = dot(mine, place)
    lane = iota((8 * N, 512), 1)
    want = ((lane % 256) // 16) * 8 + 2 * (lane // 256) + (lane % 16) // 8
    ids = jnp.sum(jnp.where(iota((8 * N, 512), 0) == want, spread, 0.0), axis=0, keepdims=True)
    one = jnp.where(iota((TOK, 512), 0).astype(F32) == ids, 1.0, 0.0)
    one_v[...] = one.astype(BF)
    pres2 = dot(one_v[...], fold2) > 0.5
    rank2 = dot(below, ones_where(pres2))
    give = jnp.where(pres2, jnp.where(rank2 == slot_lane, 1.0, 0.0), 0.0).astype(BF)
    give_t = give.T

    def gather(src, dst):
        def step(c, carry):
            cols = pl.ds(pl.multiple_of(c * CH, CH), CH)
            dst[:, :, cols] = dot(give_t, src[:, cols]).astype(BF).reshape(N, 16, CH)
            return carry
        lax.fori_loop(0, NCH, step, 0)

    phase('p06_gatherx')
    for c in range(NCH):
        cols = pl.ds(c * CH, CH)
        xsend[:, :, cols] = dot(give_t, x_v[:, cols]).astype(BF).reshape(N, 16, CH)
        for p in peers:
            push(xsend.at[p, :, cols], xrecv.at[me, :, cols], p, 1).start()
    xrecv[pl.ds(me, 1)] = xsend[pl.ds(me, 1)]

    phase('p07_gates')
    rep = ones_where(iota((64, 512), 0) == 4 * ((iota((64, 512), 1) % 256) // 16) + 2 * (iota((64, 512), 1) // 256)
                     + (iota((64, 512), 1) % 16) // 8)
    wide = 0.0
    for term in split3(probs_v[...]):
        wide = wide + dot(term, rep)
    comb = wide * one
    for i, term in enumerate(split3(comb)):
        c_v[i] = term
    gates[...] = jnp.sum(comb, axis=0, keepdims=True)
    for p in peers:
        push(gates, gates_all.at[me], p, 2).start()
    gates_all[pl.ds(me, 1)] = gates[...].reshape(1, 1, 512)

    phase('p08_gatherr')
    cp_r.wait()
    gather(r_v, rsend)
    for p in peers:
        push(rsend.at[p], rrecv.at[me], p, 3).start()
    rrecv[pl.ds(me, 1)] = rsend[pl.ds(me, 1)]

    phase('p09_waitx')
    wait_recv(xrecv, 1)

    def send_h(q, half):
        cols = pl.ds(half * HALF, HALF)
        for p in peers:
            push(hsend.at[q, p, :, cols], hrecv.at[q, me, :, cols], p, 4).start()

    def wait_h(buf, sem):
        part = buf.at[:, pl.ds(0, N - 1)]
        pltpu.make_async_copy(part, part, sem).wait()

    phase('p10_fwd')
    def fwd(q, carry):
        for j in range(2):
            e = 2 * q + j
            slot = e % 3
            xl = dot(e_v[e], xrecv[...].reshape(TOK, HID)).astype(BF)
            xl_v[e] = xl
            weight1(e, slot).wait()
            a = dot(xl_v[e], w1[slot])
            if j == 0:
                @pl.when(q == 0)
                def _():
                    weight1(3, 0).start()
            k0 = math.sqrt(2.0 / math.pi)
            t = jnp.tanh(k0 * (a + 0.044715 * (a * a * a)))
            u_v[e] = (0.5 * a * (1.0 + t)).astype(BF)
            gp_v[e] = 0.5 * (1.0 + t) + 0.5 * a * (1.0 - t * t) * (k0 * (1.0 + 3.0 * 0.044715 * (a * a)))
        weight2(2 * q, (2 * q) % 3).wait()
        weight2(2 * q + 1, (2 * q + 1) % 3).wait()

        def step(c, carry):
            cols = pl.ds(pl.multiple_of(c * CH, CH), CH)
            outs = [dot(u_v[2 * q + j], w2[(2 * q + j) % 3, :, cols]).reshape(N, 8, CH) for j in range(2)]
            hsend[q, :, :, cols] = jnp.concatenate(outs, axis=1).astype(BF)
            return carry
        lax.fori_loop(0, NCH, step, 0)

        @pl.when(q == 0)
        def _():
            weight2(3, 0).start()
        hrecv[q, pl.ds(me, 1)] = hsend[q, pl.ds(me, 1)]

        @pl.when(q == 0)
        def _():
            send_h(0, 0)
        return carry
    lax.fori_loop(0, 2, fwd, 0)
    pltpu.make_async_copy(xl_v, xl_out, out_sem.at[0]).start()
    pltpu.make_async_copy(u_v, u_out, out_sem.at[0]).start()

    phase('p11_waitr')
    wait_recv(gates_all, 2)
    wait_recv(rrecv, 3)

    def send_now(c):
        cols = pl.ds(c * CH, CH)
        for p in peers:
            push(gsend.at[1, p, :, cols], gnow_out.at[me, :, cols], p, 5).start()
        pltpu.make_async_copy(gsend.at[1, me, :, cols], gnow_out.at[me, :, cols], out_sem.at[0]).start()

    phase('p11b_pre')
    lane128 = iota((CAP, 128), 1)
    rows = jnp.broadcast_to(gates_all[...], (N, 8, 512)).reshape(CAP, 512)

    def pre(q, table):
        gcol = []
        for j in range(2):
            here = iota((CAP, 512), 1) == q * 256 + me * 16 + j * 8 + iota((CAP, 512), 0) % 8
            gcol.append(jnp.sum(jnp.where(here, rows, 0.0), axis=1, keepdims=True))

        def rstep(c, acc):
            cols = pl.ds(pl.multiple_of(c * CH, CH), CH)
            rall = rrecv[:, :, cols].reshape(TOK, CH)
            hall = hsend[q, :, :, cols].astype(F32)
            out = []
            for j in range(2):
                rl = dot(e_v[2 * q + j], rall)
                dh_v[2 * q + j, :, cols] = (gcol[j] * (rl * scale)).astype(BF)
                prod = rl * hall[:, 8 * j:8 * j + 8, :].reshape(CAP, CH)
                out.append(acc[j] + ((prod[:, 0:128] + prod[:, 128:256]) + (prod[:, 256:384] + prod[:, 384:512])))
            return tuple(out)
        zero = jnp.zeros((CAP, 128), F32)
        acc = lax.fori_loop(0, NCH, rstep, (zero, zero))
        for j in range(2):
            table = table + jnp.where(lane128 == 2 * q + j, jnp.sum(acc[j], axis=1, keepdims=True) * scale, 0.0)
        return table
    dgsend[...] = lax.fori_loop(0, 2, pre, jnp.zeros((CAP, 128), F32)).reshape(N, 8, 128)
    for p in peers:
        push(dgsend.at[p], dgall.at[me], p, 6).start()
    dgall[pl.ds(me, 1)] = dgsend[pl.ds(me, 1)]
    send_h(0, 1)
    send_h(1, 0)

    def gate_grads():
        with jax.named_scope('w_gate_grads'):
            gate_grads_wait()
        with jax.named_scope('c_gate_grads'):
            gate_grads_rest()

    def gate_grads_wait():
        wait_recv(dgall, 6)

    def gate_grads_rest():
        mine_of = []
        for l in range(LE):
            col = jnp.sum(jnp.where(iota((N, 8, 128), 2) == l, dgall[...], 0.0), axis=2, keepdims=True).reshape(CAP, 1)
            mine_of.append(jnp.where(iota((CAP, 64), 1) == 4 * (iota((CAP, 64), 0) // 8) + l, col, 0.0).reshape(N, 8, 64))
        spread_g = jnp.concatenate([jnp.concatenate(mine_of[2 * q:2 * q + 2], axis=1).reshape(256, 64) for q in range(2)], axis=0)
        ds = 0.0
        for term in split3(spread_g):
            ds = ds + dot(one_v[...], term)
        probs = probs_v[...]
        dlog = (probs * (ds - jnp.sum(probs * ds, axis=1, keepdims=True))).astype(BF)
        dlog_v[...] = dlog
        dlog_t = dlog.astype(F32).T.astype(BF)
        for c in range(NCH):
            part = dot(dlog_t, x_v[:, c * CH:(c + 1) * CH])
            for i in range(CH // 128):
                ggpart[c // 2, (c % 2) * (CH // 128) + i] = part[:, i * 128:(i + 1) * 128]
        push(ggpart.at[1 - core], ggpair, twin, 8).start()

    def gate_scatter():
        with jax.named_scope('w_gate_scatter'):
            gate_scatter_wait()
        with jax.named_scope('c_gate_scatter'):
            gate_scatter_rest()

    def gate_scatter_wait():
        push(ggpart.at[1 - core], ggpair, twin, 8).wait_recv()

    def gate_scatter_rest():
        gghalf[...] = ggpart[core] + ggpair[...]
        for p in others:
            push(gghalf.at[p // 2], ggrecv.at[chip], p, 9).start()
        ggrecv[pl.ds(chip, 1)] = gghalf[pl.ds(chip, 1)]
        send_now(0)

    def gate_gather():
        with jax.named_scope('w_gate_gather'):
            gate_gather_wait()
        with jax.named_scope('c_gate_gather'):
            gate_gather_rest()

    def gate_gather_wait():
        wait_recv(ggrecv, 9, 7)

    def gate_gather_rest():
        total = ggrecv[0]
        for i in range(1, 8):
            total = total + ggrecv[i]
        ggall[core, pl.ds(chip, 1)] = total.reshape(1, 64, 128)
        for p in others:
            push(ggall.at[core, chip], ggall.at[core, chip], p, 10).start()
        for c in range(1, NOW):
            send_now(c)

    phase('p12_bwd')
    def bwd(q, carry):
        for j in range(2):
            e = (1 - q) * (2 + j) + q * (1 - j)
            slot = (1 - q) * (2 - 2 * j) + q * (1 + j)
            if j == 1:
                @pl.when(q == 1)
                def _():
                    weight2(0, 2).wait()
            du = dot(dh_v[e], w2[slot], 1, 1).astype(BF).astype(F32)
            da_v[e] = (gp_v[e] * du).astype(BF)
            if j == 0:
                @pl.when(q == 0)
                def _():
                    weight2(0, 2).start()

        @pl.when(q == 1)
        def _():
            gate_scatter()
            weight1(0, 2).wait()

        def step(c, carry):
            cols = pl.ds(pl.multiple_of(c * CH, CH), CH)
            outs = []
            for j in range(2):
                slot = (1 - q) * (2 - 2 * j) + q * (2 - j)
                outs.append(dot(da_v[2 * (1 - q) + j], w1[slot, cols, :], 1, 1).reshape(N, 8, CH))
            gsend[1 - q, :, :, cols] = jnp.concatenate(outs, axis=1).astype(BF)
            return carry
        lax.fori_loop(0, NCH, step, 0)

        @pl.when(q == 0)
        def _():
            weight1(0, 2).start()
            gate_grads()
            send_h(1, 1)
        return carry
    lax.fori_loop(0, 2, bwd, 0)
    phase('p12b_later')
    later = [pltpu.make_async_copy(gsend.at[0], glater_out.at[:, :, pl.ds(0, HID)], out_sem.at[0])]
    if NOW < NCH:
        later.append(pltpu.make_async_copy(gsend.at[1, :, :, pl.ds(NOW * CH, HID - NOW * CH)],
                                           glater_out.at[:, :, pl.ds(HID, HID - NOW * CH)], out_sem.at[0]))
    for cp in later:
        cp.start()
    pltpu.make_async_copy(dh_v, dh_out, out_sem.at[0]).start()
    pltpu.make_async_copy(da_v, da_out, out_sem.at[0]).start()

    cp_dlog = pltpu.make_async_copy(dlog_v, dlog_out, out_sem.at[0])
    cp_dlog.start()
    cp_one = pltpu.make_async_copy(one_v, one_out, out_sem.at[0])
    cp_one.start()

    phase('p13_waith')
    wait_h(hrecv, recv_sem.at[4])
    wait_send(xsend, 1)

    phase('p15_y')
    def ystep(c, acc):
        cols = pl.ds(pl.multiple_of(c * CH, CH), CH)
        h = hrecv[:, :, :, cols].reshape(512, CH)
        tot = x_v[:, cols].astype(F32) + (dot(c_v[0], h) + dot(c_v[1], h) + dot(c_v[2], h))
        y = tot.astype(BF)
        xsend[:, :, cols] = y.reshape(N, 16, CH)
        return acc + jnp.sum(y.astype(F32) * r_v[:, cols].astype(F32), axis=0, keepdims=True)
    losssend[...] = lax.fori_loop(0, NCH, ystep, jnp.zeros((1, CH), F32))
    cp_y = pltpu.make_async_copy(xsend, y_out, out_sem.at[0])
    cp_y.start()
    for p in peers:
        push(losssend, lossall.at[me], p, 7).start()
    lossall[pl.ds(me, 1)] = losssend[...].reshape(1, 1, CH)
    phase('p19_gather')
    gate_gather()

    phase('p20_waitgg')
    wait_recv(ggall.at[core], 10, 7)
    across = push(ggall.at[core], ggall.at[core], twin, 11)
    across.start()
    across.wait_recv()
    cp_gg = [pltpu.make_async_copy(ggall.at[i // 8, i % 8], gg_out.at[:, pl.ds(i * 128, 128)], out_sem.at[0]) for i in range(N)]
    for cp in cp_gg:
        cp.start()
    phase('p21_loss')
    wait_recv(lossall, 7)
    loss_out[0, 0] = jnp.sum(lossall[...]) * scale
    phase('p21b_waitg')
    wait_recv(gnow_out, 5)

    phase('p22_drain')
    wait_send(selall, 0)
    wait_send(gates_all, 2)
    wait_h(hsend, send_sem.at[1])
    wait_send(dgall, 6)
    part = gsend.at[1, pl.ds(0, N - 1), :, pl.ds(0, NOW * CH)]
    pltpu.make_async_copy(part, part, send_sem.at[1]).wait()
    for c in range(NOW):
        cols = pl.ds(c * CH, CH)
        pltpu.make_async_copy(gsend.at[1, me, :, cols], gnow_out.at[me, :, cols], out_sem.at[0]).wait()
    wait_send(rsend, 3)
    wait_send(lossall, 7)
    push(ggpart.at[1 - core], ggpair, twin, 8).wait_send()
    wait_send(gghalf, 9, 7)
    wait_send(ggall.at[core], 10, 7)
    across.wait_send()
    for cp in later:
        cp.wait()
    cp_dlog.wait()
    cp_one.wait()
    pltpu.make_async_copy(xl_v, xl_out, out_sem.at[0]).wait()
    pltpu.make_async_copy(u_v, u_out, out_sem.at[0]).wait()
    pltpu.make_async_copy(dh_v, dh_out, out_sem.at[0]).wait()
    pltpu.make_async_copy(da_v, da_out, out_sem.at[0]).wait()
    cp_y.wait()
    for cp in cp_gg:
        cp.wait()
    phase(None)


def comm_call(sel, x, gw, up, dn, r, scale):
    any_ = pl.BlockSpec(memory_space=pl.ANY)
    vmem = pl.BlockSpec(memory_space=pltpu.VMEM)
    V = pltpu.VMEM
    shape = jax.ShapeDtypeStruct
    return pl.pallas_call(
        functools.partial(comm_kernel, scale),
        out_shape=[shape((N, 16, HID), BF), shape((N, 16, NOW * CH), BF), shape((N, 16, 2 * HID - NOW * CH), BF), shape((TOK, 512), BF),
                   shape((TOK, 64), BF), shape((64, HID), F32), shape((1, 1), F32),
                   shape((LE, CAP, HID), BF), shape((LE, CAP, FF), BF), shape((LE, CAP, HID), BF), shape((LE, CAP, FF), BF)],
        in_specs=[vmem, any_, any_, any_, any_, any_],
        out_specs=[any_, any_, any_, any_, any_, any_, pl.BlockSpec(memory_space=pltpu.SMEM), any_, any_, any_, any_],
        scratch_shapes=[
            V((TOK, HID), BF), V((TOK, HID), BF), V((64, HID), BF),
            V((3, HID, FF), BF), V((3, FF, HID), BF),
            V((N, 16, HID), BF), V((N, 16, HID), BF), V((N, 16, HID), BF), V((N, 16, HID), BF),
            V((2, N, 16, HID), BF), V((2, N, 16, HID), BF), V((2, N, 16, HID), BF),
            V((LE, CAP, HID), BF), V((LE, CAP, HID), BF), V((LE, CAP, FF), BF), V((LE, CAP, FF), F32), V((LE, CAP, FF), BF),
            V((2, 8, 64, 128), F32), V((8, 64, 128), F32), V((8, 64, 128), F32), V((8, 64, 128), F32), V((2, 8, 64, 128), F32),
            V((8, CAP), jnp.int32), V((N, 8, CAP), jnp.int32), V((1, 512), F32), V((N, 1, 512), F32),
            V((1, CH), F32), V((N, 1, CH), F32), V((N, 8, 128), F32), V((N, 8, 128), F32),
            V((TOK, 512), BF), V((3, TOK, 512), BF), V((LE, CAP, TOK), BF), V((TOK, 64), F32), V((TOK, 64), BF),
            pltpu.SemaphoreType.DMA((2,)), pltpu.SemaphoreType.DMA((2, 3)), pltpu.SemaphoreType.DMA((1,)),
            pltpu.SemaphoreType.DMA((2,)), pltpu.SemaphoreType.DMA((12,)),
        ],
        compiler_params=pltpu.CompilerParams(collective_id=0, has_side_effects=True, vmem_limit_bytes=67043328),
        name='exchange',
    )(sel, x, gw, up, dn, r)


def tile_tools(ins, bufs, outs, tiles, in_sem, out_sem, first):
    def loads(e):
        return [pltpu.make_async_copy(src.at[e], dst.at[e - first], in_sem.at[e - first]) for src, dst in zip(ins, bufs)]

    def stores(i):
        e, c = i // NCH, i % NCH
        cols = pl.ds(pl.multiple_of(c * CH, CH), CH)
        return [pltpu.make_async_copy(tiles[0].at[i - first * NCH], outs[0].at[e, cols, :], out_sem.at[0]),
                pltpu.make_async_copy(tiles[1].at[i - first * NCH], outs[1].at[e, :, cols], out_sem.at[1])]

    def step(i, carry):
        e, c = i // NCH, i % NCH
        xl_v, da_v, u_v, dh_v = bufs
        cols = pl.ds(pl.multiple_of(c * CH, CH), CH)
        tiles[0][i - first * NCH] = dot(xl_v[e - first, :, cols], da_v[e - first], 0, 0).astype(BF)
        tiles[1][i - first * NCH] = dot(u_v[e - first], dh_v[e - first, :, cols], 0, 0).astype(BF)
        for cp in stores(i):
            cp.start()
        return carry

    def finish(i, carry):
        for cp in stores(i):
            cp.wait()
        return carry
    return loads, step, finish


def wgrad1_kernel(xl_in, da_in, u_in, dh_in, y_in, gg_in, loss_in, g1, g2, y, gg, loss,
                  xl_v, da_v, u_v, dh_v, y_v, gg_v, t1, t2, in_sem, out_sem):
    loads, step, finish = tile_tools((xl_in, da_in, u_in, dh_in), (xl_v, da_v, u_v, dh_v), (g1, g2), (t1, t2), in_sem, out_sem, 0)
    cp_y = pltpu.make_async_copy(y_in, y_v, in_sem.at[LE])
    cp_gg = pltpu.make_async_copy(gg_in, gg_v, in_sem.at[LE + 1])
    for cp in loads(0):
        cp.start()
    loss[0, 0] = loss_in[0, 0]

    def expert(e, carry):
        for cp in loads(e):
            cp.wait()

        @pl.when(e + 1 < FIRST)
        def _():
            for cp in loads(e + 1):
                cp.start()

        @pl.when(e == 0)
        def _():
            cp_y.start()
            cp_gg.start()
        lax.fori_loop(e * NCH, (e + 1) * NCH, step, 0)
        return carry
    lax.fori_loop(0, FIRST, expert, 0)
    cp_y.wait()
    cp_gg.wait()
    out_y = pltpu.make_async_copy(y_v, y, in_sem.at[LE])
    out_gg = pltpu.make_async_copy(gg_v, gg, in_sem.at[LE + 1])
    out_y.start()
    out_gg.start()
    out_y.wait()
    out_gg.wait()
    lax.fori_loop(0, FIRST * NCH, finish, 0)


def wgrad1_call(xl, da, u, dh, y, gg, loss):
    shape = jax.ShapeDtypeStruct
    any_ = pl.BlockSpec(memory_space=pl.ANY)
    smem = pl.BlockSpec(memory_space=pltpu.SMEM)
    V = pltpu.VMEM
    return pl.pallas_call(
        wgrad1_kernel,
        in_specs=[any_] * 6 + [smem],
        out_specs=[any_] * 4 + [smem],
        out_shape=[shape((LE, HID, FF), BF), shape((LE, FF, HID), BF), shape((N, 16, HID), BF), shape((64, HID), F32), shape((1, 1), F32)],
        scratch_shapes=[V((FIRST, CAP, HID), BF), V((FIRST, CAP, FF), BF), V((FIRST, CAP, FF), BF), V((FIRST, CAP, HID), BF),
                        V((N, 16, HID), BF), V((64, HID), F32), V((FIRST * NCH, CH, FF), BF), V((FIRST * NCH, FF, CH), BF),
                        pltpu.SemaphoreType.DMA((LE + 2,)), pltpu.SemaphoreType.DMA((2,))],
        compiler_params=pltpu.CompilerParams(vmem_limit_bytes=67043328),
        cost_estimate=pl.CostEstimate(flops=FIRST * 4 * CAP * HID * FF, bytes_accessed=48 * 1024 * 1024, transcendentals=0),
        name='weight_grads_a',
    )(xl, da, u, dh, y, gg, loss)


def gradx_kernel(scale, late_in, now_in, r_in, one_in, dlog_in, gw_in, gx, late_v, now_v, r_v, one_v, dlog_v, gw_v, gx_v, in_sem, out_sem):
    def pieces(c):
        cols = pl.ds(c * CH, CH)
        out = [pltpu.make_async_copy(late_in.at[:, :, cols], late_v.at[:, :, cols], in_sem.at[c])]
        out.append(pltpu.make_async_copy(r_in.at[:, cols], r_v.at[:, cols], in_sem.at[c]))
        if c < NOW:
            out.append(pltpu.make_async_copy(now_in.at[:, :, cols], now_v.at[:, :, cols], in_sem.at[c]))
        else:
            more = pl.ds((NCH + c - NOW) * CH, CH)
            out.append(pltpu.make_async_copy(late_in.at[:, :, more], now_v.at[:, :, cols], in_sem.at[c]))
        return out
    first = [pltpu.make_async_copy(src, dst, in_sem.at[NCH]) for src, dst in ((one_in, one_v), (dlog_in, dlog_v), (gw_in, gw_v))]
    for cp in first:
        cp.start()
    for c in range(NCH):
        for cp in pieces(c):
            cp.start()
    for cp in first:
        cp.wait()
    for c in range(NCH):
        cols = pl.ds(c * CH, CH)
        for cp in pieces(c):
            cp.wait()
        tot = r_v[:, cols].astype(F32) * scale + dot(one_v[:, 0:256], late_v[:, :, cols].reshape(256, CH))
        tot = tot + dot(one_v[:, 256:512], now_v[:, :, cols].reshape(256, CH))
        gx_v[:, cols] = (tot + dot(dlog_v[...], gw_v[:, cols])).astype(BF)
        pltpu.make_async_copy(gx_v.at[:, cols], gx.at[:, cols], out_sem).start()
    for c in range(NCH):
        cols = pl.ds(c * CH, CH)
        pltpu.make_async_copy(gx_v.at[:, cols], gx.at[:, cols], out_sem).wait()


def gradx_call(late, now, r, one, dlog, gw, scale):
    any_ = pl.BlockSpec(memory_space=pl.ANY)
    V = pltpu.VMEM
    return pl.pallas_call(
        functools.partial(gradx_kernel, scale),
        in_specs=[any_] * 6,
        out_specs=any_,
        out_shape=jax.ShapeDtypeStruct((TOK, HID), BF),
        scratch_shapes=[V((N, 16, HID), BF), V((N, 16, HID), BF), V((TOK, HID), BF), V((TOK, 512), BF), V((TOK, 64), BF), V((64, HID), BF),
                        V((TOK, HID), BF), pltpu.SemaphoreType.DMA((NCH + 1,)), pltpu.SemaphoreType.DMA],
        compiler_params=pltpu.CompilerParams(vmem_limit_bytes=67043328),
        name='grad_x',
    )(late, now, r, one, dlog, gw)


def solution(mesh):
    def device_step(x, gate_w, up_w, down_w, expert_picks, loss_w):
        scale = 1.0 / math.sqrt(TOK * N * HID)
        gate_t = gate_w.T
        y, now, later, one, dlog, gg, loss, xl, u, dh, da = comm_call(expert_picks, x, gate_t, up_w, down_w, loss_w, scale)
        later = lax.all_to_all(later, 'ep', 0, 0, tiled=True)
        grad_up, grad_down, y, gg, loss = wgrad1_call(xl, da, u, dh, y, gg, loss)
        grad_x = gradx_call(later, now, loss_w, one, dlog, gate_t, scale)
        return y.reshape(TOK, HID), loss[0, 0], grad_x, grad_up, grad_down, gg.T

    return jax.shard_map(device_step, mesh=mesh,
                         in_specs=(P('ep'), P(), P('ep'), P('ep'), P('ep'), P('ep')),
                         out_specs=(P('ep'), P(), P('ep'), P('ep'), P('ep'), P()),
                         check_vma=False)
```

```python
import functools
import math
import jax
import jax.numpy as jnp
from jax import lax
from jax.experimental import pallas as pl
from jax.experimental.pallas import tpu as pltpu
from jax.sharding import PartitionSpec as P

BF = jnp.bfloat16
F32 = jnp.float32
MESH = pl.DeviceIdType.MESH
N = 16
TOK = 256
LE = 4
CAP = 128
HID = 2048
FF = 1408
CH = 512
NCH = HID // CH
FIRST = 4
HALF = HID // 2
NOW = 2
ORDER = (14, 15, 6, 10, 12, 7, 11, 13, 2, 4, 8, 3, 5, 9, 1)


def dot(a, b, ca=1, cb=0):
    return lax.dot_general(a, b, (((ca,), (cb,)), ((), ())), preferred_element_type=F32)


def iota(shape, dim):
    return lax.broadcasted_iota(jnp.int32, shape, dim)


def ones_where(cond):
    return jnp.where(cond, 1.0, 0.0).astype(BF)


def split3(v):
    hi = v.astype(BF)
    rest = v - hi.astype(F32)
    mid = rest.astype(BF)
    low = (rest - mid.astype(F32)).astype(BF)
    return hi, mid, low


def flip(me, k):
    out = 0
    for b in range(4):
        bit = (me // (1 << b)) % 2
        if (k >> b) & 1:
            bit = 1 - bit
        out = out + bit * (1 << b)
    return out


def comm_kernel(scale, sel_ref, x_hbm, gw_hbm, up_hbm, dn_hbm, r_hbm,
                y_out, gnow_out, glater_out, tab_out, gg_out, loss_out, xl_out, u_out, dh_out, da_out,
                x_v, r_v, gw_v, w1, w2, xsend, rsend, xrecv, rrecv, hsend, hrecv, gsend,
                xl_v, dh_v, u_v, gp_v, da_v, ggpart, ggpair, gghalf, ggrecv, ggall, selsend, selall, gates, gates_all,
                losssend, lossall, dgsend, dgall, one_v, c_v, e_v, probs_v, dlog_v,
                ld_sem, w_sem, out_sem, send_sem, recv_sem):
    me = lax.axis_index('ep')
    peers = [flip(me, k) for k in ORDER]
    core, chip, twin = me % 2, me // 2, flip(me, 1)
    others = [flip(me, k) for k in ORDER if k % 2 == 0]

    def load(src, dst, i):
        return pltpu.make_async_copy(src, dst, ld_sem.at[i])

    def weight1(e, slot):
        return pltpu.make_async_copy(up_hbm.at[e], w1.at[slot], w_sem.at[0, slot])

    def weight2(e, slot):
        return pltpu.make_async_copy(dn_hbm.at[e], w2.at[slot], w_sem.at[1, slot])

    def push(src, dst, peer, i):
        return pltpu.make_async_remote_copy(src_ref=src, dst_ref=dst, send_sem=send_sem.at[0 if i == 1 else 1], recv_sem=recv_sem.at[i],
                                            device_id=(peer,), device_id_type=MESH)

    def wait_recv(buf, i, n=N - 1):
        part = buf.at[pl.ds(0, n)]
        pltpu.make_async_copy(part, part, recv_sem.at[i]).wait()

    def wait_send(buf, i, n=N - 1):
        part = buf.at[pl.ds(0, n)]
        pltpu.make_async_copy(part, part, send_sem.at[0 if i == 1 else 1]).wait()

    cp_x = load(x_hbm, x_v, 0)
    cp_g = load(gw_hbm, gw_v, 0)
    cp_r = load(r_hbm, r_v, 1)
    cp_x.start()
    cp_g.start()
    cp_r.start()

    sel = sel_ref[...]
    selsend[...] = jnp.zeros_like(selsend)
    selsend[0:LE, :] = sel
    selall[pl.ds(me, 1)] = selsend[...].reshape(1, 8, CAP)

    barrier = pltpu.get_barrier_semaphore()
    for p in peers:
        pl.semaphore_signal(barrier, inc=1, device_id=(p,), device_id_type=MESH)
    pl.semaphore_wait(barrier, N - 1)

    for p in peers:
        push(selsend, selall.at[me], p, 0).start()
    for e in range(3):
        weight1(e, e).start()
        weight2(e, e).start()

    cp_g.wait()
    cp_x.wait()
    logits = dot(x_v[...], gw_v[...], 1, 1)
    ex = jnp.exp(logits - jnp.max(logits, axis=1, keepdims=True))
    probs = ex / jnp.sum(ex, axis=1, keepdims=True)
    probs_v[...] = probs

    below = ones_where(iota((TOK, TOK), 1) < iota((TOK, TOK), 0))
    slot_lane = (iota((TOK, TOK), 1) % 16).astype(F32)

    tok_row = iota((TOK, CAP), 0)
    same = iota((CAP, TOK), 0) // 8 == iota((CAP, TOK), 1) // 16
    fold = ones_where(same)
    base = (iota((1, CAP), 1) // 8) * TOK
    hits = [ones_where(tok_row == sel[l:l + 1, :] - base) for l in range(LE)]
    count = dot(hits[0], fold)
    for l in range(1, LE):
        count = count + dot(hits[l], fold)
    pres = count > 0.5
    rank = dot(below, ones_where(pres))
    pick_of = jnp.where(pres, jnp.where(rank == slot_lane, 1.0, 0.0), 0.0).astype(BF)
    for l in range(LE):
        e_v[l] = jnp.where(same, dot(hits[l], pick_of, 0, 0), 0.0).astype(BF)

    place = ones_where(iota((CAP, 512), 0) % 8 == iota((CAP, 512), 1) % 8)
    fold2 = ones_where((iota((512, TOK), 0) % 256) // 16 == iota((512, TOK), 1) // 16)
    for_wait = selall.at[pl.ds(0, N - 1)]
    pltpu.make_async_copy(for_wait, for_wait, recv_sem.at[0]).wait()
    everyone = selall[...].reshape(8 * N, CAP)
    mine = jnp.where(iota((8 * N, CAP), 1) // 8 == me, everyone - me * TOK, 0).astype(F32).astype(BF)
    spread = dot(mine, place)
    lane = iota((8 * N, 512), 1)
    want = ((lane % 256) // 16) * 8 + 2 * (lane // 256) + (lane % 16) // 8
    ids = jnp.sum(jnp.where(iota((8 * N, 512), 0) == want, spread, 0.0), axis=0, keepdims=True)
    one = jnp.where(iota((TOK, 512), 0).astype(F32) == ids, 1.0, 0.0)
    one_v[...] = one.astype(BF)
    pres2 = dot(one_v[...], fold2) > 0.5
    rank2 = dot(below, ones_where(pres2))
    give = jnp.where(pres2, jnp.where(rank2 == slot_lane, 1.0, 0.0), 0.0).astype(BF)
    give_t = give.T

    def gather(src, dst):
        def step(c, carry):
            cols = pl.ds(pl.multiple_of(c * CH, CH), CH)
            dst[:, :, cols] = dot(give_t, src[:, cols]).astype(BF).reshape(N, 16, CH)
            return carry
        lax.fori_loop(0, NCH, step, 0)

    for c in range(NCH):
        cols = pl.ds(c * CH, CH)
        xsend[:, :, cols] = dot(give_t, x_v[:, cols]).astype(BF).reshape(N, 16, CH)
        for p in peers:
            push(xsend.at[p, :, cols], xrecv.at[me, :, cols], p, 1).start()
    xrecv[pl.ds(me, 1)] = xsend[pl.ds(me, 1)]

    rep = ones_where(iota((64, 512), 0) == 4 * ((iota((64, 512), 1) % 256) // 16) + 2 * (iota((64, 512), 1) // 256)
                     + (iota((64, 512), 1) % 16) // 8)
    wide = 0.0
    for term in split3(probs_v[...]):
        wide = wide + dot(term, rep)
    comb = wide * one
    for i, term in enumerate(split3(comb)):
        c_v[i] = term
    gates[...] = jnp.sum(comb, axis=0, keepdims=True)
    for p in peers:
        push(gates, gates_all.at[me], p, 2).start()
    gates_all[pl.ds(me, 1)] = gates[...].reshape(1, 1, 512)

    cp_r.wait()
    gather(r_v, rsend)
    for p in peers:
        push(rsend.at[p], rrecv.at[me], p, 3).start()
    rrecv[pl.ds(me, 1)] = rsend[pl.ds(me, 1)]

    wait_recv(xrecv, 1)

    def send_h(q, start, width):
        cols = pl.ds(start, width)
        for p in peers:
            push(hsend.at[q, p, :, cols], hrecv.at[q, me, :, cols], p, 4).start()

    def wait_h(buf, sem):
        part = buf.at[:, pl.ds(0, N - 1)]
        pltpu.make_async_copy(part, part, sem).wait()

    def fwd(q, carry):
        for j in range(2):
            e = 2 * q + j
            slot = e % 3
            xl = dot(e_v[e], xrecv[...].reshape(TOK, HID)).astype(BF)
            xl_v[e] = xl
            weight1(e, slot).wait()
            a = dot(xl_v[e], w1[slot])
            if j == 0:
                @pl.when(q == 0)
                def _():
                    weight1(3, 0).start()
            k0 = math.sqrt(2.0 / math.pi)
            t = jnp.tanh(k0 * (a + 0.044715 * (a * a * a)))
            u_v[e] = (0.5 * a * (1.0 + t)).astype(BF)
            gp_v[e] = 0.5 * (1.0 + t) + 0.5 * a * (1.0 - t * t) * (k0 * (1.0 + 3.0 * 0.044715 * (a * a)))
        weight2(2 * q, (2 * q) % 3).wait()
        weight2(2 * q + 1, (2 * q + 1) % 3).wait()

        def step(c, carry):
            cols = pl.ds(pl.multiple_of(c * CH, CH), CH)
            outs = [dot(u_v[2 * q + j], w2[(2 * q + j) % 3, :, cols]).reshape(N, 8, CH) for j in range(2)]
            hsend[q, :, :, cols] = jnp.concatenate(outs, axis=1).astype(BF)
            return carry
        lax.fori_loop(0, NCH, step, 0)

        @pl.when(q == 0)
        def _():
            weight2(3, 0).start()
        hrecv[q, pl.ds(me, 1)] = hsend[q, pl.ds(me, 1)]

        @pl.when(q == 0)
        def _():
            send_h(0, 0, HALF)
        return carry
    lax.fori_loop(0, 2, fwd, 0)
    pltpu.make_async_copy(xl_v, xl_out, out_sem.at[0]).start()
    pltpu.make_async_copy(u_v, u_out, out_sem.at[0]).start()

    wait_recv(gates_all, 2)
    wait_recv(rrecv, 3)

    def send_now(c):
        cols = pl.ds(c * CH, CH)
        for p in peers:
            push(gsend.at[1, p, :, cols], gnow_out.at[me, :, cols], p, 5).start()
        pltpu.make_async_copy(gsend.at[1, me, :, cols], gnow_out.at[me, :, cols], out_sem.at[0]).start()

    lane128 = iota((CAP, 128), 1)
    rows = jnp.broadcast_to(gates_all[...], (N, 8, 512)).reshape(CAP, 512)

    def pre(q, table):
        gcol = []
        for j in range(2):
            here = iota((CAP, 512), 1) == q * 256 + me * 16 + j * 8 + iota((CAP, 512), 0) % 8
            gcol.append(jnp.sum(jnp.where(here, rows, 0.0), axis=1, keepdims=True))

        def rstep(c, acc):
            cols = pl.ds(pl.multiple_of(c * CH, CH), CH)
            rall = rrecv[:, :, cols].reshape(TOK, CH)
            hall = hsend[q, :, :, cols].astype(F32)
            out = []
            for j in range(2):
                rl = dot(e_v[2 * q + j], rall)
                dh_v[2 * q + j, :, cols] = (gcol[j] * (rl * scale)).astype(BF)
                prod = rl * hall[:, 8 * j:8 * j + 8, :].reshape(CAP, CH)
                out.append(acc[j] + ((prod[:, 0:128] + prod[:, 128:256]) + (prod[:, 256:384] + prod[:, 384:512])))
            return tuple(out)
        zero = jnp.zeros((CAP, 128), F32)
        acc = lax.fori_loop(0, NCH, rstep, (zero, zero))
        for j in range(2):
            table = table + jnp.where(lane128 == 2 * q + j, jnp.sum(acc[j], axis=1, keepdims=True) * scale, 0.0)
        return table
    dgsend[...] = lax.fori_loop(0, 2, pre, jnp.zeros((CAP, 128), F32)).reshape(N, 8, 128)
    for p in peers:
        push(dgsend.at[p], dgall.at[me], p, 6).start()
    dgall[pl.ds(me, 1)] = dgsend[pl.ds(me, 1)]
    send_h(0, HALF, HALF)
    send_h(1, 0, HALF)

    def gate_grads():
        wait_recv(dgall, 6)
        mine_of = []
        for l in range(LE):
            col = jnp.sum(jnp.where(iota((N, 8, 128), 2) == l, dgall[...], 0.0), axis=2, keepdims=True).reshape(CAP, 1)
            mine_of.append(jnp.where(iota((CAP, 64), 1) == 4 * (iota((CAP, 64), 0) // 8) + l, col, 0.0).reshape(N, 8, 64))
        spread_g = jnp.concatenate([jnp.concatenate(mine_of[2 * q:2 * q + 2], axis=1).reshape(256, 64) for q in range(2)], axis=0)
        ds = 0.0
        for term in split3(spread_g):
            ds = ds + dot(one_v[...], term)
        probs = probs_v[...]
        dlog = (probs * (ds - jnp.sum(probs * ds, axis=1, keepdims=True))).astype(BF)
        dlog_v[...] = jnp.concatenate([dlog, jnp.zeros_like(dlog)], axis=1)
        dlog_t = dlog.astype(F32).T.astype(BF)
        for c in range(NCH):
            part = dot(dlog_t, x_v[:, c * CH:(c + 1) * CH])
            for i in range(CH // 128):
                ggpart[c // 2, (c % 2) * (CH // 128) + i] = part[:, i * 128:(i + 1) * 128]
        push(ggpart.at[1 - core], ggpair, twin, 8).start()

    def gate_scatter():
        push(ggpart.at[1 - core], ggpair, twin, 8).wait_recv()
        gghalf[...] = ggpart[core] + ggpair[...]
        for p in others:
            push(gghalf.at[p // 2], ggrecv.at[chip], p, 9).start()
        ggrecv[pl.ds(chip, 1)] = gghalf[pl.ds(chip, 1)]
        send_h(1, HALF + CH, CH)
        send_now(0)

    def gate_gather():
        wait_recv(ggrecv, 9, 7)
        total = ggrecv[0]
        for i in range(1, 8):
            total = total + ggrecv[i]
        ggall[core, pl.ds(chip, 1)] = total.reshape(1, 64, 128)
        for p in others:
            push(ggall.at[core, chip], ggall.at[core, chip], p, 10).start()
        for c in range(1, NOW):
            send_now(c)

    def bwd(q, carry):
        for j in range(2):
            e = (1 - q) * (2 + j) + q * (1 - j)
            slot = (1 - q) * (2 - 2 * j) + q * (1 + j)
            if j == 1:
                @pl.when(q == 1)
                def _():
                    weight2(0, 2).wait()
            du = dot(dh_v[e], w2[slot], 1, 1).astype(BF).astype(F32)
            da_v[e] = (gp_v[e] * du).astype(BF)
            if j == 0:
                @pl.when(q == 0)
                def _():
                    weight2(0, 2).start()

        @pl.when(q == 1)
        def _():
            gate_scatter()
            weight1(0, 2).wait()

        def step(c, carry):
            cols = pl.ds(pl.multiple_of(c * CH, CH), CH)
            outs = []
            for j in range(2):
                slot = (1 - q) * (2 - 2 * j) + q * (2 - j)
                outs.append(dot(da_v[2 * (1 - q) + j], w1[slot, cols, :], 1, 1).reshape(N, 8, CH))
            gsend[1 - q, :, :, cols] = jnp.concatenate(outs, axis=1).astype(BF)
            return carry
        lax.fori_loop(0, NCH, step, 0)

        @pl.when(q == 0)
        def _():
            weight1(0, 2).start()
            gate_grads()
            send_h(1, HALF, CH)
        return carry
    lax.fori_loop(0, 2, bwd, 0)
    later = [pltpu.make_async_copy(gsend.at[0], glater_out.at[:, :, pl.ds(0, HID)], out_sem.at[0])]
    if NOW < NCH:
        later.append(pltpu.make_async_copy(gsend.at[1, :, :, pl.ds(NOW * CH, HID - NOW * CH)],
                                           glater_out.at[:, :, pl.ds(HID, HID - NOW * CH)], out_sem.at[0]))
    for cp in later:
        cp.start()
    pltpu.make_async_copy(dh_v, dh_out, out_sem.at[0]).start()
    pltpu.make_async_copy(da_v, da_out, out_sem.at[0]).start()

    cp_dlog = pltpu.make_async_copy(dlog_v, tab_out.at[:, pl.ds(512, 128)], out_sem.at[0])
    cp_dlog.start()
    cp_one = pltpu.make_async_copy(one_v, tab_out.at[:, pl.ds(0, 512)], out_sem.at[0])
    cp_one.start()

    gate_gather()

    wait_h(hrecv, recv_sem.at[4])
    wait_send(xsend, 1)

    def ystep(c, acc):
        cols = pl.ds(pl.multiple_of(c * CH, CH), CH)
        h = hrecv[:, :, :, cols].reshape(512, CH)
        tot = x_v[:, cols].astype(F32) + (dot(c_v[0], h) + dot(c_v[1], h) + dot(c_v[2], h))
        y = tot.astype(BF)
        xsend[:, :, cols] = y.reshape(N, 16, CH)
        return acc + jnp.sum(y.astype(F32) * r_v[:, cols].astype(F32), axis=0, keepdims=True)
    losssend[...] = lax.fori_loop(0, NCH, ystep, jnp.zeros((1, CH), F32))
    cp_y = pltpu.make_async_copy(xsend, y_out, out_sem.at[0])
    cp_y.start()
    for p in peers:
        push(losssend, lossall.at[me], p, 7).start()
    lossall[pl.ds(me, 1)] = losssend[...].reshape(1, 1, CH)

    wait_recv(ggall.at[core], 10, 7)
    across = push(ggall.at[core], ggall.at[core], twin, 11)
    across.start()
    across.wait_recv()
    cp_gg = [pltpu.make_async_copy(ggall.at[i // 8, i % 8], gg_out.at[:, pl.ds(i * 128, 128)], out_sem.at[0]) for i in range(N)]
    for cp in cp_gg:
        cp.start()
    wait_recv(lossall, 7)
    loss_out[0, 0] = jnp.sum(lossall[...]) * scale
    wait_recv(gnow_out, 5)

    wait_send(selall, 0)
    wait_send(gates_all, 2)
    wait_h(hsend, send_sem.at[1])
    wait_send(dgall, 6)
    part = gsend.at[1, pl.ds(0, N - 1), :, pl.ds(0, NOW * CH)]
    pltpu.make_async_copy(part, part, send_sem.at[1]).wait()
    for c in range(NOW):
        cols = pl.ds(c * CH, CH)
        pltpu.make_async_copy(gsend.at[1, me, :, cols], gnow_out.at[me, :, cols], out_sem.at[0]).wait()
    wait_send(rsend, 3)
    wait_send(lossall, 7)
    push(ggpart.at[1 - core], ggpair, twin, 8).wait_send()
    wait_send(gghalf, 9, 7)
    wait_send(ggall.at[core], 10, 7)
    across.wait_send()
    for cp in later:
        cp.wait()
    cp_dlog.wait()
    cp_one.wait()
    pltpu.make_async_copy(xl_v, xl_out, out_sem.at[0]).wait()
    pltpu.make_async_copy(u_v, u_out, out_sem.at[0]).wait()
    pltpu.make_async_copy(dh_v, dh_out, out_sem.at[0]).wait()
    pltpu.make_async_copy(da_v, da_out, out_sem.at[0]).wait()
    cp_y.wait()
    for cp in cp_gg:
        cp.wait()


def comm_call(sel, x, gw, up, dn, r, scale):
    any_ = pl.BlockSpec(memory_space=pl.ANY)
    vmem = pl.BlockSpec(memory_space=pltpu.VMEM)
    V = pltpu.VMEM
    shape = jax.ShapeDtypeStruct
    return pl.pallas_call(
        functools.partial(comm_kernel, scale),
        out_shape=[shape((N, 16, HID), BF), shape((N, 16, NOW * CH), BF), shape((N, 16, 2 * HID - NOW * CH), BF), shape((TOK, 640), BF),
                   shape((64, HID), F32), shape((1, 1), F32),
                   shape((LE, CAP, HID), BF), shape((LE, CAP, FF), BF), shape((LE, CAP, HID), BF), shape((LE, CAP, FF), BF)],
        in_specs=[vmem, any_, any_, any_, any_, any_],
        out_specs=[any_, any_, any_, any_, any_, pl.BlockSpec(memory_space=pltpu.SMEM), any_, any_, any_, any_],
        scratch_shapes=[
            V((TOK, HID), BF), V((TOK, HID), BF), V((64, HID), BF),
            V((3, HID, FF), BF), V((3, FF, HID), BF),
            V((N, 16, HID), BF), V((N, 16, HID), BF), V((N, 16, HID), BF), V((N, 16, HID), BF),
            V((2, N, 16, HID), BF), V((2, N, 16, HID), BF), V((2, N, 16, HID), BF),
            V((LE, CAP, HID), BF), V((LE, CAP, HID), BF), V((LE, CAP, FF), BF), V((LE, CAP, FF), F32), V((LE, CAP, FF), BF),
            V((2, 8, 64, 128), F32), V((8, 64, 128), F32), V((8, 64, 128), F32), V((8, 64, 128), F32), V((2, 8, 64, 128), F32),
            V((8, CAP), jnp.int32), V((N, 8, CAP), jnp.int32), V((1, 512), F32), V((N, 1, 512), F32),
            V((1, CH), F32), V((N, 1, CH), F32), V((N, 8, 128), F32), V((N, 8, 128), F32),
            V((TOK, 512), BF), V((3, TOK, 512), BF), V((LE, CAP, TOK), BF), V((TOK, 64), F32), V((TOK, 128), BF),
            pltpu.SemaphoreType.DMA((2,)), pltpu.SemaphoreType.DMA((2, 3)), pltpu.SemaphoreType.DMA((1,)),
            pltpu.SemaphoreType.DMA((2,)), pltpu.SemaphoreType.DMA((12,)),
        ],
        compiler_params=pltpu.CompilerParams(collective_id=0, has_side_effects=True, vmem_limit_bytes=67043328),
        name='exchange',
    )(sel, x, gw, up, dn, r)


def tile_tools(ins, bufs, outs, tiles, in_sem, out_sem, first):
    def loads(e):
        return [pltpu.make_async_copy(src.at[e], dst.at[e - first], in_sem.at[e - first]) for src, dst in zip(ins, bufs)]

    def stores(i):
        e, c = i // NCH, i % NCH
        cols = pl.ds(pl.multiple_of(c * CH, CH), CH)
        return [pltpu.make_async_copy(tiles[0].at[i - first * NCH], outs[0].at[e, cols, :], out_sem.at[0]),
                pltpu.make_async_copy(tiles[1].at[i - first * NCH], outs[1].at[e, :, cols], out_sem.at[1])]

    def step(i, carry):
        e, c = i // NCH, i % NCH
        xl_v, da_v, u_v, dh_v = bufs
        cols = pl.ds(pl.multiple_of(c * CH, CH), CH)
        tiles[0][i - first * NCH] = dot(xl_v[e - first, :, cols], da_v[e - first], 0, 0).astype(BF)
        tiles[1][i - first * NCH] = dot(u_v[e - first], dh_v[e - first, :, cols], 0, 0).astype(BF)
        for cp in stores(i):
            cp.start()
        return carry

    def finish(i, carry):
        for cp in stores(i):
            cp.wait()
        return carry
    return loads, step, finish


def wgrad1_kernel(xl_in, da_in, u_in, dh_in, y_in, gg_in, loss_in, g1, g2, y, gg, loss,
                  xl_v, da_v, u_v, dh_v, y_v, gg_v, t1, t2, in_sem, out_sem):
    loads, step, finish = tile_tools((xl_in, da_in, u_in, dh_in), (xl_v, da_v, u_v, dh_v), (g1, g2), (t1, t2), in_sem, out_sem, 0)
    cp_y = pltpu.make_async_copy(y_in, y_v, in_sem.at[LE])
    cp_gg = pltpu.make_async_copy(gg_in, gg_v, in_sem.at[LE + 1])
    for cp in loads(0):
        cp.start()
    loss[0, 0] = loss_in[0, 0]

    def expert(e, carry):
        for cp in loads(e):
            cp.wait()

        @pl.when(e + 1 < FIRST)
        def _():
            for cp in loads(e + 1):
                cp.start()

        @pl.when(e == 0)
        def _():
            cp_y.start()
            cp_gg.start()
        lax.fori_loop(e * NCH, (e + 1) * NCH, step, 0)
        return carry
    lax.fori_loop(0, FIRST, expert, 0)
    cp_y.wait()
    cp_gg.wait()
    out_y = pltpu.make_async_copy(y_v, y, in_sem.at[LE])
    out_gg = pltpu.make_async_copy(gg_v, gg, in_sem.at[LE + 1])
    out_y.start()
    out_gg.start()
    out_y.wait()
    out_gg.wait()
    lax.fori_loop(0, FIRST * NCH, finish, 0)


def wgrad1_call(xl, da, u, dh, y, gg, loss):
    shape = jax.ShapeDtypeStruct
    any_ = pl.BlockSpec(memory_space=pl.ANY)
    smem = pl.BlockSpec(memory_space=pltpu.SMEM)
    V = pltpu.VMEM
    return pl.pallas_call(
        wgrad1_kernel,
        in_specs=[any_] * 6 + [smem],
        out_specs=[any_] * 4 + [smem],
        out_shape=[shape((LE, HID, FF), BF), shape((LE, FF, HID), BF), shape((N, 16, HID), BF), shape((64, HID), F32), shape((1, 1), F32)],
        scratch_shapes=[V((FIRST, CAP, HID), BF), V((FIRST, CAP, FF), BF), V((FIRST, CAP, FF), BF), V((FIRST, CAP, HID), BF),
                        V((N, 16, HID), BF), V((64, HID), F32), V((FIRST * NCH, CH, FF), BF), V((FIRST * NCH, FF, CH), BF),
                        pltpu.SemaphoreType.DMA((LE + 2,)), pltpu.SemaphoreType.DMA((2,))],
        compiler_params=pltpu.CompilerParams(vmem_limit_bytes=59000000),
        cost_estimate=pl.CostEstimate(flops=FIRST * 4 * CAP * HID * FF, bytes_accessed=48 * 1024 * 1024, transcendentals=0),
        name='weight_grads_a',
    )(xl, da, u, dh, y, gg, loss)


def gradx_kernel(scale, late_in, now_v, r_v, tab_in, gw_v, gx, late_v, tab_v, gx_v, in_sem, out_sem):
    def pieces(c):
        cols = pl.ds(c * CH, CH)
        out = [pltpu.make_async_copy(late_in.at[:, :, cols], late_v.at[:, :, cols], in_sem.at[c])]
        if c >= NOW:
            more = pl.ds((NCH + c - NOW) * CH, CH)
            out.append(pltpu.make_async_copy(late_in.at[:, :, more], late_v.at[:, :, more], in_sem.at[c]))
        return out
    cp_tab = pltpu.make_async_copy(tab_in, tab_v, in_sem.at[NCH])
    cp_tab.start()
    for c in range(NCH):
        for cp in pieces(c):
            cp.start()
    cp_tab.wait()
    for c in range(NCH):
        cols = pl.ds(c * CH, CH)
        tot = r_v[:, cols].astype(F32) * scale + dot(tab_v[:, 512:576], gw_v[:, cols])
        if c < NOW:
            tot = tot + dot(tab_v[:, 256:512], now_v[:, :, cols].reshape(256, CH))
        for cp in pieces(c):
            cp.wait()
        if c >= NOW:
            tot = tot + dot(tab_v[:, 256:512], late_v[:, :, pl.ds((NCH + c - NOW) * CH, CH)].reshape(256, CH))
        gx_v[:, cols] = (tot + dot(tab_v[:, 0:256], late_v[:, :, cols].reshape(256, CH))).astype(BF)
        pltpu.make_async_copy(gx_v.at[:, cols], gx.at[:, cols], out_sem).start()
    for c in range(NCH):
        cols = pl.ds(c * CH, CH)
        pltpu.make_async_copy(gx_v.at[:, cols], gx.at[:, cols], out_sem).wait()


def gradx_call(late, now, r, tab, gw, scale):
    any_ = pl.BlockSpec(memory_space=pl.ANY)
    vmem = pl.BlockSpec(memory_space=pltpu.VMEM)
    hbm = pl.BlockSpec(memory_space=pltpu.HBM)
    V = pltpu.VMEM
    return pl.pallas_call(
        functools.partial(gradx_kernel, scale),
        in_specs=[hbm, vmem, vmem, hbm, vmem],
        out_specs=any_,
        out_shape=jax.ShapeDtypeStruct((TOK, HID), BF),
        scratch_shapes=[V((N, 16, 2 * HID - NOW * CH), BF), V((TOK, 640), BF), V((TOK, HID), BF), pltpu.SemaphoreType.DMA((NCH + 1,)),
                        pltpu.SemaphoreType.DMA],
        compiler_params=pltpu.CompilerParams(vmem_limit_bytes=16000000),
        name='grad_x',
    )(late, now, r, tab, gw)


def solution(mesh):
    def device_step(x, gate_w, up_w, down_w, expert_picks, loss_w):
        scale = 1.0 / math.sqrt(TOK * N * HID)
        gate_t = gate_w.T
        y, now, later, tab, gg, loss, xl, u, dh, da = comm_call(expert_picks, x, gate_t, up_w, down_w, loss_w, scale)
        later = lax.all_to_all(later, 'ep', 0, 0, tiled=True)
        grad_up, grad_down, y, gg, loss = wgrad1_call(xl, da, u, dh, y, gg, loss)
        grad_x = gradx_call(later, now, loss_w, tab, gate_t, scale)
        return y.reshape(TOK, HID), loss[0, 0], grad_x, grad_up, grad_down, gg.T

    return jax.shard_map(device_step, mesh=mesh,
                         in_specs=(P('ep'), P(), P('ep'), P('ep'), P('ep'), P('ep')),
                         out_specs=(P('ep'), P(), P('ep'), P('ep'), P('ep'), P()),
                         check_vma=False)
```

```python
import functools
import math
import jax
import jax.numpy as jnp
from jax import lax
from jax.experimental import pallas as pl
from jax.experimental.pallas import tpu as pltpu
from jax.sharding import PartitionSpec as P

BF = jnp.bfloat16
F32 = jnp.float32
MESH = pl.DeviceIdType.MESH
N = 16
TOK = 256
LE = 4
CAP = 128
HID = 2048
FF = 1408
CH = 512
NCH = HID // CH
FIRST = 4
HALF = HID // 2
NOW = 2
ORDER = (14, 12, 8, 15, 13, 9, 6, 4, 7, 5, 10, 11, 2, 3, 1)


def dot(a, b, ca=1, cb=0):
    return lax.dot_general(a, b, (((ca,), (cb,)), ((), ())), preferred_element_type=F32)


def iota(shape, dim):
    return lax.broadcasted_iota(jnp.int32, shape, dim)


def ones_where(cond):
    return jnp.where(cond, 1.0, 0.0).astype(BF)


def split3(v):
    hi = v.astype(BF)
    rest = v - hi.astype(F32)
    mid = rest.astype(BF)
    low = (rest - mid.astype(F32)).astype(BF)
    return hi, mid, low


def flip(me, k):
    out = 0
    for b in range(4):
        bit = (me // (1 << b)) % 2
        if (k >> b) & 1:
            bit = 1 - bit
        out = out + bit * (1 << b)
    return out


def comm_kernel(scale, sel_ref, x_hbm, gw_hbm, up_hbm, dn_hbm, r_hbm,
                y_out, gnow_out, glater_out, tab_out, gg_out, loss_out, xl_out, u_out, dh_out, da_out,
                x_v, r_v, gw_v, w1, w2, xsend, rsend, xrecv, rrecv, hsend, hrecv, gsend,
                xl_v, dh_v, u_v, gp_v, da_v, ggpart, ggpair, gghalf, ggrecv, ggall, selsend, selall, gates, gates_all,
                losssend, lossall, dgsend, dgall, one_v, c_v, e_v, probs_v, dlog_v,
                ld_sem, w_sem, out_sem, send_sem, recv_sem):
    me = lax.axis_index('ep')
    peers = [flip(me, k) for k in ORDER]
    core, chip, twin = me % 2, me // 2, flip(me, 1)
    others = [flip(me, k) for k in ORDER if k % 2 == 0]

    def load(src, dst, i):
        return pltpu.make_async_copy(src, dst, ld_sem.at[i])

    def weight1(e, slot):
        return pltpu.make_async_copy(up_hbm.at[e], w1.at[slot], w_sem.at[0, slot])

    def weight2(e, slot):
        return pltpu.make_async_copy(dn_hbm.at[e], w2.at[slot], w_sem.at[1, slot])

    def push(src, dst, peer, i):
        return pltpu.make_async_remote_copy(src_ref=src, dst_ref=dst, send_sem=send_sem.at[0 if i == 1 else 1], recv_sem=recv_sem.at[i],
                                            device_id=(peer,), device_id_type=MESH)

    def wait_recv(buf, i, n=N - 1):
        part = buf.at[pl.ds(0, n)]
        pltpu.make_async_copy(part, part, recv_sem.at[i]).wait()

    def wait_send(buf, i, n=N - 1):
        part = buf.at[pl.ds(0, n)]
        pltpu.make_async_copy(part, part, send_sem.at[0 if i == 1 else 1]).wait()

    cp_x = load(x_hbm, x_v, 0)
    cp_g = load(gw_hbm, gw_v, 0)
    cp_r = load(r_hbm, r_v, 1)
    cp_x.start()
    cp_g.start()
    cp_r.start()

    sel = sel_ref[...]
    selsend[...] = jnp.zeros_like(selsend)
    selsend[0:LE, :] = sel
    selall[pl.ds(me, 1)] = selsend[...].reshape(1, 8, CAP)

    barrier = pltpu.get_barrier_semaphore()
    for p in peers:
        pl.semaphore_signal(barrier, inc=1, device_id=(p,), device_id_type=MESH)
    pl.semaphore_wait(barrier, N - 1)

    for p in peers:
        push(selsend, selall.at[me], p, 0).start()
    for e in range(3):
        weight1(e, e).start()
        weight2(e, e).start()

    cp_g.wait()
    cp_x.wait()
    logits = dot(x_v[...], gw_v[...], 1, 1)
    ex = jnp.exp(logits - jnp.max(logits, axis=1, keepdims=True))
    probs = ex / jnp.sum(ex, axis=1, keepdims=True)
    probs_v[...] = probs

    below = ones_where(iota((TOK, TOK), 1) < iota((TOK, TOK), 0))
    slot_lane = (iota((TOK, TOK), 1) % 16).astype(F32)

    tok_row = iota((TOK, CAP), 0)
    same = iota((CAP, TOK), 0) // 8 == iota((CAP, TOK), 1) // 16
    fold = ones_where(same)
    base = (iota((1, CAP), 1) // 8) * TOK
    hits = [ones_where(tok_row == sel[l:l + 1, :] - base) for l in range(LE)]
    count = dot(hits[0], fold)
    for l in range(1, LE):
        count = count + dot(hits[l], fold)
    pres = count > 0.5
    rank = dot(below, ones_where(pres))
    pick_of = jnp.where(pres, jnp.where(rank == slot_lane, 1.0, 0.0), 0.0).astype(BF)
    for l in range(LE):
        e_v[l] = jnp.where(same, dot(hits[l], pick_of, 0, 0), 0.0).astype(BF)

    place = ones_where(iota((CAP, 512), 0) % 8 == iota((CAP, 512), 1) % 8)
    fold2 = ones_where((iota((512, TOK), 0) % 256) // 16 == iota((512, TOK), 1) // 16)
    for_wait = selall.at[pl.ds(0, N - 1)]
    pltpu.make_async_copy(for_wait, for_wait, recv_sem.at[0]).wait()
    everyone = selall[...].reshape(8 * N, CAP)
    mine = jnp.where(iota((8 * N, CAP), 1) // 8 == me, everyone - me * TOK, 0).astype(F32).astype(BF)
    spread = dot(mine, place)
    lane = iota((8 * N, 512), 1)
    want = ((lane % 256) // 16) * 8 + 2 * (lane // 256) + (lane % 16) // 8
    ids = jnp.sum(jnp.where(iota((8 * N, 512), 0) == want, spread, 0.0), axis=0, keepdims=True)
    one = jnp.where(iota((TOK, 512), 0).astype(F32) == ids, 1.0, 0.0)
    one_v[...] = one.astype(BF)
    pres2 = dot(one_v[...], fold2) > 0.5
    rank2 = dot(below, ones_where(pres2))
    give = jnp.where(pres2, jnp.where(rank2 == slot_lane, 1.0, 0.0), 0.0).astype(BF)
    give_t = give.T

    def gather(src, dst):
        def step(c, carry):
            cols = pl.ds(pl.multiple_of(c * CH, CH), CH)
            dst[:, :, cols] = dot(give_t, src[:, cols]).astype(BF).reshape(N, 16, CH)
            return carry
        lax.fori_loop(0, NCH, step, 0)

    for c in range(NCH):
        cols = pl.ds(c * CH, CH)
        xsend[:, :, cols] = dot(give_t, x_v[:, cols]).astype(BF).reshape(N, 16, CH)
        for p in peers:
            push(xsend.at[p, :, cols], xrecv.at[me, :, cols], p, 1).start()
    xrecv[pl.ds(me, 1)] = xsend[pl.ds(me, 1)]

    rep = ones_where(iota((64, 512), 0) == 4 * ((iota((64, 512), 1) % 256) // 16) + 2 * (iota((64, 512), 1) // 256)
                     + (iota((64, 512), 1) % 16) // 8)
    wide = 0.0
    for term in split3(probs_v[...]):
        wide = wide + dot(term, rep)
    comb = wide * one
    for i, term in enumerate(split3(comb)):
        c_v[i] = term
    gates[...] = jnp.sum(comb, axis=0, keepdims=True)
    for p in peers:
        push(gates, gates_all.at[me], p, 2).start()
    gates_all[pl.ds(me, 1)] = gates[...].reshape(1, 1, 512)

    cp_r.wait()
    gather(r_v, rsend)
    for p in peers:
        push(rsend.at[p], rrecv.at[me], p, 3).start()
    rrecv[pl.ds(me, 1)] = rsend[pl.ds(me, 1)]

    wait_recv(xrecv, 1)

    def send_h(q, start, width):
        cols = pl.ds(start, width)
        for p in peers:
            push(hsend.at[q, p, :, cols], hrecv.at[q, me, :, cols], p, 4).start()

    def wait_h(buf, sem):
        part = buf.at[:, pl.ds(0, N - 1)]
        pltpu.make_async_copy(part, part, sem).wait()

    def fwd(q, carry):
        for j in range(2):
            e = 2 * q + j
            slot = e % 3
            xl = dot(e_v[e], xrecv[...].reshape(TOK, HID)).astype(BF)
            xl_v[e] = xl
            weight1(e, slot).wait()
            a = dot(xl_v[e], w1[slot])
            if j == 0:
                @pl.when(q == 0)
                def _():
                    weight1(3, 0).start()
            k0 = math.sqrt(2.0 / math.pi)
            t = jnp.tanh(k0 * (a + 0.044715 * (a * a * a)))
            u_v[e] = (0.5 * a * (1.0 + t)).astype(BF)
            gp_v[e] = 0.5 * (1.0 + t) + 0.5 * a * (1.0 - t * t) * (k0 * (1.0 + 3.0 * 0.044715 * (a * a)))
        weight2(2 * q, (2 * q) % 3).wait()
        weight2(2 * q + 1, (2 * q + 1) % 3).wait()

        def step(c, carry):
            cols = pl.ds(pl.multiple_of(c * CH, CH), CH)
            outs = [dot(u_v[2 * q + j], w2[(2 * q + j) % 3, :, cols]).reshape(N, 8, CH) for j in range(2)]
            hsend[q, :, :, cols] = jnp.concatenate(outs, axis=1).astype(BF)
            return carry
        lax.fori_loop(0, NCH, step, 0)

        @pl.when(q == 0)
        def _():
            weight2(3, 0).start()
        hrecv[q, pl.ds(me, 1)] = hsend[q, pl.ds(me, 1)]

        @pl.when(q == 0)
        def _():
            send_h(0, 0, HALF)
        return carry
    lax.fori_loop(0, 2, fwd, 0)
    pltpu.make_async_copy(xl_v, xl_out, out_sem.at[0]).start()
    pltpu.make_async_copy(u_v, u_out, out_sem.at[0]).start()

    wait_recv(gates_all, 2)
    wait_recv(rrecv, 3)

    def send_now(c):
        cols = pl.ds(c * CH, CH)
        for p in peers:
            push(gsend.at[1, p, :, cols], gnow_out.at[me, :, cols], p, 5).start()
        pltpu.make_async_copy(gsend.at[1, me, :, cols], gnow_out.at[me, :, cols], out_sem.at[0]).start()

    lane128 = iota((CAP, 128), 1)
    rows = jnp.broadcast_to(gates_all[...], (N, 8, 512)).reshape(CAP, 512)

    def pre(q, table):
        gcol = []
        for j in range(2):
            here = iota((CAP, 512), 1) == q * 256 + me * 16 + j * 8 + iota((CAP, 512), 0) % 8
            gcol.append(jnp.sum(jnp.where(here, rows, 0.0), axis=1, keepdims=True))

        def rstep(c, acc):
            cols = pl.ds(pl.multiple_of(c * CH, CH), CH)
            rall = rrecv[:, :, cols].reshape(TOK, CH)
            hall = hsend[q, :, :, cols].astype(F32)
            out = []
            for j in range(2):
                rl = dot(e_v[2 * q + j], rall)
                dh_v[2 * q + j, :, cols] = (gcol[j] * (rl * scale)).astype(BF)
                prod = rl * hall[:, 8 * j:8 * j + 8, :].reshape(CAP, CH)
                out.append(acc[j] + ((prod[:, 0:128] + prod[:, 128:256]) + (prod[:, 256:384] + prod[:, 384:512])))
            return tuple(out)
        zero = jnp.zeros((CAP, 128), F32)
        acc = lax.fori_loop(0, NCH, rstep, (zero, zero))
        for j in range(2):
            table = table + jnp.where(lane128 == 2 * q + j, jnp.sum(acc[j], axis=1, keepdims=True) * scale, 0.0)
        return table
    dgsend[...] = lax.fori_loop(0, 2, pre, jnp.zeros((CAP, 128), F32)).reshape(N, 8, 128)
    for p in peers:
        push(dgsend.at[p], dgall.at[me], p, 6).start()
    dgall[pl.ds(me, 1)] = dgsend[pl.ds(me, 1)]
    send_h(0, HALF, HALF)
    send_h(1, 0, HALF)

    def gate_grads():
        wait_recv(dgall, 6)
        mine_of = []
        for l in range(LE):
            col = jnp.sum(jnp.where(iota((N, 8, 128), 2) == l, dgall[...], 0.0), axis=2, keepdims=True).reshape(CAP, 1)
            mine_of.append(jnp.where(iota((CAP, 64), 1) == 4 * (iota((CAP, 64), 0) // 8) + l, col, 0.0).reshape(N, 8, 64))
        spread_g = jnp.concatenate([jnp.concatenate(mine_of[2 * q:2 * q + 2], axis=1).reshape(256, 64) for q in range(2)], axis=0)
        ds = 0.0
        for term in split3(spread_g):
            ds = ds + dot(one_v[...], term)
        probs = probs_v[...]
        dlog = (probs * (ds - jnp.sum(probs * ds, axis=1, keepdims=True))).astype(BF)
        dlog_v[...] = jnp.concatenate([dlog, jnp.zeros_like(dlog)], axis=1)
        dlog_t = dlog.astype(F32).T.astype(BF)
        for c in range(NCH):
            part = dot(dlog_t, x_v[:, c * CH:(c + 1) * CH])
            for i in range(CH // 128):
                ggpart[c // 2, (c % 2) * (CH // 128) + i] = part[:, i * 128:(i + 1) * 128]
        push(ggpart.at[1 - core], ggpair, twin, 8).start()

    def gate_scatter():
        push(ggpart.at[1 - core], ggpair, twin, 8).wait_recv()
        gghalf[...] = ggpart[core] + ggpair[...]
        for p in others:
            push(gghalf.at[p // 2], ggrecv.at[chip], p, 9).start()
        ggrecv[pl.ds(chip, 1)] = gghalf[pl.ds(chip, 1)]
        send_h(1, HALF + CH, CH)
        send_now(0)

    def gate_gather():
        wait_recv(ggrecv, 9, 7)
        total = ggrecv[0]
        for i in range(1, 8):
            total = total + ggrecv[i]
        ggall[core, pl.ds(chip, 1)] = total.reshape(1, 64, 128)
        for p in others:
            push(ggall.at[core, chip], ggall.at[core, chip], p, 10).start()
        for c in range(1, NOW):
            send_now(c)

    def bwd(q, carry):
        for j in range(2):
            e = (1 - q) * (2 + j) + q * (1 - j)
            slot = (1 - q) * (2 - 2 * j) + q * (1 + j)
            if j == 1:
                @pl.when(q == 1)
                def _():
                    weight2(0, 2).wait()
            du = dot(dh_v[e], w2[slot], 1, 1).astype(BF).astype(F32)
            da_v[e] = (gp_v[e] * du).astype(BF)
            if j == 0:
                @pl.when(q == 0)
                def _():
                    weight2(0, 2).start()

        @pl.when(q == 1)
        def _():
            gate_scatter()
            weight1(0, 2).wait()

        def step(c, carry):
            cols = pl.ds(pl.multiple_of(c * CH, CH), CH)
            outs = []
            for j in range(2):
                slot = (1 - q) * (2 - 2 * j) + q * (2 - j)
                outs.append(dot(da_v[2 * (1 - q) + j], w1[slot, cols, :], 1, 1).reshape(N, 8, CH))
            gsend[1 - q, :, :, cols] = jnp.concatenate(outs, axis=1).astype(BF)
            return carry
        lax.fori_loop(0, NCH, step, 0)

        @pl.when(q == 0)
        def _():
            weight1(0, 2).start()
            gate_grads()
            send_h(1, HALF, CH)
        return carry
    lax.fori_loop(0, 2, bwd, 0)
    later = [pltpu.make_async_copy(gsend.at[0], glater_out.at[:, :, pl.ds(0, HID)], out_sem.at[0])]
    if NOW < NCH:
        later.append(pltpu.make_async_copy(gsend.at[1, :, :, pl.ds(NOW * CH, HID - NOW * CH)],
                                           glater_out.at[:, :, pl.ds(HID, HID - NOW * CH)], out_sem.at[0]))
    for cp in later:
        cp.start()
    pltpu.make_async_copy(dh_v, dh_out, out_sem.at[0]).start()
    pltpu.make_async_copy(da_v, da_out, out_sem.at[0]).start()

    cp_dlog = pltpu.make_async_copy(dlog_v, tab_out.at[:, pl.ds(512, 128)], out_sem.at[0])
    cp_dlog.start()
    cp_one = pltpu.make_async_copy(one_v, tab_out.at[:, pl.ds(0, 512)], out_sem.at[0])
    cp_one.start()

    gate_gather()

    wait_h(hrecv, recv_sem.at[4])
    wait_send(xsend, 1)

    def ystep(c, acc):
        cols = pl.ds(pl.multiple_of(c * CH, CH), CH)
        h = hrecv[:, :, :, cols].reshape(512, CH)
        tot = x_v[:, cols].astype(F32) + (dot(c_v[0], h) + dot(c_v[1], h) + dot(c_v[2], h))
        y = tot.astype(BF)
        xsend[:, :, cols] = y.reshape(N, 16, CH)
        return acc + jnp.sum(y.astype(F32) * r_v[:, cols].astype(F32), axis=0, keepdims=True)
    losssend[...] = lax.fori_loop(0, NCH, ystep, jnp.zeros((1, CH), F32))
    cp_y = pltpu.make_async_copy(xsend, y_out, out_sem.at[0])
    cp_y.start()
    for p in peers:
        push(losssend, lossall.at[me], p, 7).start()
    lossall[pl.ds(me, 1)] = losssend[...].reshape(1, 1, CH)

    wait_recv(ggall.at[core], 10, 7)
    across = push(ggall.at[core], ggall.at[core], twin, 11)
    across.start()
    across.wait_recv()
    cp_gg = [pltpu.make_async_copy(ggall.at[i // 8, i % 8], gg_out.at[:, pl.ds(i * 128, 128)], out_sem.at[0]) for i in range(N)]
    for cp in cp_gg:
        cp.start()
    wait_recv(lossall, 7)
    loss_out[0, 0] = jnp.sum(lossall[...]) * scale
    wait_recv(gnow_out, 5)

    wait_send(selall, 0)
    wait_send(gates_all, 2)
    wait_h(hsend, send_sem.at[1])
    wait_send(dgall, 6)
    part = gsend.at[1, pl.ds(0, N - 1), :, pl.ds(0, NOW * CH)]
    pltpu.make_async_copy(part, part, send_sem.at[1]).wait()
    for c in range(NOW):
        cols = pl.ds(c * CH, CH)
        pltpu.make_async_copy(gsend.at[1, me, :, cols], gnow_out.at[me, :, cols], out_sem.at[0]).wait()
    wait_send(rsend, 3)
    wait_send(lossall, 7)
    push(ggpart.at[1 - core], ggpair, twin, 8).wait_send()
    wait_send(gghalf, 9, 7)
    wait_send(ggall.at[core], 10, 7)
    across.wait_send()
    for cp in later:
        cp.wait()
    cp_dlog.wait()
    cp_one.wait()
    pltpu.make_async_copy(xl_v, xl_out, out_sem.at[0]).wait()
    pltpu.make_async_copy(u_v, u_out, out_sem.at[0]).wait()
    pltpu.make_async_copy(dh_v, dh_out, out_sem.at[0]).wait()
    pltpu.make_async_copy(da_v, da_out, out_sem.at[0]).wait()
    cp_y.wait()
    for cp in cp_gg:
        cp.wait()


def comm_call(sel, x, gw, up, dn, r, scale):
    any_ = pl.BlockSpec(memory_space=pl.ANY)
    vmem = pl.BlockSpec(memory_space=pltpu.VMEM)
    V = pltpu.VMEM
    shape = jax.ShapeDtypeStruct
    return pl.pallas_call(
        functools.partial(comm_kernel, scale),
        out_shape=[shape((N, 16, HID), BF), shape((N, 16, NOW * CH), BF), shape((N, 16, 2 * HID - NOW * CH), BF), shape((TOK, 640), BF),
                   shape((64, HID), F32), shape((1, 1), F32),
                   shape((LE, CAP, HID), BF), shape((LE, CAP, FF), BF), shape((LE, CAP, HID), BF), shape((LE, CAP, FF), BF)],
        in_specs=[vmem, any_, any_, any_, any_, any_],
        out_specs=[any_, any_, any_, any_, any_, pl.BlockSpec(memory_space=pltpu.SMEM), any_, any_, any_, any_],
        scratch_shapes=[
            V((TOK, HID), BF), V((TOK, HID), BF), V((64, HID), BF),
            V((3, HID, FF), BF), V((3, FF, HID), BF),
            V((N, 16, HID), BF), V((N, 16, HID), BF), V((N, 16, HID), BF), V((N, 16, HID), BF),
            V((2, N, 16, HID), BF), V((2, N, 16, HID), BF), V((2, N, 16, HID), BF),
            V((LE, CAP, HID), BF), V((LE, CAP, HID), BF), V((LE, CAP, FF), BF), V((LE, CAP, FF), F32), V((LE, CAP, FF), BF),
            V((2, 8, 64, 128), F32), V((8, 64, 128), F32), V((8, 64, 128), F32), V((8, 64, 128), F32), V((2, 8, 64, 128), F32),
            V((8, CAP), jnp.int32), V((N, 8, CAP), jnp.int32), V((1, 512), F32), V((N, 1, 512), F32),
            V((1, CH), F32), V((N, 1, CH), F32), V((N, 8, 128), F32), V((N, 8, 128), F32),
            V((TOK, 512), BF), V((3, TOK, 512), BF), V((LE, CAP, TOK), BF), V((TOK, 64), F32), V((TOK, 128), BF),
            pltpu.SemaphoreType.DMA((2,)), pltpu.SemaphoreType.DMA((2, 3)), pltpu.SemaphoreType.DMA((1,)),
            pltpu.SemaphoreType.DMA((2,)), pltpu.SemaphoreType.DMA((12,)),
        ],
        compiler_params=pltpu.CompilerParams(collective_id=0, has_side_effects=True, vmem_limit_bytes=67043328),
        name='exchange',
    )(sel, x, gw, up, dn, r)


def tile_tools(ins, bufs, outs, tiles, in_sem, out_sem, first):
    def loads(e):
        return [pltpu.make_async_copy(src.at[e], dst.at[e - first], in_sem.at[e - first]) for src, dst in zip(ins, bufs)]

    def stores(i):
        e, c = i // NCH, i % NCH
        cols = pl.ds(pl.multiple_of(c * CH, CH), CH)
        return [pltpu.make_async_copy(tiles[0].at[i - first * NCH], outs[0].at[e, cols, :], out_sem.at[0]),
                pltpu.make_async_copy(tiles[1].at[i - first * NCH], outs[1].at[e, :, cols], out_sem.at[1])]

    def step(i, carry):
        e, c = i // NCH, i % NCH
        xl_v, da_v, u_v, dh_v = bufs
        cols = pl.ds(pl.multiple_of(c * CH, CH), CH)
        tiles[0][i - first * NCH] = dot(xl_v[e - first, :, cols], da_v[e - first], 0, 0).astype(BF)
        tiles[1][i - first * NCH] = dot(u_v[e - first], dh_v[e - first, :, cols], 0, 0).astype(BF)
        for cp in stores(i):
            cp.start()
        return carry

    def finish(i, carry):
        for cp in stores(i):
            cp.wait()
        return carry
    return loads, step, finish


def wgrad1_kernel(xl_in, da_in, u_in, dh_in, y_in, gg_in, loss_in, g1, g2, y, gg, loss,
                  xl_v, da_v, u_v, dh_v, y_v, gg_v, t1, t2, in_sem, out_sem):
    loads, step, finish = tile_tools((xl_in, da_in, u_in, dh_in), (xl_v, da_v, u_v, dh_v), (g1, g2), (t1, t2), in_sem, out_sem, 0)
    cp_y = pltpu.make_async_copy(y_in, y_v, in_sem.at[LE])
    cp_gg = pltpu.make_async_copy(gg_in, gg_v, in_sem.at[LE + 1])
    for cp in loads(0):
        cp.start()
    loss[0, 0] = loss_in[0, 0]

    def expert(e, carry):
        for cp in loads(e):
            cp.wait()

        @pl.when(e + 1 < FIRST)
        def _():
            for cp in loads(e + 1):
                cp.start()

        @pl.when(e == 0)
        def _():
            cp_y.start()
            cp_gg.start()
        lax.fori_loop(e * NCH, (e + 1) * NCH, step, 0)
        return carry
    lax.fori_loop(0, FIRST, expert, 0)
    cp_y.wait()
    cp_gg.wait()
    out_y = pltpu.make_async_copy(y_v, y, in_sem.at[LE])
    out_gg = pltpu.make_async_copy(gg_v, gg, in_sem.at[LE + 1])
    out_y.start()
    out_gg.start()
    out_y.wait()
    out_gg.wait()
    lax.fori_loop(0, FIRST * NCH, finish, 0)


def wgrad1_call(xl, da, u, dh, y, gg, loss):
    shape = jax.ShapeDtypeStruct
    any_ = pl.BlockSpec(memory_space=pl.ANY)
    smem = pl.BlockSpec(memory_space=pltpu.SMEM)
    V = pltpu.VMEM
    return pl.pallas_call(
        wgrad1_kernel,
        in_specs=[any_] * 6 + [smem],
        out_specs=[any_] * 4 + [smem],
        out_shape=[shape((LE, HID, FF), BF), shape((LE, FF, HID), BF), shape((N, 16, HID), BF), shape((64, HID), F32), shape((1, 1), F32)],
        scratch_shapes=[V((FIRST, CAP, HID), BF), V((FIRST, CAP, FF), BF), V((FIRST, CAP, FF), BF), V((FIRST, CAP, HID), BF),
                        V((N, 16, HID), BF), V((64, HID), F32), V((FIRST * NCH, CH, FF), BF), V((FIRST * NCH, FF, CH), BF),
                        pltpu.SemaphoreType.DMA((LE + 2,)), pltpu.SemaphoreType.DMA((2,))],
        compiler_params=pltpu.CompilerParams(vmem_limit_bytes=59000000),
        cost_estimate=pl.CostEstimate(flops=FIRST * 4 * CAP * HID * FF, bytes_accessed=48 * 1024 * 1024, transcendentals=0),
        name='weight_grads_a',
    )(xl, da, u, dh, y, gg, loss)


def gradx_kernel(scale, late_in, now_v, r_v, tab_in, gw_v, gx, late_v, tab_v, gx_v, in_sem, out_sem):
    def pieces(c):
        cols = pl.ds(c * CH, CH)
        out = [pltpu.make_async_copy(late_in.at[:, :, cols], late_v.at[:, :, cols], in_sem.at[c])]
        if c >= NOW:
            more = pl.ds((NCH + c - NOW) * CH, CH)
            out.append(pltpu.make_async_copy(late_in.at[:, :, more], late_v.at[:, :, more], in_sem.at[c]))
        return out
    cp_tab = pltpu.make_async_copy(tab_in, tab_v, in_sem.at[NCH])
    cp_tab.start()
    for c in range(NCH):
        for cp in pieces(c):
            cp.start()
    cp_tab.wait()
    for c in range(NCH):
        cols = pl.ds(c * CH, CH)
        tot = r_v[:, cols].astype(F32) * scale + dot(tab_v[:, 512:576], gw_v[:, cols])
        if c < NOW:
            tot = tot + dot(tab_v[:, 256:512], now_v[:, :, cols].reshape(256, CH))
        for cp in pieces(c):
            cp.wait()
        if c >= NOW:
            tot = tot + dot(tab_v[:, 256:512], late_v[:, :, pl.ds((NCH + c - NOW) * CH, CH)].reshape(256, CH))
        gx_v[:, cols] = (tot + dot(tab_v[:, 0:256], late_v[:, :, cols].reshape(256, CH))).astype(BF)
        pltpu.make_async_copy(gx_v.at[:, cols], gx.at[:, cols], out_sem).start()
    for c in range(NCH):
        cols = pl.ds(c * CH, CH)
        pltpu.make_async_copy(gx_v.at[:, cols], gx.at[:, cols], out_sem).wait()


def gradx_call(late, now, r, tab, gw, scale):
    any_ = pl.BlockSpec(memory_space=pl.ANY)
    vmem = pl.BlockSpec(memory_space=pltpu.VMEM)
    hbm = pl.BlockSpec(memory_space=pltpu.HBM)
    V = pltpu.VMEM
    return pl.pallas_call(
        functools.partial(gradx_kernel, scale),
        in_specs=[hbm, vmem, vmem, hbm, vmem],
        out_specs=any_,
        out_shape=jax.ShapeDtypeStruct((TOK, HID), BF),
        scratch_shapes=[V((N, 16, 2 * HID - NOW * CH), BF), V((TOK, 640), BF), V((TOK, HID), BF), pltpu.SemaphoreType.DMA((NCH + 1,)),
                        pltpu.SemaphoreType.DMA],
        compiler_params=pltpu.CompilerParams(vmem_limit_bytes=16000000),
        name='grad_x',
    )(late, now, r, tab, gw)


def solution(mesh):
    def device_step(x, gate_w, up_w, down_w, expert_picks, loss_w):
        scale = 1.0 / math.sqrt(TOK * N * HID)
        gate_t = gate_w.T
        y, now, later, tab, gg, loss, xl, u, dh, da = comm_call(expert_picks, x, gate_t, up_w, down_w, loss_w, scale)
        later = lax.all_to_all(later, 'ep', 0, 0, tiled=True)
        grad_up, grad_down, y, gg, loss = wgrad1_call(xl, da, u, dh, y, gg, loss)
        grad_x = gradx_call(later, now, loss_w, tab, gate_t, scale)
        return y.reshape(TOK, HID), loss[0, 0], grad_x, grad_up, grad_down, gg.T

    return jax.shard_map(device_step, mesh=mesh,
                         in_specs=(P('ep'), P(), P('ep'), P('ep'), P('ep'), P('ep')),
                         out_specs=(P('ep'), P(), P('ep'), P('ep'), P('ep'), P()),
                         check_vma=False)
```

```python
import functools
import math
import jax
import jax.numpy as jnp
from jax import lax
from jax.experimental import pallas as pl
from jax.experimental.pallas import tpu as pltpu
from jax.sharding import PartitionSpec as P

BF = jnp.bfloat16
F32 = jnp.float32
MESH = pl.DeviceIdType.MESH
N = 16
TOK = 256
LE = 4
CAP = 128
HID = 2048
FF = 1408
CH = 512
NCH = HID // CH
FIRST = 4
HALF = HID // 2
NOW = 2
ORDER = (14, 12, 8, 15, 13, 9, 6, 4, 7, 5, 10, 11, 2, 3, 1)


def dot(a, b, ca=1, cb=0):
    return lax.dot_general(a, b, (((ca,), (cb,)), ((), ())), preferred_element_type=F32)


def iota(shape, dim):
    return lax.broadcasted_iota(jnp.int32, shape, dim)


def ones_where(cond):
    return jnp.where(cond, 1.0, 0.0).astype(BF)


def split3(v):
    hi = v.astype(BF)
    rest = v - hi.astype(F32)
    mid = rest.astype(BF)
    low = (rest - mid.astype(F32)).astype(BF)
    return hi, mid, low


def flip(me, k):
    out = 0
    for b in range(4):
        bit = (me // (1 << b)) % 2
        if (k >> b) & 1:
            bit = 1 - bit
        out = out + bit * (1 << b)
    return out


def comm_kernel(scale, sel_ref, x_hbm, gw_hbm, up_hbm, dn_hbm, r_hbm,
                y_out, tab_out, glater_out, gg_out, loss_out, xl_out, u_out, dh_out, da_out,
                x_v, r_v, gw_v, w1, w2, xsend, rsend, xrecv, rrecv, hsend, hrecv, gsend,
                xl_v, dh_v, u_v, gp_v, da_v, ggpart, ggpair, gghalf, ggrecv, ggall, selsend, selall, gates, gates_all,
                losssend, lossall, dgsend, dgall, one_v, c_v, e_v, probs_v, dlog_v, ids_v,
                ld_sem, w_sem, out_sem, send_sem, recv_sem):
    me = lax.axis_index('ep')
    peers = [flip(me, k) for k in ORDER]
    core, chip, twin = me % 2, me // 2, flip(me, 1)
    others = [flip(me, k) for k in ORDER if k % 2 == 0]

    def load(src, dst, i):
        return pltpu.make_async_copy(src, dst, ld_sem.at[i])

    def weight1(e, slot):
        return pltpu.make_async_copy(up_hbm.at[e], w1.at[slot], w_sem.at[0, slot])

    def weight2(e, slot):
        return pltpu.make_async_copy(dn_hbm.at[e], w2.at[slot], w_sem.at[1, slot])

    def push(src, dst, peer, i):
        return pltpu.make_async_remote_copy(src_ref=src, dst_ref=dst, send_sem=send_sem.at[0 if i == 1 else 1], recv_sem=recv_sem.at[i],
                                            device_id=(peer,), device_id_type=MESH)

    def wait_recv(buf, i, n=N - 1):
        part = buf.at[pl.ds(0, n)]
        pltpu.make_async_copy(part, part, recv_sem.at[i]).wait()

    def wait_send(buf, i, n=N - 1):
        part = buf.at[pl.ds(0, n)]
        pltpu.make_async_copy(part, part, send_sem.at[0 if i == 1 else 1]).wait()

    cp_x = load(x_hbm, x_v, 0)
    cp_g = load(gw_hbm, gw_v, 0)
    cp_r = load(r_hbm, r_v, 1)
    cp_x.start()
    cp_g.start()
    cp_r.start()

    sel = sel_ref[...]
    selsend[...] = jnp.zeros_like(selsend)
    selsend[0:LE, :] = sel
    selall[pl.ds(me, 1)] = selsend[...].reshape(1, 8, CAP)

    barrier = pltpu.get_barrier_semaphore()
    for p in peers:
        pl.semaphore_signal(barrier, inc=1, device_id=(p,), device_id_type=MESH)
    pl.semaphore_wait(barrier, N - 1)

    for p in peers:
        push(selsend, selall.at[me], p, 0).start()
    for e in range(3):
        weight1(e, e).start()
        weight2(e, e).start()

    cp_g.wait()
    cp_x.wait()
    logits = dot(x_v[...], gw_v[...], 1, 1)
    ex = jnp.exp(logits - jnp.max(logits, axis=1, keepdims=True))
    probs = ex / jnp.sum(ex, axis=1, keepdims=True)
    probs_v[...] = probs

    below = ones_where(iota((TOK, TOK), 1) < iota((TOK, TOK), 0))
    slot_lane = (iota((TOK, TOK), 1) % 16).astype(F32)

    tok_row = iota((TOK, CAP), 0)
    same = iota((CAP, TOK), 0) // 8 == iota((CAP, TOK), 1) // 16
    fold = ones_where(same)
    base = (iota((1, CAP), 1) // 8) * TOK
    hits = [ones_where(tok_row == sel[l:l + 1, :] - base) for l in range(LE)]
    count = dot(hits[0], fold)
    for l in range(1, LE):
        count = count + dot(hits[l], fold)
    pres = count > 0.5
    rank = dot(below, ones_where(pres))
    pick_of = jnp.where(pres, jnp.where(rank == slot_lane, 1.0, 0.0), 0.0).astype(BF)
    for l in range(LE):
        e_v[l] = jnp.where(same, dot(hits[l], pick_of, 0, 0), 0.0).astype(BF)

    place = ones_where(iota((CAP, 512), 0) % 8 == iota((CAP, 512), 1) % 8)
    fold2 = ones_where((iota((512, TOK), 0) % 256) // 16 == iota((512, TOK), 1) // 16)
    for_wait = selall.at[pl.ds(0, N - 1)]
    pltpu.make_async_copy(for_wait, for_wait, recv_sem.at[0]).wait()
    everyone = selall[...].reshape(8 * N, CAP)
    mine = jnp.where(iota((8 * N, CAP), 1) // 8 == me, everyone - me * TOK, 0).astype(F32).astype(BF)
    spread = dot(mine, place)
    lane = iota((8 * N, 512), 1)
    want = ((lane % 256) // 16) * 8 + 2 * (lane // 256) + (lane % 16) // 8
    ids = jnp.sum(jnp.where(iota((8 * N, 512), 0) == want, spread, 0.0), axis=0, keepdims=True)
    one = jnp.where(iota((TOK, 512), 0).astype(F32) == ids, 1.0, 0.0)
    one_v[...] = one.astype(BF)
    pres2 = dot(one_v[...], fold2) > 0.5
    rank2 = dot(below, ones_where(pres2))
    give = jnp.where(pres2, jnp.where(rank2 == slot_lane, 1.0, 0.0), 0.0).astype(BF)
    give_t = give.T

    def gather(src, dst):
        def step(c, carry):
            cols = pl.ds(pl.multiple_of(c * CH, CH), CH)
            dst[:, :, cols] = dot(give_t, src[:, cols]).astype(BF).reshape(N, 16, CH)
            return carry
        lax.fori_loop(0, NCH, step, 0)

    for c in range(NCH):
        cols = pl.ds(c * CH, CH)
        xsend[:, :, cols] = dot(give_t, x_v[:, cols]).astype(BF).reshape(N, 16, CH)
        for p in peers:
            push(xsend.at[p, :, cols], xrecv.at[me, :, cols], p, 1).start()
    xrecv[pl.ds(me, 1)] = xsend[pl.ds(me, 1)]

    rows16 = jnp.where(iota((16, 512), 1) // 64 == iota((16, 512), 0), jnp.broadcast_to(ids, (16, 512)), 0.0).astype(BF)
    ids_v[...] = dot(rows16, ones_where(iota((512, 128), 1) == 64 + iota((512, 128), 0) % 64))

    rep = ones_where(iota((64, 512), 0) == 4 * ((iota((64, 512), 1) % 256) // 16) + 2 * (iota((64, 512), 1) // 256)
                     + (iota((64, 512), 1) % 16) // 8)
    wide = 0.0
    for term in split3(probs_v[...]):
        wide = wide + dot(term, rep)
    comb = wide * one
    for i, term in enumerate(split3(comb)):
        c_v[i] = term
    gates[...] = jnp.sum(comb, axis=0, keepdims=True)
    for p in peers:
        push(gates, gates_all.at[me], p, 2).start()
    gates_all[pl.ds(me, 1)] = gates[...].reshape(1, 1, 512)

    cp_r.wait()
    gather(r_v, rsend)
    for p in peers:
        push(rsend.at[p], rrecv.at[me], p, 3).start()
    rrecv[pl.ds(me, 1)] = rsend[pl.ds(me, 1)]

    wait_recv(xrecv, 1)

    def send_h(q, start, width):
        cols = pl.ds(start, width)
        for p in peers:
            push(hsend.at[q, p, :, cols], hrecv.at[q, me, :, cols], p, 4).start()

    def wait_h(buf, sem):
        part = buf.at[:, pl.ds(0, N - 1)]
        pltpu.make_async_copy(part, part, sem).wait()

    def fwd(q, carry):
        for j in range(2):
            e = 2 * q + j
            slot = e % 3
            xl = dot(e_v[e], xrecv[...].reshape(TOK, HID)).astype(BF)
            xl_v[e] = xl
            weight1(e, slot).wait()
            a = dot(xl_v[e], w1[slot])
            if j == 0:
                @pl.when(q == 0)
                def _():
                    weight1(3, 0).start()
            k0 = math.sqrt(2.0 / math.pi)
            t = jnp.tanh(k0 * (a + 0.044715 * (a * a * a)))
            u_v[e] = (0.5 * a * (1.0 + t)).astype(BF)
            gp_v[e] = 0.5 * (1.0 + t) + 0.5 * a * (1.0 - t * t) * (k0 * (1.0 + 3.0 * 0.044715 * (a * a)))
        weight2(2 * q, (2 * q) % 3).wait()
        weight2(2 * q + 1, (2 * q + 1) % 3).wait()

        def step(c, carry):
            cols = pl.ds(pl.multiple_of(c * CH, CH), CH)
            outs = [dot(u_v[2 * q + j], w2[(2 * q + j) % 3, :, cols]).reshape(N, 8, CH) for j in range(2)]
            hsend[q, :, :, cols] = jnp.concatenate(outs, axis=1).astype(BF)
            return carry
        lax.fori_loop(0, NCH, step, 0)

        @pl.when(q == 0)
        def _():
            weight2(3, 0).start()
        hrecv[q, pl.ds(me, 1)] = hsend[q, pl.ds(me, 1)]

        @pl.when(q == 0)
        def _():
            send_h(0, 0, HALF)
        return carry
    lax.fori_loop(0, 2, fwd, 0)
    pltpu.make_async_copy(xl_v, xl_out, out_sem.at[0]).start()
    pltpu.make_async_copy(u_v, u_out, out_sem.at[0]).start()

    wait_recv(gates_all, 2)
    wait_recv(rrecv, 3)

    def send_now(c):
        cols = pl.ds(c * CH, CH)
        mine_rows = pl.ds(pl.multiple_of(me * 16, 16), 16)
        for p in peers:
            push(gsend.at[1, p, :, cols], tab_out.at[mine_rows, cols], p, 5).start()
        pltpu.make_async_copy(gsend.at[1, me, :, cols], tab_out.at[mine_rows, cols], out_sem.at[0]).start()

    lane128 = iota((CAP, 128), 1)
    rows = jnp.broadcast_to(gates_all[...], (N, 8, 512)).reshape(CAP, 512)

    def pre(q, table):
        gcol = []
        for j in range(2):
            here = iota((CAP, 512), 1) == q * 256 + me * 16 + j * 8 + iota((CAP, 512), 0) % 8
            gcol.append(jnp.sum(jnp.where(here, rows, 0.0), axis=1, keepdims=True))

        def rstep(c, acc):
            cols = pl.ds(pl.multiple_of(c * CH, CH), CH)
            rall = rrecv[:, :, cols].reshape(TOK, CH)
            hall = hsend[q, :, :, cols].astype(F32)
            out = []
            for j in range(2):
                rl = dot(e_v[2 * q + j], rall)
                dh_v[2 * q + j, :, cols] = (gcol[j] * (rl * scale)).astype(BF)
                prod = rl * hall[:, 8 * j:8 * j + 8, :].reshape(CAP, CH)
                out.append(acc[j] + ((prod[:, 0:128] + prod[:, 128:256]) + (prod[:, 256:384] + prod[:, 384:512])))
            return tuple(out)
        zero = jnp.zeros((CAP, 128), F32)
        acc = lax.fori_loop(0, NCH, rstep, (zero, zero))
        for j in range(2):
            table = table + jnp.where(lane128 == 2 * q + j, jnp.sum(acc[j], axis=1, keepdims=True) * scale, 0.0)
        return table
    dgsend[...] = lax.fori_loop(0, 2, pre, jnp.zeros((CAP, 128), F32)).reshape(N, 8, 128)
    for p in peers:
        push(dgsend.at[p], dgall.at[me], p, 6).start()
    dgall[pl.ds(me, 1)] = dgsend[pl.ds(me, 1)]
    send_h(0, HALF, HALF)
    send_h(1, 0, HALF)

    def gate_grads():
        wait_recv(dgall, 6)
        mine_of = []
        for l in range(LE):
            col = jnp.sum(jnp.where(iota((N, 8, 128), 2) == l, dgall[...], 0.0), axis=2, keepdims=True).reshape(CAP, 1)
            mine_of.append(jnp.where(iota((CAP, 64), 1) == 4 * (iota((CAP, 64), 0) // 8) + l, col, 0.0).reshape(N, 8, 64))
        spread_g = jnp.concatenate([jnp.concatenate(mine_of[2 * q:2 * q + 2], axis=1).reshape(256, 64) for q in range(2)], axis=0)
        ds = 0.0
        for term in split3(spread_g):
            ds = ds + dot(one_v[...], term)
        probs = probs_v[...]
        dlog = (probs * (ds - jnp.sum(probs * ds, axis=1, keepdims=True))).astype(BF)
        wide_d = jnp.concatenate([dlog, jnp.zeros_like(dlog)], axis=1)
        dlog_v[...] = wide_d
        dlog_v[0:16, :] = (wide_d[0:16].astype(F32) + ids_v[...]).astype(BF)
        dlog_t = dlog.astype(F32).T.astype(BF)
        for c in range(NCH):
            part = dot(dlog_t, x_v[:, c * CH:(c + 1) * CH])
            for i in range(CH // 128):
                ggpart[c // 2, (c % 2) * (CH // 128) + i] = part[:, i * 128:(i + 1) * 128]
        push(ggpart.at[1 - core], ggpair, twin, 8).start()

    def gate_scatter():
        push(ggpart.at[1 - core], ggpair, twin, 8).wait_recv()
        gghalf[...] = ggpart[core] + ggpair[...]
        for p in others:
            push(gghalf.at[p // 2], ggrecv.at[chip], p, 9).start()
        ggrecv[pl.ds(chip, 1)] = gghalf[pl.ds(chip, 1)]
        send_h(1, HALF + CH, CH)
        send_now(0)

    def gate_gather():
        wait_recv(ggrecv, 9, 7)
        total = ggrecv[0]
        for i in range(1, 8):
            total = total + ggrecv[i]
        ggall[core, pl.ds(chip, 1)] = total.reshape(1, 64, 128)
        for p in others:
            push(ggall.at[core, chip], ggall.at[core, chip], p, 10).start()
        for c in range(1, NOW):
            send_now(c)

    def bwd(q, carry):
        for j in range(2):
            e = (1 - q) * (2 + j) + q * (1 - j)
            slot = (1 - q) * (2 - 2 * j) + q * (1 + j)
            if j == 1:
                @pl.when(q == 1)
                def _():
                    weight2(0, 2).wait()
            du = dot(dh_v[e], w2[slot], 1, 1).astype(BF).astype(F32)
            da_v[e] = (gp_v[e] * du).astype(BF)
            if j == 0:
                @pl.when(q == 0)
                def _():
                    weight2(0, 2).start()

        @pl.when(q == 1)
        def _():
            gate_scatter()
            weight1(0, 2).wait()

        def step(c, carry):
            cols = pl.ds(pl.multiple_of(c * CH, CH), CH)
            outs = []
            for j in range(2):
                slot = (1 - q) * (2 - 2 * j) + q * (2 - j)
                outs.append(dot(da_v[2 * (1 - q) + j], w1[slot, cols, :], 1, 1).reshape(N, 8, CH))
            gsend[1 - q, :, :, cols] = jnp.concatenate(outs, axis=1).astype(BF)
            return carry
        lax.fori_loop(0, NCH, step, 0)

        @pl.when(q == 0)
        def _():
            weight1(0, 2).start()
            gate_grads()
            send_h(1, HALF, CH)
        return carry
    lax.fori_loop(0, 2, bwd, 0)
    later = [pltpu.make_async_copy(gsend.at[0], glater_out.at[:, :, pl.ds(0, HID)], out_sem.at[0])]
    if NOW < NCH:
        later.append(pltpu.make_async_copy(gsend.at[1, :, :, pl.ds(NOW * CH, HID - NOW * CH)],
                                           glater_out.at[:, :, pl.ds(HID, HID - NOW * CH)], out_sem.at[0]))
    for cp in later:
        cp.start()
    pltpu.make_async_copy(dh_v, dh_out, out_sem.at[0]).start()
    pltpu.make_async_copy(da_v, da_out, out_sem.at[0]).start()

    cp_dlog = pltpu.make_async_copy(dlog_v, tab_out.at[:, pl.ds(NOW * CH, 128)], out_sem.at[0])
    cp_dlog.start()

    gate_gather()

    wait_h(hrecv, recv_sem.at[4])
    wait_send(xsend, 1)

    def ystep(c, acc):
        cols = pl.ds(pl.multiple_of(c * CH, CH), CH)
        h = hrecv[:, :, :, cols].reshape(512, CH)
        tot = x_v[:, cols].astype(F32) + (dot(c_v[0], h) + dot(c_v[1], h) + dot(c_v[2], h))
        y = tot.astype(BF)
        xsend[:, :, cols] = y.reshape(N, 16, CH)
        return acc + jnp.sum(y.astype(F32) * r_v[:, cols].astype(F32), axis=0, keepdims=True)
    losssend[...] = lax.fori_loop(0, NCH, ystep, jnp.zeros((1, CH), F32))
    cp_y = pltpu.make_async_copy(xsend, y_out, out_sem.at[0])
    cp_y.start()
    for p in peers:
        push(losssend, lossall.at[me], p, 7).start()
    lossall[pl.ds(me, 1)] = losssend[...].reshape(1, 1, CH)

    wait_recv(ggall.at[core], 10, 7)
    across = push(ggall.at[core], ggall.at[core], twin, 11)
    across.start()
    across.wait_recv()
    cp_gg = [pltpu.make_async_copy(ggall.at[i // 8, i % 8], gg_out.at[:, pl.ds(i * 128, 128)], out_sem.at[0]) for i in range(N)]
    for cp in cp_gg:
        cp.start()
    wait_recv(lossall, 7)
    loss_out[0, 0] = jnp.sum(lossall[...]) * scale
    part = tab_out.at[pl.ds(0, (N - 1) * 16), pl.ds(0, NOW * CH)]
    pltpu.make_async_copy(part, part, recv_sem.at[5]).wait()

    wait_send(selall, 0)
    wait_send(gates_all, 2)
    wait_h(hsend, send_sem.at[1])
    wait_send(dgall, 6)
    part = gsend.at[1, pl.ds(0, N - 1), :, pl.ds(0, NOW * CH)]
    pltpu.make_async_copy(part, part, send_sem.at[1]).wait()
    for c in range(NOW):
        cols = pl.ds(c * CH, CH)
        pltpu.make_async_copy(gsend.at[1, me, :, cols], tab_out.at[pl.ds(pl.multiple_of(me * 16, 16), 16), cols], out_sem.at[0]).wait()
    wait_send(rsend, 3)
    wait_send(lossall, 7)
    push(ggpart.at[1 - core], ggpair, twin, 8).wait_send()
    wait_send(gghalf, 9, 7)
    wait_send(ggall.at[core], 10, 7)
    across.wait_send()
    for cp in later:
        cp.wait()
    cp_dlog.wait()
    pltpu.make_async_copy(xl_v, xl_out, out_sem.at[0]).wait()
    pltpu.make_async_copy(u_v, u_out, out_sem.at[0]).wait()
    pltpu.make_async_copy(dh_v, dh_out, out_sem.at[0]).wait()
    pltpu.make_async_copy(da_v, da_out, out_sem.at[0]).wait()
    cp_y.wait()
    for cp in cp_gg:
        cp.wait()


def comm_call(sel, x, gw, up, dn, r, scale):
    any_ = pl.BlockSpec(memory_space=pl.ANY)
    vmem = pl.BlockSpec(memory_space=pltpu.VMEM)
    V = pltpu.VMEM
    shape = jax.ShapeDtypeStruct
    return pl.pallas_call(
        functools.partial(comm_kernel, scale),
        out_shape=[shape((N, 16, HID), BF), shape((TOK, NOW * CH + 128), BF), shape((N, 16, 2 * HID - NOW * CH), BF),
                   shape((64, HID), F32), shape((1, 1), F32),
                   shape((LE, CAP, HID), BF), shape((LE, CAP, FF), BF), shape((LE, CAP, HID), BF), shape((LE, CAP, FF), BF)],
        in_specs=[vmem, any_, any_, any_, any_, any_],
        out_specs=[any_, any_, any_, any_, pl.BlockSpec(memory_space=pltpu.SMEM), any_, any_, any_, any_],
        scratch_shapes=[
            V((TOK, HID), BF), V((TOK, HID), BF), V((64, HID), BF),
            V((3, HID, FF), BF), V((3, FF, HID), BF),
            V((N, 16, HID), BF), V((N, 16, HID), BF), V((N, 16, HID), BF), V((N, 16, HID), BF),
            V((2, N, 16, HID), BF), V((2, N, 16, HID), BF), V((2, N, 16, HID), BF),
            V((LE, CAP, HID), BF), V((LE, CAP, HID), BF), V((LE, CAP, FF), BF), V((LE, CAP, FF), F32), V((LE, CAP, FF), BF),
            V((2, 8, 64, 128), F32), V((8, 64, 128), F32), V((8, 64, 128), F32), V((8, 64, 128), F32), V((2, 8, 64, 128), F32),
            V((8, CAP), jnp.int32), V((N, 8, CAP), jnp.int32), V((1, 512), F32), V((N, 1, 512), F32),
            V((1, CH), F32), V((N, 1, CH), F32), V((N, 8, 128), F32), V((N, 8, 128), F32),
            V((TOK, 512), BF), V((3, TOK, 512), BF), V((LE, CAP, TOK), BF), V((TOK, 64), F32), V((TOK, 128), BF), V((16, 128), F32),
            pltpu.SemaphoreType.DMA((2,)), pltpu.SemaphoreType.DMA((2, 3)), pltpu.SemaphoreType.DMA((1,)),
            pltpu.SemaphoreType.DMA((2,)), pltpu.SemaphoreType.DMA((12,)),
        ],
        compiler_params=pltpu.CompilerParams(collective_id=0, has_side_effects=True, vmem_limit_bytes=67043328),
        name='exchange',
    )(sel, x, gw, up, dn, r)


def tile_tools(ins, bufs, outs, tiles, in_sem, out_sem, first):
    def loads(e):
        return [pltpu.make_async_copy(src.at[e], dst.at[e - first], in_sem.at[e - first]) for src, dst in zip(ins, bufs)]

    def stores(i):
        e, c = i // NCH, i % NCH
        cols = pl.ds(pl.multiple_of(c * CH, CH), CH)
        return [pltpu.make_async_copy(tiles[0].at[i - first * NCH], outs[0].at[e, cols, :], out_sem.at[0]),
                pltpu.make_async_copy(tiles[1].at[i - first * NCH], outs[1].at[e, :, cols], out_sem.at[1])]

    def step(i, carry):
        e, c = i // NCH, i % NCH
        xl_v, da_v, u_v, dh_v = bufs
        cols = pl.ds(pl.multiple_of(c * CH, CH), CH)
        tiles[0][i - first * NCH] = dot(xl_v[e - first, :, cols], da_v[e - first], 0, 0).astype(BF)
        tiles[1][i - first * NCH] = dot(u_v[e - first], dh_v[e - first, :, cols], 0, 0).astype(BF)
        for cp in stores(i):
            cp.start()
        return carry

    def finish(i, carry):
        for cp in stores(i):
            cp.wait()
        return carry
    return loads, step, finish


def wgrad1_kernel(xl_in, da_in, u_in, dh_in, y_in, gg_in, loss_in, g1, g2, y, gg, loss,
                  xl_v, da_v, u_v, dh_v, y_v, gg_v, t1, t2, in_sem, out_sem):
    loads, step, finish = tile_tools((xl_in, da_in, u_in, dh_in), (xl_v, da_v, u_v, dh_v), (g1, g2), (t1, t2), in_sem, out_sem, 0)
    cp_y = pltpu.make_async_copy(y_in, y_v, in_sem.at[LE])
    cp_gg = pltpu.make_async_copy(gg_in, gg_v, in_sem.at[LE + 1])
    for cp in loads(0):
        cp.start()
    loss[0, 0] = loss_in[0, 0]

    def expert(e, carry):
        for cp in loads(e):
            cp.wait()

        @pl.when(e + 1 < FIRST)
        def _():
            for cp in loads(e + 1):
                cp.start()

        @pl.when(e == 0)
        def _():
            cp_y.start()
            cp_gg.start()
        lax.fori_loop(e * NCH, (e + 1) * NCH, step, 0)
        return carry
    lax.fori_loop(0, FIRST, expert, 0)
    cp_y.wait()
    cp_gg.wait()
    out_y = pltpu.make_async_copy(y_v, y, in_sem.at[LE])
    out_gg = pltpu.make_async_copy(gg_v, gg, in_sem.at[LE + 1])
    out_y.start()
    out_gg.start()
    out_y.wait()
    out_gg.wait()
    lax.fori_loop(0, FIRST * NCH, finish, 0)


def wgrad1_call(xl, da, u, dh, y, gg, loss):
    shape = jax.ShapeDtypeStruct
    any_ = pl.BlockSpec(memory_space=pl.ANY)
    smem = pl.BlockSpec(memory_space=pltpu.SMEM)
    V = pltpu.VMEM
    return pl.pallas_call(
        wgrad1_kernel,
        in_specs=[any_] * 6 + [smem],
        out_specs=[any_] * 4 + [smem],
        out_shape=[shape((LE, HID, FF), BF), shape((LE, FF, HID), BF), shape((N, 16, HID), BF), shape((64, HID), F32), shape((1, 1), F32)],
        scratch_shapes=[V((FIRST, CAP, HID), BF), V((FIRST, CAP, FF), BF), V((FIRST, CAP, FF), BF), V((FIRST, CAP, HID), BF),
                        V((N, 16, HID), BF), V((64, HID), F32), V((FIRST * NCH, CH, FF), BF), V((FIRST * NCH, FF, CH), BF),
                        pltpu.SemaphoreType.DMA((LE + 2,)), pltpu.SemaphoreType.DMA((2,))],
        compiler_params=pltpu.CompilerParams(vmem_limit_bytes=59000000),
        cost_estimate=pl.CostEstimate(flops=FIRST * 4 * CAP * HID * FF, bytes_accessed=48 * 1024 * 1024, transcendentals=0),
        name='weight_grads_a',
    )(xl, da, u, dh, y, gg, loss)


def gradx_kernel(scale, late_in, r_v, tab_v, gw_v, gx, late_v, gx_v, in_sem, out_sem):
    def pieces(c):
        cols = pl.ds(c * CH, CH)
        out = [pltpu.make_async_copy(late_in.at[:, :, cols], late_v.at[:, :, cols], in_sem.at[c])]
        if c >= NOW:
            more = pl.ds((NCH + c - NOW) * CH, CH)
            out.append(pltpu.make_async_copy(late_in.at[:, :, more], late_v.at[:, :, more], in_sem.at[c]))
        return out
    for c in range(NCH):
        for cp in pieces(c):
            cp.start()
    block = tab_v[0:16, NOW * CH:NOW * CH + 128]
    rows16 = dot(block, ones_where(iota((128, 512), 0) == 64 + iota((128, 512), 1) % 64))
    ids = jnp.sum(jnp.where(iota((16, 512), 1) // 64 == iota((16, 512), 0), rows16, 0.0), axis=0, keepdims=True)
    one = jnp.where(iota((TOK, 512), 0).astype(F32) == ids, 1.0, 0.0).astype(BF)
    dlog = tab_v[:, NOW * CH:NOW * CH + 64]
    for c in range(NCH):
        cols = pl.ds(c * CH, CH)
        tot = r_v[:, cols].astype(F32) * scale + dot(dlog, gw_v[:, cols])
        if c < NOW:
            tot = tot + dot(one[:, 256:512], tab_v[:, cols])
        for cp in pieces(c):
            cp.wait()
        if c >= NOW:
            tot = tot + dot(one[:, 256:512], late_v[:, :, pl.ds((NCH + c - NOW) * CH, CH)].reshape(256, CH))
        gx_v[:, cols] = (tot + dot(one[:, 0:256], late_v[:, :, cols].reshape(256, CH))).astype(BF)
        pltpu.make_async_copy(gx_v.at[:, cols], gx.at[:, cols], out_sem).start()
    for c in range(NCH):
        cols = pl.ds(c * CH, CH)
        pltpu.make_async_copy(gx_v.at[:, cols], gx.at[:, cols], out_sem).wait()


def gradx_call(late, r, tab, gw, scale):
    any_ = pl.BlockSpec(memory_space=pl.ANY)
    vmem = pl.BlockSpec(memory_space=pltpu.VMEM)
    V = pltpu.VMEM
    return pl.pallas_call(
        functools.partial(gradx_kernel, scale),
        in_specs=[any_, vmem, vmem, vmem],
        out_specs=any_,
        out_shape=jax.ShapeDtypeStruct((TOK, HID), BF),
        scratch_shapes=[V((N, 16, 2 * HID - NOW * CH), BF), V((TOK, HID), BF), pltpu.SemaphoreType.DMA((NCH,)), pltpu.SemaphoreType.DMA],
        compiler_params=pltpu.CompilerParams(vmem_limit_bytes=16000000),
        name='grad_x',
    )(late, r, tab, gw)


def solution(mesh):
    def device_step(x, gate_w, up_w, down_w, expert_picks, loss_w):
        scale = 1.0 / math.sqrt(TOK * N * HID)
        gate_t = gate_w.T
        y, tab, later, gg, loss, xl, u, dh, da = comm_call(expert_picks, x, gate_t, up_w, down_w, loss_w, scale)
        later = lax.all_to_all(later, 'ep', 0, 0, tiled=True)
        grad_up, grad_down, y, gg, loss = wgrad1_call(xl, da, u, dh, y, gg, loss)
        grad_x = gradx_call(later, loss_w, tab, gate_t, scale)
        return y.reshape(TOK, HID), loss[0, 0], grad_x, grad_up, grad_down, gg.T

    return jax.shard_map(device_step, mesh=mesh,
                         in_specs=(P('ep'), P(), P('ep'), P('ep'), P('ep'), P('ep')),
                         out_specs=(P('ep'), P(), P('ep'), P('ep'), P('ep'), P()),
                         check_vma=False)
```

```python
import functools
import math
import jax
import jax.numpy as jnp
from jax import lax
from jax.experimental import pallas as pl
from jax.experimental.pallas import tpu as pltpu
from jax.sharding import PartitionSpec as P

BF = jnp.bfloat16
F32 = jnp.float32
MESH = pl.DeviceIdType.MESH
N = 16
TOK = 256
LE = 4
CAP = 128
HID = 2048
FF = 1408
CH = 512
NCH = HID // CH
FIRST = 4
HALF = HID // 2
NOW = 2
ORDER = (14, 12, 8, 15, 13, 9, 6, 4, 7, 5, 10, 11, 2, 3, 1)


def dot(a, b, ca=1, cb=0):
    return lax.dot_general(a, b, (((ca,), (cb,)), ((), ())), preferred_element_type=F32)


def iota(shape, dim):
    return lax.broadcasted_iota(jnp.int32, shape, dim)


def ones_where(cond):
    return jnp.where(cond, 1.0, 0.0).astype(BF)


def split3(v):
    hi = v.astype(BF)
    rest = v - hi.astype(F32)
    mid = rest.astype(BF)
    low = (rest - mid.astype(F32)).astype(BF)
    return hi, mid, low


def flip(me, k):
    out = 0
    for b in range(4):
        bit = (me // (1 << b)) % 2
        if (k >> b) & 1:
            bit = 1 - bit
        out = out + bit * (1 << b)
    return out


def comm_kernel(scale, sel_ref, x_hbm, gw_hbm, up_hbm, dn_hbm, r_hbm,
                y_out, gnow_out, glater_out, tab_out, gg_out, loss_out, xl_out, u_out, dh_out, da_out,
                x_v, r_v, gw_v, w1, w2, xsend, rsend, xrecv, rrecv, hsend, hrecv, gsend,
                xl_v, dh_v, u_v, gp_v, da_v, ggpart, ggpair, gghalf, ggrecv, ggall, selsend, selall, gates, gates_all,
                losssend, lossall, dgsend, dgall, one_v, c_v, e_v, probs_v, dlog_v, ids_v,
                ld_sem, w_sem, out_sem, send_sem, recv_sem):
    me = lax.axis_index('ep')
    peers = [flip(me, k) for k in ORDER]
    core, chip, twin = me % 2, me // 2, flip(me, 1)
    others = [flip(me, k) for k in ORDER if k % 2 == 0]

    def load(src, dst, i):
        return pltpu.make_async_copy(src, dst, ld_sem.at[i])

    def weight1(e, slot):
        return pltpu.make_async_copy(up_hbm.at[e], w1.at[slot], w_sem.at[0, slot])

    def weight2(e, slot):
        return pltpu.make_async_copy(dn_hbm.at[e], w2.at[slot], w_sem.at[1, slot])

    def push(src, dst, peer, i):
        return pltpu.make_async_remote_copy(src_ref=src, dst_ref=dst, send_sem=send_sem.at[0 if i == 1 else 1], recv_sem=recv_sem.at[i],
                                            device_id=(peer,), device_id_type=MESH)

    def wait_recv(buf, i, n=N - 1):
        part = buf.at[pl.ds(0, n)]
        pltpu.make_async_copy(part, part, recv_sem.at[i]).wait()

    def wait_send(buf, i, n=N - 1):
        part = buf.at[pl.ds(0, n)]
        pltpu.make_async_copy(part, part, send_sem.at[0 if i == 1 else 1]).wait()

    cp_x = load(x_hbm, x_v, 0)
    cp_g = load(gw_hbm, gw_v, 0)
    cp_r = load(r_hbm, r_v, 1)
    cp_x.start()
    cp_g.start()
    cp_r.start()

    sel = sel_ref[...]
    selsend[...] = jnp.zeros_like(selsend)
    selsend[0:LE, :] = sel
    selall[pl.ds(me, 1)] = selsend[...].reshape(1, 8, CAP)

    barrier = pltpu.get_barrier_semaphore()
    for p in peers:
        pl.semaphore_signal(barrier, inc=1, device_id=(p,), device_id_type=MESH)
    pl.semaphore_wait(barrier, N - 1)

    for p in peers:
        push(selsend, selall.at[me], p, 0).start()
    for e in range(3):
        weight1(e, e).start()
        weight2(e, e).start()

    cp_g.wait()
    cp_x.wait()
    logits = dot(x_v[...], gw_v[...], 1, 1)
    ex = jnp.exp(logits - jnp.max(logits, axis=1, keepdims=True))
    probs = ex / jnp.sum(ex, axis=1, keepdims=True)
    probs_v[...] = probs

    below = ones_where(iota((TOK, TOK), 1) < iota((TOK, TOK), 0))
    slot_lane = (iota((TOK, TOK), 1) % 16).astype(F32)

    tok_row = iota((TOK, CAP), 0)
    same = iota((CAP, TOK), 0) // 8 == iota((CAP, TOK), 1) // 16
    fold = ones_where(same)
    base = (iota((1, CAP), 1) // 8) * TOK
    hits = [ones_where(tok_row == sel[l:l + 1, :] - base) for l in range(LE)]
    count = dot(hits[0], fold)
    for l in range(1, LE):
        count = count + dot(hits[l], fold)
    pres = count > 0.5
    rank = dot(below, ones_where(pres))
    pick_of = jnp.where(pres, jnp.where(rank == slot_lane, 1.0, 0.0), 0.0).astype(BF)
    for l in range(LE):
        e_v[l] = jnp.where(same, dot(hits[l], pick_of, 0, 0), 0.0).astype(BF)

    place = ones_where(iota((CAP, 512), 0) % 8 == iota((CAP, 512), 1) % 8)
    fold2 = ones_where((iota((512, TOK), 0) % 256) // 16 == iota((512, TOK), 1) // 16)
    for_wait = selall.at[pl.ds(0, N - 1)]
    pltpu.make_async_copy(for_wait, for_wait, recv_sem.at[0]).wait()
    everyone = selall[...].reshape(8 * N, CAP)
    mine = jnp.where(iota((8 * N, CAP), 1) // 8 == me, everyone - me * TOK, 0).astype(F32).astype(BF)
    spread = dot(mine, place)
    lane = iota((8 * N, 512), 1)
    want = ((lane % 256) // 16) * 8 + 2 * (lane // 256) + (lane % 16) // 8
    ids = jnp.sum(jnp.where(iota((8 * N, 512), 0) == want, spread, 0.0), axis=0, keepdims=True)
    one = jnp.where(iota((TOK, 512), 0).astype(F32) == ids, 1.0, 0.0)
    one_v[...] = one.astype(BF)
    pres2 = dot(one_v[...], fold2) > 0.5
    rank2 = dot(below, ones_where(pres2))
    give = jnp.where(pres2, jnp.where(rank2 == slot_lane, 1.0, 0.0), 0.0).astype(BF)
    give_t = give.T

    def gather(src, dst):
        def step(c, carry):
            cols = pl.ds(pl.multiple_of(c * CH, CH), CH)
            dst[:, :, cols] = dot(give_t, src[:, cols]).astype(BF).reshape(N, 16, CH)
            return carry
        lax.fori_loop(0, NCH, step, 0)

    for c in range(NCH):
        cols = pl.ds(c * CH, CH)
        xsend[:, :, cols] = dot(give_t, x_v[:, cols]).astype(BF).reshape(N, 16, CH)
        for p in peers:
            push(xsend.at[p, :, cols], xrecv.at[me, :, cols], p, 1).start()
    xrecv[pl.ds(me, 1)] = xsend[pl.ds(me, 1)]

    rep = ones_where(iota((64, 512), 0) == 4 * ((iota((64, 512), 1) % 256) // 16) + 2 * (iota((64, 512), 1) // 256)
                     + (iota((64, 512), 1) % 16) // 8)
    wide = 0.0
    for term in split3(probs_v[...]):
        wide = wide + dot(term, rep)
    comb = wide * one
    for i, term in enumerate(split3(comb)):
        c_v[i] = term
    gates[...] = jnp.sum(comb, axis=0, keepdims=True)
    for p in peers:
        push(gates, gates_all.at[me], p, 2).start()
    gates_all[pl.ds(me, 1)] = gates[...].reshape(1, 1, 512)

    cp_r.wait()
    gather(r_v, rsend)
    for p in peers:
        push(rsend.at[p], rrecv.at[me], p, 3).start()
    rrecv[pl.ds(me, 1)] = rsend[pl.ds(me, 1)]

    rows16 = jnp.where(iota((16, 512), 1) // 64 == iota((16, 512), 0), jnp.broadcast_to(ids, (16, 512)), 0.0).astype(BF)
    ids_v[...] = dot(rows16, ones_where(iota((512, 128), 1) == 64 + iota((512, 128), 0) % 64))

    wait_recv(xrecv, 1)

    def send_h(q, start, width):
        cols = pl.ds(start, width)
        for p in peers:
            push(hsend.at[q, p, :, cols], hrecv.at[q, me, :, cols], p, 4).start()

    def wait_h(buf, sem):
        part = buf.at[:, pl.ds(0, N - 1)]
        pltpu.make_async_copy(part, part, sem).wait()

    def fwd(q, carry):
        for j in range(2):
            e = 2 * q + j
            slot = e % 3
            xl = dot(e_v[e], xrecv[...].reshape(TOK, HID)).astype(BF)
            xl_v[e] = xl
            weight1(e, slot).wait()
            a = dot(xl_v[e], w1[slot])
            if j == 0:
                @pl.when(q == 0)
                def _():
                    weight1(3, 0).start()
            k0 = math.sqrt(2.0 / math.pi)
            t = jnp.tanh(k0 * (a + 0.044715 * (a * a * a)))
            u_v[e] = (0.5 * a * (1.0 + t)).astype(BF)
            gp_v[e] = 0.5 * (1.0 + t) + 0.5 * a * (1.0 - t * t) * (k0 * (1.0 + 3.0 * 0.044715 * (a * a)))
        weight2(2 * q, (2 * q) % 3).wait()
        weight2(2 * q + 1, (2 * q + 1) % 3).wait()

        def step(c, carry):
            cols = pl.ds(pl.multiple_of(c * CH, CH), CH)
            outs = [dot(u_v[2 * q + j], w2[(2 * q + j) % 3, :, cols]).reshape(N, 8, CH) for j in range(2)]
            hsend[q, :, :, cols] = jnp.concatenate(outs, axis=1).astype(BF)
            return carry
        lax.fori_loop(0, NCH, step, 0)

        @pl.when(q == 0)
        def _():
            weight2(3, 0).start()
        hrecv[q, pl.ds(me, 1)] = hsend[q, pl.ds(me, 1)]

        @pl.when(q == 0)
        def _():
            send_h(0, 0, HALF)
        return carry
    lax.fori_loop(0, 2, fwd, 0)
    pltpu.make_async_copy(xl_v, xl_out, out_sem.at[0]).start()
    pltpu.make_async_copy(u_v, u_out, out_sem.at[0]).start()

    wait_recv(gates_all, 2)
    wait_recv(rrecv, 3)

    def send_now(c):
        cols = pl.ds(c * CH, CH)
        for p in peers:
            push(gsend.at[1, p, :, cols], gnow_out.at[me, :, cols], p, 5).start()
        pltpu.make_async_copy(gsend.at[1, me, :, cols], gnow_out.at[me, :, cols], out_sem.at[0]).start()

    lane128 = iota((CAP, 128), 1)
    rows = jnp.broadcast_to(gates_all[...], (N, 8, 512)).reshape(CAP, 512)

    def pre(q, table):
        gcol = []
        for j in range(2):
            here = iota((CAP, 512), 1) == q * 256 + me * 16 + j * 8 + iota((CAP, 512), 0) % 8
            gcol.append(jnp.sum(jnp.where(here, rows, 0.0), axis=1, keepdims=True))

        def rstep(c, acc):
            cols = pl.ds(pl.multiple_of(c * CH, CH), CH)
            rall = rrecv[:, :, cols].reshape(TOK, CH)
            hall = hsend[q, :, :, cols].astype(F32)
            out = []
            for j in range(2):
                rl = dot(e_v[2 * q + j], rall)
                dh_v[2 * q + j, :, cols] = (gcol[j] * (rl * scale)).astype(BF)
                prod = rl * hall[:, 8 * j:8 * j + 8, :].reshape(CAP, CH)
                out.append(acc[j] + ((prod[:, 0:128] + prod[:, 128:256]) + (prod[:, 256:384] + prod[:, 384:512])))
            return tuple(out)
        zero = jnp.zeros((CAP, 128), F32)
        acc = lax.fori_loop(0, NCH, rstep, (zero, zero))
        for j in range(2):
            table = table + jnp.where(lane128 == 2 * q + j, jnp.sum(acc[j], axis=1, keepdims=True) * scale, 0.0)
        return table
    dgsend[...] = lax.fori_loop(0, 2, pre, jnp.zeros((CAP, 128), F32)).reshape(N, 8, 128)
    for p in peers:
        push(dgsend.at[p], dgall.at[me], p, 6).start()
    dgall[pl.ds(me, 1)] = dgsend[pl.ds(me, 1)]
    send_h(0, HALF, HALF)
    send_h(1, 0, HALF)

    def gate_grads():
        wait_recv(dgall, 6)
        mine_of = []
        for l in range(LE):
            col = jnp.sum(jnp.where(iota((N, 8, 128), 2) == l, dgall[...], 0.0), axis=2, keepdims=True).reshape(CAP, 1)
            mine_of.append(jnp.where(iota((CAP, 64), 1) == 4 * (iota((CAP, 64), 0) // 8) + l, col, 0.0).reshape(N, 8, 64))
        spread_g = jnp.concatenate([jnp.concatenate(mine_of[2 * q:2 * q + 2], axis=1).reshape(256, 64) for q in range(2)], axis=0)
        ds = 0.0
        for term in split3(spread_g):
            ds = ds + dot(one_v[...], term)
        probs = probs_v[...]
        dlog = (probs * (ds - jnp.sum(probs * ds, axis=1, keepdims=True))).astype(BF)
        wide_d = jnp.concatenate([dlog, jnp.zeros_like(dlog)], axis=1)
        dlog_v[...] = wide_d
        dlog_v[0:16, :] = (wide_d[0:16].astype(F32) + ids_v[...]).astype(BF)
        dlog_t = dlog.astype(F32).T.astype(BF)
        for c in range(NCH):
            part = dot(dlog_t, x_v[:, c * CH:(c + 1) * CH])
            for i in range(CH // 128):
                ggpart[c // 2, (c % 2) * (CH // 128) + i] = part[:, i * 128:(i + 1) * 128]
        push(ggpart.at[1 - core], ggpair, twin, 8).start()

    def gate_scatter():
        push(ggpart.at[1 - core], ggpair, twin, 8).wait_recv()
        gghalf[...] = ggpart[core] + ggpair[...]
        for p in others:
            push(gghalf.at[p // 2], ggrecv.at[chip], p, 9).start()
        ggrecv[pl.ds(chip, 1)] = gghalf[pl.ds(chip, 1)]
        send_h(1, HALF + CH, CH)
        send_now(0)

    def gate_gather():
        wait_recv(ggrecv, 9, 7)
        total = ggrecv[0]
        for i in range(1, 8):
            total = total + ggrecv[i]
        ggall[core, pl.ds(chip, 1)] = total.reshape(1, 64, 128)
        for p in others:
            push(ggall.at[core, chip], ggall.at[core, chip], p, 10).start()
        for c in range(1, NOW):
            send_now(c)

    def bwd(q, carry):
        for j in range(2):
            e = (1 - q) * (2 + j) + q * (1 - j)
            slot = (1 - q) * (2 - 2 * j) + q * (1 + j)
            if j == 1:
                @pl.when(q == 1)
                def _():
                    weight2(0, 2).wait()
            du = dot(dh_v[e], w2[slot], 1, 1).astype(BF).astype(F32)
            da_v[e] = (gp_v[e] * du).astype(BF)
            if j == 0:
                @pl.when(q == 0)
                def _():
                    weight2(0, 2).start()

        @pl.when(q == 1)
        def _():
            gate_scatter()
            weight1(0, 2).wait()

        def step(c, carry):
            cols = pl.ds(pl.multiple_of(c * CH, CH), CH)
            outs = []
            for j in range(2):
                slot = (1 - q) * (2 - 2 * j) + q * (2 - j)
                outs.append(dot(da_v[2 * (1 - q) + j], w1[slot, cols, :], 1, 1).reshape(N, 8, CH))
            gsend[1 - q, :, :, cols] = jnp.concatenate(outs, axis=1).astype(BF)
            return carry
        lax.fori_loop(0, NCH, step, 0)

        @pl.when(q == 0)
        def _():
            weight1(0, 2).start()
            gate_grads()
            send_h(1, HALF, CH)
        return carry
    lax.fori_loop(0, 2, bwd, 0)
    later = [pltpu.make_async_copy(gsend.at[0], glater_out.at[:, :, pl.ds(0, HID)], out_sem.at[0])]
    if NOW < NCH:
        later.append(pltpu.make_async_copy(gsend.at[1, :, :, pl.ds(NOW * CH, HID - NOW * CH)],
                                           glater_out.at[:, :, pl.ds(HID, HID - NOW * CH)], out_sem.at[0]))
    for cp in later:
        cp.start()
    pltpu.make_async_copy(dh_v, dh_out, out_sem.at[0]).start()
    pltpu.make_async_copy(da_v, da_out, out_sem.at[0]).start()

    cp_dlog = pltpu.make_async_copy(dlog_v, tab_out, out_sem.at[0])
    cp_dlog.start()

    gate_gather()

    wait_h(hrecv, recv_sem.at[4])
    wait_send(xsend, 1)

    def ystep(c, acc):
        cols = pl.ds(pl.multiple_of(c * CH, CH), CH)
        h = hrecv[:, :, :, cols].reshape(512, CH)
        tot = x_v[:, cols].astype(F32) + (dot(c_v[0], h) + dot(c_v[1], h) + dot(c_v[2], h))
        y = tot.astype(BF)
        xsend[:, :, cols] = y.reshape(N, 16, CH)
        return acc + jnp.sum(y.astype(F32) * r_v[:, cols].astype(F32), axis=0, keepdims=True)
    losssend[...] = lax.fori_loop(0, NCH, ystep, jnp.zeros((1, CH), F32))
    cp_y = pltpu.make_async_copy(xsend, y_out, out_sem.at[0])
    cp_y.start()
    for p in peers:
        push(losssend, lossall.at[me], p, 7).start()
    lossall[pl.ds(me, 1)] = losssend[...].reshape(1, 1, CH)

    wait_recv(ggall.at[core], 10, 7)
    across = push(ggall.at[core], ggall.at[core], twin, 11)
    across.start()
    across.wait_recv()
    cp_gg = [pltpu.make_async_copy(ggall.at[i // 8, i % 8], gg_out.at[:, pl.ds(i * 128, 128)], out_sem.at[0]) for i in range(N)]
    for cp in cp_gg:
        cp.start()
    wait_recv(lossall, 7)
    loss_out[0, 0] = jnp.sum(lossall[...]) * scale
    wait_recv(gnow_out, 5)

    wait_send(selall, 0)
    wait_send(gates_all, 2)
    wait_h(hsend, send_sem.at[1])
    wait_send(dgall, 6)
    part = gsend.at[1, pl.ds(0, N - 1), :, pl.ds(0, NOW * CH)]
    pltpu.make_async_copy(part, part, send_sem.at[1]).wait()
    for c in range(NOW):
        cols = pl.ds(c * CH, CH)
        pltpu.make_async_copy(gsend.at[1, me, :, cols], gnow_out.at[me, :, cols], out_sem.at[0]).wait()
    wait_send(rsend, 3)
    wait_send(lossall, 7)
    push(ggpart.at[1 - core], ggpair, twin, 8).wait_send()
    wait_send(gghalf, 9, 7)
    wait_send(ggall.at[core], 10, 7)
    across.wait_send()
    for cp in later:
        cp.wait()
    cp_dlog.wait()
    pltpu.make_async_copy(xl_v, xl_out, out_sem.at[0]).wait()
    pltpu.make_async_copy(u_v, u_out, out_sem.at[0]).wait()
    pltpu.make_async_copy(dh_v, dh_out, out_sem.at[0]).wait()
    pltpu.make_async_copy(da_v, da_out, out_sem.at[0]).wait()
    cp_y.wait()
    for cp in cp_gg:
        cp.wait()


def comm_call(sel, x, gw, up, dn, r, scale):
    any_ = pl.BlockSpec(memory_space=pl.ANY)
    vmem = pl.BlockSpec(memory_space=pltpu.VMEM)
    V = pltpu.VMEM
    shape = jax.ShapeDtypeStruct
    return pl.pallas_call(
        functools.partial(comm_kernel, scale),
        out_shape=[shape((N, 16, HID), BF), shape((N, 16, NOW * CH), BF), shape((N, 16, 2 * HID - NOW * CH), BF), shape((TOK, 128), BF),
                   shape((64, HID), F32), shape((1, 1), F32),
                   shape((LE, CAP, HID), BF), shape((LE, CAP, FF), BF), shape((LE, CAP, HID), BF), shape((LE, CAP, FF), BF)],
        in_specs=[vmem, any_, any_, any_, any_, any_],
        out_specs=[any_, any_, any_, any_, any_, pl.BlockSpec(memory_space=pltpu.SMEM), any_, any_, any_, any_],
        scratch_shapes=[
            V((TOK, HID), BF), V((TOK, HID), BF), V((64, HID), BF),
            V((3, HID, FF), BF), V((3, FF, HID), BF),
            V((N, 16, HID), BF), V((N, 16, HID), BF), V((N, 16, HID), BF), V((N, 16, HID), BF),
            V((2, N, 16, HID), BF), V((2, N, 16, HID), BF), V((2, N, 16, HID), BF),
            V((LE, CAP, HID), BF), V((LE, CAP, HID), BF), V((LE, CAP, FF), BF), V((LE, CAP, FF), F32), V((LE, CAP, FF), BF),
            V((2, 8, 64, 128), F32), V((8, 64, 128), F32), V((8, 64, 128), F32), V((8, 64, 128), F32), V((2, 8, 64, 128), F32),
            V((8, CAP), jnp.int32), V((N, 8, CAP), jnp.int32), V((1, 512), F32), V((N, 1, 512), F32),
            V((1, CH), F32), V((N, 1, CH), F32), V((N, 8, 128), F32), V((N, 8, 128), F32),
            V((TOK, 512), BF), V((3, TOK, 512), BF), V((LE, CAP, TOK), BF), V((TOK, 64), F32), V((TOK, 128), BF), V((16, 128), F32),
            pltpu.SemaphoreType.DMA((2,)), pltpu.SemaphoreType.DMA((2, 3)), pltpu.SemaphoreType.DMA((1,)),
            pltpu.SemaphoreType.DMA((2,)), pltpu.SemaphoreType.DMA((12,)),
        ],
        compiler_params=pltpu.CompilerParams(collective_id=0, has_side_effects=True, vmem_limit_bytes=67043328),
        name='exchange',
    )(sel, x, gw, up, dn, r)


def tile_tools(ins, bufs, outs, tiles, in_sem, out_sem, first):
    def loads(e):
        return [pltpu.make_async_copy(src.at[e], dst.at[e - first], in_sem.at[e - first]) for src, dst in zip(ins, bufs)]

    def stores(i):
        e, c = i // NCH, i % NCH
        cols = pl.ds(pl.multiple_of(c * CH, CH), CH)
        return [pltpu.make_async_copy(tiles[0].at[i - first * NCH], outs[0].at[e, cols, :], out_sem.at[0]),
                pltpu.make_async_copy(tiles[1].at[i - first * NCH], outs[1].at[e, :, cols], out_sem.at[1])]

    def step(i, carry):
        e, c = i // NCH, i % NCH
        xl_v, da_v, u_v, dh_v = bufs
        cols = pl.ds(pl.multiple_of(c * CH, CH), CH)
        tiles[0][i - first * NCH] = dot(xl_v[e - first, :, cols], da_v[e - first], 0, 0).astype(BF)
        tiles[1][i - first * NCH] = dot(u_v[e - first], dh_v[e - first, :, cols], 0, 0).astype(BF)
        for cp in stores(i):
            cp.start()
        return carry

    def finish(i, carry):
        for cp in stores(i):
            cp.wait()
        return carry
    return loads, step, finish


def wgrad1_kernel(xl_in, da_in, u_in, dh_in, y_in, gg_in, loss_in, g1, g2, y, gg, loss,
                  xl_v, da_v, u_v, dh_v, y_v, gg_v, t1, t2, in_sem, out_sem):
    loads, step, finish = tile_tools((xl_in, da_in, u_in, dh_in), (xl_v, da_v, u_v, dh_v), (g1, g2), (t1, t2), in_sem, out_sem, 0)
    cp_y = pltpu.make_async_copy(y_in, y_v, in_sem.at[LE])
    cp_gg = pltpu.make_async_copy(gg_in, gg_v, in_sem.at[LE + 1])
    for cp in loads(0):
        cp.start()
    loss[0, 0] = loss_in[0, 0]

    def expert(e, carry):
        for cp in loads(e):
            cp.wait()

        @pl.when(e + 1 < FIRST)
        def _():
            for cp in loads(e + 1):
                cp.start()

        @pl.when(e == 0)
        def _():
            cp_y.start()
            cp_gg.start()
        lax.fori_loop(e * NCH, (e + 1) * NCH, step, 0)
        return carry
    lax.fori_loop(0, FIRST, expert, 0)
    cp_y.wait()
    cp_gg.wait()
    out_y = pltpu.make_async_copy(y_v, y, in_sem.at[LE])
    out_gg = pltpu.make_async_copy(gg_v, gg, in_sem.at[LE + 1])
    out_y.start()
    out_gg.start()
    out_y.wait()
    out_gg.wait()
    lax.fori_loop(0, FIRST * NCH, finish, 0)


def wgrad1_call(xl, da, u, dh, y, gg, loss):
    shape = jax.ShapeDtypeStruct
    any_ = pl.BlockSpec(memory_space=pl.ANY)
    smem = pl.BlockSpec(memory_space=pltpu.SMEM)
    V = pltpu.VMEM
    return pl.pallas_call(
        wgrad1_kernel,
        in_specs=[any_] * 6 + [smem],
        out_specs=[any_] * 4 + [smem],
        out_shape=[shape((LE, HID, FF), BF), shape((LE, FF, HID), BF), shape((N, 16, HID), BF), shape((64, HID), F32), shape((1, 1), F32)],
        scratch_shapes=[V((FIRST, CAP, HID), BF), V((FIRST, CAP, FF), BF), V((FIRST, CAP, FF), BF), V((FIRST, CAP, HID), BF),
                        V((N, 16, HID), BF), V((64, HID), F32), V((FIRST * NCH, CH, FF), BF), V((FIRST * NCH, FF, CH), BF),
                        pltpu.SemaphoreType.DMA((LE + 2,)), pltpu.SemaphoreType.DMA((2,))],
        compiler_params=pltpu.CompilerParams(vmem_limit_bytes=59000000),
        cost_estimate=pl.CostEstimate(flops=FIRST * 4 * CAP * HID * FF, bytes_accessed=48 * 1024 * 1024, transcendentals=0),
        name='weight_grads_a',
    )(xl, da, u, dh, y, gg, loss)


def gradx_kernel(scale, late_in, now_v, r_v, tab_v, gw_v, gx, late_v, gx_v, in_sem, out_sem):
    def pieces(c):
        cols = pl.ds(c * CH, CH)
        out = [pltpu.make_async_copy(late_in.at[:, :, cols], late_v.at[:, :, cols], in_sem.at[c])]
        if c >= NOW:
            more = pl.ds((NCH + c - NOW) * CH, CH)
            out.append(pltpu.make_async_copy(late_in.at[:, :, more], late_v.at[:, :, more], in_sem.at[c]))
        return out
    for c in range(NCH):
        for cp in pieces(c):
            cp.start()
    block = tab_v[0:16, :]
    rows16 = dot(block, ones_where(iota((128, 512), 0) == 64 + iota((128, 512), 1) % 64))
    ids = jnp.sum(jnp.where(iota((16, 512), 1) // 64 == iota((16, 512), 0), rows16, 0.0), axis=0, keepdims=True)
    one = jnp.where(iota((TOK, 512), 0).astype(F32) == ids, 1.0, 0.0).astype(BF)
    dlog = tab_v[:, 0:64]
    for c in range(NCH):
        cols = pl.ds(c * CH, CH)
        tot = r_v[:, cols].astype(F32) * scale + dot(dlog, gw_v[:, cols])
        if c < NOW:
            tot = tot + dot(one[:, 256:512], now_v[:, :, cols].reshape(256, CH))
        for cp in pieces(c):
            cp.wait()
        if c >= NOW:
            tot = tot + dot(one[:, 256:512], late_v[:, :, pl.ds((NCH + c - NOW) * CH, CH)].reshape(256, CH))
        gx_v[:, cols] = (tot + dot(one[:, 0:256], late_v[:, :, cols].reshape(256, CH))).astype(BF)
        pltpu.make_async_copy(gx_v.at[:, cols], gx.at[:, cols], out_sem).start()
    for c in range(NCH):
        cols = pl.ds(c * CH, CH)
        pltpu.make_async_copy(gx_v.at[:, cols], gx.at[:, cols], out_sem).wait()


def gradx_call(late, now, r, tab, gw, scale):
    any_ = pl.BlockSpec(memory_space=pl.ANY)
    vmem = pl.BlockSpec(memory_space=pltpu.VMEM)
    V = pltpu.VMEM
    return pl.pallas_call(
        functools.partial(gradx_kernel, scale),
        in_specs=[any_, vmem, vmem, vmem, vmem],
        out_specs=any_,
        out_shape=jax.ShapeDtypeStruct((TOK, HID), BF),
        scratch_shapes=[V((N, 16, 2 * HID - NOW * CH), BF), V((TOK, HID), BF), pltpu.SemaphoreType.DMA((NCH,)), pltpu.SemaphoreType.DMA],
        compiler_params=pltpu.CompilerParams(vmem_limit_bytes=16000000),
        name='grad_x',
    )(late, now, r, tab, gw)


def solution(mesh):
    def device_step(x, gate_w, up_w, down_w, expert_picks, loss_w):
        scale = 1.0 / math.sqrt(TOK * N * HID)
        gate_t = gate_w.T
        y, now, later, tab, gg, loss, xl, u, dh, da = comm_call(expert_picks, x, gate_t, up_w, down_w, loss_w, scale)
        later = lax.all_to_all(later, 'ep', 0, 0, tiled=True)
        grad_up, grad_down, y, gg, loss = wgrad1_call(xl, da, u, dh, y, gg, loss)
        grad_x = gradx_call(later, now, loss_w, tab, gate_t, scale)
        return y.reshape(TOK, HID), loss[0, 0], grad_x, grad_up, grad_down, gg.T

    return jax.shard_map(device_step, mesh=mesh,
                         in_specs=(P('ep'), P(), P('ep'), P('ep'), P('ep'), P('ep')),
                         out_specs=(P('ep'), P(), P('ep'), P('ep'), P('ep'), P()),
                         check_vma=False)
```
